32 devices in a mesh: ctx: 8 (over y, x, core), head: 4 (over z).
Axes of the slice: x: 2, y: 2, z: 4, core: 2. Of those that a mesh axis runs over, the one named last changes fastest.
Arguments:
- prompt_values: bfloat16 [4096, 8192], P('ctx', 'head'), may hold values from -6 to 6
- prompt_gate: bfloat16 [4096, 8192], P('ctx', 'head'), may hold values from -6 to 6
- prompt_inject: bfloat16 [4096, 4, 256], P('ctx', 'head'), may hold values from -6 to 6
- prompt_read: bfloat16 [4096, 4, 256], P('ctx', 'head'), may hold values from -0.375 to 0.375
- prompt_step: float32 [128, 4096], P('head', 'ctx'), may hold values from -8 to 256
- decay_log: float32 [128], P('head'), may hold values from -10 to 0
- skip_gain: float32 [128], P('head'), may hold values from 0.5 to 1.5
- norm_weight: float32 [8192], P('head'), may hold values from 0.1 to 1.9
- out_weight: bfloat16 [8192, 4096], P('head'), may hold values from -0.0625 to 0.0625
- sample_values: bfloat16 [16, 16, 8192], P('ctx', None, 'head'), may hold values from -6 to 6
- sample_gate: bfloat16 [16, 16, 8192], P('ctx', None, 'head'), may hold values from -6 to 6
- sample_inject: bfloat16 [16, 16, 4, 256], P('ctx', None, 'head'), may hold values from -6 to 6
- sample_read: bfloat16 [16, 16, 4, 256], P('ctx', None, 'head'), may hold values from -0.375 to 0.375
- sample_step: float32 [128, 16, 16], P('head', 'ctx'), may hold values from -8 to 256
- sample_length: int32 [16], P('ctx'), may hold values from 1 to 16
Outputs:
- prompt_mixed: bfloat16 [4096, 4096], P('head', 'ctx')
- sample_mixed: bfloat16 [4096, 16], P('head', 'ctx')
The draws below stay inside these ranges and needn't reach their ends.
All inputs are finite; a program needn't handle non-finite values.
Results may differ from the reference program's by a relative error of at most 0.02.
Values may be sent and summed in bfloat16 or wider, within the bound.
A program may use at most 192 MiB of HBM per device.

```python
import jax
import jax.numpy as jnp
from jax import lax

LOCAL_HEAD_COUNT = 128
HEAD_DIM = 64
STATE = 256
HEAD_GROUPS = 4
OUT_COLS = 4096
BLOCK = 128
SLEN = 16
TOK_DEV = 512
NTOK = 4096
SAMPLES = 16


def head_memory(key):
    base_key = jax.random.fold_in(key, 11)
    sorter, spreader = jax.random.split(base_key, 2)
    chooser = jax.random.uniform(sorter, (LOCAL_HEAD_COUNT,), jnp.float32)
    fast_share = 0.3
    middle_share = 0.5
    position = jax.random.uniform(spreader, (LOCAL_HEAD_COUNT,), jnp.float32)
    fast_memory = 30.0 * (5.0 / 3.0) ** position
    middle_memory = 50.0 * (2.5 * NTOK / 50.0) ** position
    slow_memory = 2.5 * NTOK * 2.4 ** position
    return jnp.where(chooser < fast_share, fast_memory, jnp.where(chooser < middle_share, middle_memory, slow_memory))


def spike_mask(key):
    places = jax.random.randint(jax.random.fold_in(key, 23), (HEAD_GROUPS, 2), 0, NTOK)
    positions = jnp.arange(NTOK)
    return jnp.any(positions[:, None, None] == places[None], axis=2)


def draw_decay_log(key, part):
    return (-0.5 * jnp.log(head_memory(key))).astype(jnp.float32)


def draw_prompt_step(key, part):
    memory = head_memory(key)
    decay_velocity = memory ** (-0.5)
    token_key, device_key, keeper_key = jax.random.split(jax.random.fold_in(key, 37), 3)
    token_factor = jnp.exp(jax.random.uniform(token_key, (LOCAL_HEAD_COUNT, NTOK), jnp.float32, -0.7, 0.7))
    device_factor = jnp.exp(jax.random.uniform(device_key, (LOCAL_HEAD_COUNT, NTOK // TOK_DEV), jnp.float32, -0.7, 0.7))
    stable_state = decay_velocity[:, None] * token_factor * jnp.repeat(device_factor, TOK_DEV, axis=1)
    retained_fraction = jax.random.uniform(keeper_key, (LOCAL_HEAD_COUNT, NTOK), jnp.float32, 0.5, 0.8)
    spike_steps = jnp.minimum(-jnp.log(retained_fraction) / decay_velocity[:, None], 250.0)
    inside_spike = jnp.repeat(spike_mask(key).T, LOCAL_HEAD_COUNT // HEAD_GROUPS, axis=0)
    selected_rows = jnp.where(inside_spike, spike_steps, stable_state)
    return (selected_rows + jnp.log(-jnp.expm1(-selected_rows))).astype(jnp.float32)


def draw_sample_step(key, part):
    memory = head_memory(key)
    token_factor = jnp.exp(jax.random.uniform(jax.random.fold_in(key, 53), (LOCAL_HEAD_COUNT, SAMPLES, SLEN), jnp.float32, -0.7, 0.7))
    stable_state = (memory ** (-0.5))[:, None, None] * token_factor
    return (stable_state + jnp.log(-jnp.expm1(-stable_state))).astype(jnp.float32)


def draw_prompt_inject(key, part):
    noise_key = jax.random.fold_in(key, 41)
    raw_noise = jnp.clip(jax.random.normal(noise_key, (NTOK, HEAD_GROUPS, STATE), jnp.float32), -6.0, 6.0)
    attenuation = jnp.where(spike_mask(key)[:, :, None], 0.02, 1.0)
    return (raw_noise * attenuation).astype(jnp.bfloat16)


def touch_ends(array, stream_key, smallest, high):
    spot = [jax.random.randint(jax.random.fold_in(stream_key, axis), (), 0, length) for axis, length in enumerate(array.shape)]
    main_axis = array.shape.index(max(array.shape))
    next_to = spot[:main_axis] + [(spot[main_axis] + 1) % array.shape[main_axis]] + spot[main_axis + 1:]
    return array.at[tuple(spot)].set(smallest).at[tuple(next_to)].set(high)


def steps_of(stream_key, extent, pieces, low, high):
    factor_of, own = 1.0, jax.random.fold_in(stream_key, 6)
    for dim, parts in pieces:
        steps = jnp.exp(jax.random.uniform(jax.random.fold_in(own, dim), (parts,), jnp.float32, low / len(pieces), high / len(pieces)))
        factor_of = factor_of * jnp.repeat(steps, extent[dim] // parts).reshape([-1 if axis == dim else 1 for axis in range(len(extent))])
    return factor_of


def gaussian(stream_key, shape, deviation, reach, pieces=(), dtype=jnp.bfloat16):
    gain = steps_of(stream_key, shape, pieces, -0.22, 0.18) if pieces else 1.0
    array = jax.random.normal(stream_key, shape, jnp.float32) * deviation * gain
    return jnp.minimum(jnp.maximum(array, -reach), reach).astype(dtype)


def setup_inputs(seed: int = 0) -> dict:
    splits = jax.random.split(jax.random.key(seed), 16)
    return {
        "prompt_values": gaussian(splits[0], (NTOK, LOCAL_HEAD_COUNT * HEAD_DIM), 1.0, 6.0, ((0, 8), (1, 4))),
        "prompt_gate": gaussian(splits[1], (NTOK, LOCAL_HEAD_COUNT * HEAD_DIM), 1.0, 6.0, ((0, 8), (1, 4))),
        "prompt_inject": draw_prompt_inject(jax.random.fold_in(splits[15], 71), 0),
        "prompt_read": gaussian(splits[3], (NTOK, HEAD_GROUPS, STATE), STATE ** -0.5, 0.375, ((0, 8), (1, 4))),
        "prompt_step": draw_prompt_step(jax.random.fold_in(splits[15], 71), 0),
        "decay_log": draw_decay_log(jax.random.fold_in(splits[15], 71), 0),
        "skip_gain": jnp.clip(0.5 + 1.0 * jax.random.uniform(splits[6], (LOCAL_HEAD_COUNT,), jnp.float32) ** steps_of(splits[6], (LOCAL_HEAD_COUNT,), ((0, 4),), -0.2, 0.2), 0.5, 1.5),
        "norm_weight": jnp.clip(1.0 + 0.18 * jax.random.normal(splits[7], (LOCAL_HEAD_COUNT * HEAD_DIM,), jnp.float32), 0.1, 1.9),
        "out_weight": gaussian(splits[8], (LOCAL_HEAD_COUNT * HEAD_DIM, OUT_COLS), (LOCAL_HEAD_COUNT * HEAD_DIM) ** -0.5, 0.0625, ((0, 4),)),
        "sample_values": gaussian(splits[9], (SAMPLES, SLEN, LOCAL_HEAD_COUNT * HEAD_DIM), 1.0, 6.0, ((0, 8), (2, 4))),
        "sample_gate": gaussian(splits[10], (SAMPLES, SLEN, LOCAL_HEAD_COUNT * HEAD_DIM), 1.0, 6.0, ((0, 8), (2, 4))),
        "sample_inject": gaussian(splits[11], (SAMPLES, SLEN, HEAD_GROUPS, STATE), 1.0, 6.0, ((0, 8), (2, 4))),
        "sample_read": gaussian(splits[12], (SAMPLES, SLEN, HEAD_GROUPS, STATE), STATE ** -0.5, 0.375, ((0, 8), (2, 4))),
        "sample_step": draw_sample_step(jax.random.fold_in(splits[15], 71), 0),
        "sample_length": touch_ends(jax.random.randint(splits[14], (SAMPLES,), 1, SLEN + 1), jax.random.fold_in(splits[14], 1), 1, SLEN).astype(jnp.int32),
    }


full_precision = lax.Precision.HIGHEST

def block_terms(values, inject, readout, steps, decay_rate):
    length = values.shape[0]
    log_decay = steps * decay_rate[:, None]
    running = jnp.cumsum(log_decay, axis=1)
    scores = jnp.dot(readout.astype(jnp.float32), inject.astype(jnp.float32).T, precision=full_precision)
    causal = jnp.arange(length)[:, None] >= jnp.arange(length)[None, :]
    gap_logs = jnp.where(causal[None], running[:, :, None] - running[:, None, :], 0.0)
    mixing = jnp.where(causal[None], scores[None] * jnp.exp(gap_logs) * steps[:, None, :], 0.0).astype(jnp.bfloat16)
    local_out = jnp.einsum('hts,shp->thp', mixing.astype(jnp.float32), values.astype(jnp.float32), precision=full_precision)
    to_end = jnp.exp(running[:, -1:] - running) * steps
    weighted = (to_end[:, :, None] * inject.astype(jnp.float32)[None]).astype(jnp.bfloat16)
    local_state = jnp.einsum('shp,hsn->hpn', values.astype(jnp.float32), weighted.astype(jnp.float32), precision=full_precision)
    return (local_out, local_state, running)

def group_block(values, inject, readout, steps, decay_rate, carry_state):
    local_out, local_state, running = block_terms(values, inject, readout, steps, decay_rate)
    carried = jnp.einsum('tn,hpn->thp', readout.astype(jnp.float32), carry_state, precision=full_precision)
    carried = carried * jnp.exp(running).T[:, :, None]
    next_state = jnp.exp(running[:, -1])[:, None, None] * carry_state + local_state
    return (local_out + carried, next_state, running)

def finish(outputs, values, gate, skip_gain, norm_weight, groups):
    row_count = values.shape[0]
    with_skip = outputs + skip_gain[None, :, None] * values.reshape(row_count, skip_gain.shape[0], -1).astype(jnp.float32)
    gated_out = with_skip.reshape(row_count, -1) * jax.nn.silu(gate.astype(jnp.float32))
    grouped = gated_out.reshape(row_count, groups, -1)
    inverse_rms = lax.rsqrt(lax.optimization_barrier(jnp.mean(grouped * grouped, axis=2, keepdims=True)) + 1e-05)
    return ((grouped * inverse_rms).reshape(row_count, -1) * norm_weight[None]).astype(jnp.bfloat16)

def reference(prompt_values, prompt_gate, prompt_inject, prompt_read, prompt_step, decay_log, skip_gain, norm_weight, out_weight, sample_values, sample_gate, sample_inject, sample_read, sample_step, sample_length):
    per_group = LOCAL_HEAD_COUNT // HEAD_GROUPS
    blocks = NTOK // BLOCK
    decay_rate = (-jnp.exp(decay_log)).reshape(HEAD_GROUPS, per_group)
    steps = jax.nn.softplus(prompt_step).reshape(HEAD_GROUPS, per_group, blocks, BLOCK).transpose(2, 0, 1, 3)
    values = prompt_values.reshape(blocks, BLOCK, HEAD_GROUPS, per_group, HEAD_DIM)
    inject = prompt_inject.reshape(blocks, BLOCK, HEAD_GROUPS, STATE)
    readout = prompt_read.reshape(blocks, BLOCK, HEAD_GROUPS, STATE)
    grouped_block = jax.vmap(group_block, in_axes=(1, 1, 1, 0, 0, 0), out_axes=(1, 0, 0))

    def advance(carry_state, block_data):
        block_values, block_inject, block_readout, block_steps = block_data
        block_out, next_state, running = grouped_block(block_values, block_inject, block_readout, block_steps, decay_rate, carry_state)
        return (next_state, block_out)
    start_state = jnp.zeros((HEAD_GROUPS, per_group, HEAD_DIM, STATE), jnp.float32)
    final_state, outputs = lax.scan(advance, start_state, (values, inject, readout, steps))
    outputs = outputs.reshape(NTOK, LOCAL_HEAD_COUNT, HEAD_DIM)
    normed = finish(outputs, prompt_values, prompt_gate, skip_gain, norm_weight, HEAD_GROUPS)
    weight_full = out_weight.astype(jnp.float32)
    prompt_mixed = jnp.dot(normed.astype(jnp.float32), weight_full, precision=full_precision).T.astype(jnp.bfloat16)
    sample_steps = jax.nn.softplus(sample_step).reshape(HEAD_GROUPS, per_group, SAMPLES, SLEN).transpose(2, 0, 1, 3)
    sample_vals = sample_values.reshape(SAMPLES, SLEN, HEAD_GROUPS, per_group, HEAD_DIM)
    per_sample = jax.vmap(grouped_block, in_axes=(0, 0, 0, 0, None, None), out_axes=(0, 0, 0))
    sample_out = per_sample(sample_vals, sample_inject, sample_read, sample_steps, decay_rate, final_state)[0]
    sample_out = sample_out.reshape(SAMPLES * SLEN, LOCAL_HEAD_COUNT, HEAD_DIM)
    sample_normed = finish(sample_out, sample_values.reshape(SAMPLES * SLEN, -1), sample_gate.reshape(SAMPLES * SLEN, -1), skip_gain, norm_weight, HEAD_GROUPS)
    onehot = (jnp.arange(SLEN)[None, :] == (sample_length - 1)[:, None]).astype(jnp.float32)
    picked = lax.optimization_barrier(jnp.sum(onehot[:, :, None] * sample_normed.reshape(SAMPLES, SLEN, -1).astype(jnp.float32), axis=1)).astype(jnp.bfloat16)
    sample_mixed = jnp.dot(picked.astype(jnp.float32), weight_full, precision=full_precision).T.astype(jnp.bfloat16)
    return (prompt_mixed, sample_mixed)
```

```python
import functools

import jax
import jax.numpy as jnp
from jax import lax
from jax.experimental import pallas as pl
from jax.experimental.pallas import tpu as pltpu
from jax.sharding import PartitionSpec as P

BLOCK = 128
LANES = 128
PAD = 8
F32 = jnp.float32
BF16 = jnp.bfloat16
EXACT = lax.Precision.HIGHEST
VMEM_LIMIT = 60 * 1024 * 1024


def dot(a, b, dims=((1,), (0,)), precision=None):
    return lax.dot_general(a, b, (dims, ((), ())), precision=precision, preferred_element_type=F32)


def softplus(v):
    return jnp.maximum(v, 0.0) + jnp.log1p(jnp.exp(-jnp.abs(v)))


def silu(v):
    return v / (1.0 + jnp.exp(-v))


def spread(w, expander):
    high = w.astype(BF16)
    low = (w - high.astype(F32)).astype(BF16)
    return dot(jnp.concatenate([high, low], axis=1), expander)


def expander_of(heads, dim):
    row = lax.broadcasted_iota(jnp.int32, (2 * heads, heads * dim), 0)
    lane = lax.broadcasted_iota(jnp.int32, (2 * heads, heads * dim), 1)
    head = lane // dim
    return jnp.where((row == head) | (row == head + heads), 1.0, 0.0).astype(BF16)


def square(n):
    return (
        lax.broadcasted_iota(jnp.int32, (n, n), 0),
        lax.broadcasted_iota(jnp.int32, (n, n), 1),
    )


def finish_rows(total, weight):
    mean = jnp.mean(total * total, axis=1, keepdims=True)
    return (total * lax.rsqrt(mean + 1e-05) * weight).astype(BF16)


CHUNK = 4 * LANES


def turn_over(w):
    return jnp.transpose(w, (1, 0))


def layer_kernel(
    dim,
    n,
    peers,
    length_ref,
    values_hbm,
    gate_hbm,
    inject_ref,
    read_ref,
    step_ref,
    decay_ref,
    gain_in_ref,
    norm_ref,
    weight_hbm,
    svalues_ref,
    sgate_ref,
    sinject_ref,
    sread_ref,
    sstep_ref,
    out_hbm,
    sout_ref,
    values_ref,
    gate_ref,
    tiles_ref,
    steps_ref,
    logs_ref,
    wide_ref,
    expander_ref,
    turned_ref,
    skip_ref,
    mine_state,
    pair_state,
    totals,
    arrived,
    before_ref,
    swap_ref,
    enter_ref,
    log_sent,
    log_got,
    pair_scale,
    scale_ref,
    state_ref,
    offset_ref,
    part_ref,
    local_ref,
    gain_ref,
    normed_ref,
    slocal_ref,
    sgain_ref,
    picked_ref,
    picked_got,
    reply_ref,
    reply_got,
    acc_ref,
    own_ref,
    sent,
    landing,
    ssent,
    slanding,
    sown_ref,
    result_ref,
    value_sems,
    gate_sem,
    tile_sems,
    out_sems,
    log_ssems,
    log_rsems,
    pair_ssems,
    pair_rsems,
    scan_ssems,
    scan_rsems,
    swap_ssems,
    swap_rsems,
    small_ssems,
    small_rsems,
    sent_sems,
    land_sems,
    ssent_sems,
    sland_sems,
):
    tokens, channels = values_ref.shape
    heads = step_ref.shape[0]
    entries = inject_ref.shape[1]
    half = entries // 2
    cols = acc_ref.shape[1]
    chunks = channels // CHUNK
    blocks = tokens // BLOCK
    levels = totals.shape[0] - 1
    place = lax.axis_index("head")
    seat = lax.axis_index("ctx")
    side = seat % 2
    odd = side == 1
    own_rows = pl.ds(pl.multiple_of(side * half, half), half)
    other_rows = pl.ds(pl.multiple_of((1 - side) * half, half), half)

    def lanes_of(c):
        return slice(c * CHUNK, (c + 1) * CHUNK)

    def some_lanes(c):
        return pl.ds(pl.multiple_of(c * CHUNK, CHUNK), CHUNK)

    def value_copy(c):
        return pltpu.make_async_copy(
            values_hbm.at[:, lanes_of(c)], values_ref.at[:, lanes_of(c)], value_sems.at[c]
        )

    gate_copy = pltpu.make_async_copy(gate_hbm, gate_ref, gate_sem.at[0])

    def tile_copy(d):
        return pltpu.make_async_copy(
            weight_hbm.at[:, pl.ds(d * cols, cols)], tiles_ref.at[d], tile_sems.at[d]
        )

    for c in range(chunks):
        value_copy(c).start()
    gate_copy.start()
    for k in range((n + 1) // 2):
        for d in sorted({n - 1 - k, k}, reverse=True):
            tile_copy(d).start()

    def digit(s):
        return (seat // (1 << s)) % 2

    def mate(s):
        return seat + (1 << s) - (2 << s) * digit(s)

    barrier = pltpu.get_barrier_semaphore()

    def greet(device):
        pl.semaphore_signal(
            barrier, inc=1, device_id=device, device_id_type=pl.DeviceIdType.MESH
        )

    for s in range(levels + 1):
        greet({"ctx": mate(s)})

    @pl.when(place > 0)
    def _():
        greet({"head": place - 1})

    @pl.when(place < n - 1)
    def _():
        greet({"head": place + 1})

    rows, lanes = square(heads)
    rate_row = -jnp.exp(decay_ref[...])
    rate = jnp.sum(jnp.where(rows == lanes, rate_row, 0.0), axis=1, keepdims=True)
    steps = softplus(step_ref[...])
    logs = steps * rate
    i, j = square(BLOCK)
    expander_ref[...] = expander_of(heads, dim)
    later = jnp.zeros((heads, 1), F32)
    for b in reversed(range(blocks)):
        span = slice(b * BLOCK, (b + 1) * BLOCK)
        steps_ref[b] = steps[:, span]
        logs_ref[b] = logs[:, span]
        after = dot(logs[:, span], jnp.where(i > j, 1.0, 0.0), precision=EXACT) + later
        later = later + jnp.sum(logs[:, span], axis=1, keepdims=True)
        w = turn_over(jnp.exp(after) * steps[:, span])
        high = w.astype(BF16)
        low = (w - high.astype(F32)).astype(BF16)
        wide_ref[span, :] = jnp.concatenate([high, low], axis=1)
    total_logs = jnp.sum(jnp.where(rows == lanes, later, 0.0), axis=0, keepdims=True)
    total_logs = jnp.broadcast_to(total_logs, (PAD, heads))
    turned_ref[...] = turn_over(inject_ref[...].astype(F32)).astype(BF16)
    top = lax.broadcasted_iota(jnp.int32, (PAD, heads), 0) == 0

    inside = (place > 0) & (place < n - 1)

    @pl.when(inside)
    def _():
        pl.semaphore_wait(barrier, levels + 3)

    @pl.when(jnp.logical_not(inside))
    def _():
        pl.semaphore_wait(barrier, levels + 2)

    def remote(src, dst, ssem, rsem, device):
        return pltpu.make_async_remote_copy(
            src_ref=src,
            dst_ref=dst,
            send_sem=ssem,
            recv_sem=rsem,
            device_id=device,
            device_id_type=pl.DeviceIdType.MESH,
        )

    def log_copy(s):
        return remote(
            log_sent.at[s], log_got.at[s], log_ssems.at[s], log_rsems.at[s], {"ctx": mate(s)}
        )

    def pair_copy(c):
        return remote(
            mine_state.at[c, other_rows],
            pair_state.at[c],
            pair_ssems.at[c],
            pair_rsems.at[c],
            {"ctx": mate(0)},
        )

    def scan_copy(s, c):
        return remote(
            totals.at[s - 1, c],
            arrived.at[s - 1, c],
            scan_ssems.at[s - 1, c],
            scan_rsems.at[s - 1, c],
            {"ctx": mate(s)},
        )

    def swap_copy(c, where):
        return remote(
            swap_ref.at[c],
            enter_ref.at[c, where],
            swap_ssems.at[c],
            swap_rsems.at[c],
            {"ctx": mate(0)},
        )

    log_sent[0] = total_logs
    log_copy(0).start()
    before_logs = [jnp.zeros((PAD, heads), F32)]
    group_logs = [total_logs]

    def exchange_logs(s):
        log_copy(s).wait_recv()
        got, own = log_got[s], group_logs[0]
        upper = digit(s) == 1
        above = jnp.where(upper, own, got)
        if s == 0:
            pair = jnp.where(top, above, jnp.where(odd, got, own))
            pair_scale[...] = spread(jnp.exp(pair), expander_ref[...])
        else:
            both = jnp.where(top, above, before_logs[0])
            scale_ref[s - 1] = spread(jnp.exp(both), expander_ref[...])
            before_logs[0] = before_logs[0] + jnp.where(upper, got, 0.0)
        group_logs[0] = own + got
        if s < levels:
            log_sent[s + 1] = group_logs[0]
            log_copy(s + 1).start()

    def state_of(c):
        value_copy(c).wait()
        wide = dot(wide_ref[...], expander_ref[:, lanes_of(c)])
        scaled = (wide * values_ref[:, lanes_of(c)].astype(F32)).astype(BF16)
        mine_state[c] = dot(turned_ref[...], scaled).astype(BF16)
        pair_copy(c).start()

    def pair_up(c):
        pair_copy(c).wait_recv()
        mine = mine_state[c, own_rows].astype(F32)
        theirs = pair_state[c].astype(F32)
        first, second = jnp.where(odd, theirs, mine), jnp.where(odd, mine, theirs)
        totals[0, c] = (first * pair_scale[0:1, lanes_of(c)] + second).astype(BF16)
        scan_copy(1, c).start()

    for c in range(chunks):
        state_of(c)
        if c <= levels:
            exchange_logs(c)
        if c > 0:
            pair_up(c - 1)
    pair_up(chunks - 1)
    for s in range(chunks, levels + 1):
        exchange_logs(s)
    for s in range(levels + 1):
        log_copy(s).wait_send()

    def scan_step(s, c):
        scan_copy(s, c).wait_recv()
        upper = digit(s) == 1
        far = arrived[s - 1, c].astype(F32)
        near = totals[s - 1, c].astype(F32)
        first, second = jnp.where(upper, far, near), jnp.where(upper, near, far)
        total_scale = scale_ref[s - 1, 0:1, some_lanes(c)]
        totals[s, c] = (first * total_scale + second).astype(BF16)
        if s == 1:
            before = jnp.where(upper, far, 0.0)
        else:
            held = before_ref[c]
            before = jnp.where(upper, far * scale_ref[s - 1, 1:2, some_lanes(c)] + held, held)
        if s < levels:
            before_ref[c] = before
            scan_copy(s + 1, c).start()
        else:
            even_state = jnp.where(odd, pair_state[c].astype(F32), mine_state[c, own_rows].astype(F32))
            moved = before * pair_scale[1:2, some_lanes(c)] + even_state
            enter_ref[c, own_rows] = jnp.where(odd, moved, before).astype(BF16)
            swap_ref[c] = jnp.where(odd, before, moved).astype(BF16)
            swap_copy(c, own_rows).start()

    skip_ref[...] = spread(jnp.broadcast_to(gain_in_ref[...], (PAD, heads)), expander_ref[...])

    def sample_local():
        samples, length = svalues_ref.shape[:2]
        slocal_ref[...] = jnp.zeros_like(slocal_ref)
        sgain_ref[...] = jnp.zeros_like(sgain_ref)
        picked_ref[...] = jnp.zeros_like(picked_ref)
        u, s = square(length)
        own = lax.broadcasted_iota(jnp.int32, (heads, channels), 1) // dim == (
            lax.broadcasted_iota(jnp.int32, (heads, channels), 0)
        )
        at = lax.broadcasted_iota(jnp.int32, (1, length), 1)
        for k in range(samples):
            last = length_ref[k] - 1
            hot = jnp.where(
                lax.broadcasted_iota(jnp.int32, (PAD, length), 1) == last, 1.0, 0.0
            ).astype(BF16)
            tall = softplus(sstep_ref[k])
            tall_logs = tall * rate_row
            flip = ((0,), (0,))
            gap = dot(tall_logs, jnp.where((u > s) & (u <= last), 1.0, 0.0), flip, EXACT)
            running = dot(tall_logs, jnp.where(u <= last, 1.0, 0.0), flip, EXACT)[:, 0:1]
            wide_steps = dot(tall, jnp.where(u == s, 1.0, 0.0), flip, EXACT)
            row = dot(hot, sread_ref[k])
            score = dot(row.astype(BF16), sinject_ref[k], ((1,), (1,)))[0:1]
            mixing = jnp.where(at <= last, score * jnp.exp(gap) * wide_steps, 0.0).astype(BF16)
            values = svalues_ref[k]
            local = jnp.sum(jnp.where(own, dot(mixing, values), 0.0), axis=0, keepdims=True)
            decay = jnp.sum(jnp.where(own, jnp.exp(running), 0.0), axis=0, keepdims=True)
            value = dot(hot, values)[0:1]
            opened = silu(dot(hot, sgate_ref[k])[0:1])
            slocal_ref[k : k + 1, :] = (local + skip_ref[0:1, :] * value) * opened
            sgain_ref[k : k + 1, :] = decay * opened
            picked_ref[k : k + 1, :] = row[0:1].astype(BF16)

    state_ref[...] = jnp.zeros_like(state_ref)
    offset_ref[...] = jnp.zeros_like(offset_ref)
    gate_copy.wait()

    def block_local(b):
        span = pl.ds(pl.multiple_of(b * BLOCK, BLOCK), BLOCK)
        steps, logs = steps_ref[b], logs_ref[b]
        i, j = square(BLOCK)
        lower = jnp.where(i >= j, 1.0, 0.0)
        running = dot(logs, lower, ((1,), (1,)), EXACT)
        running_t = turn_over(running)
        after = turn_over(dot(logs, jnp.where(i > j, 1.0, 0.0), precision=EXACT))
        turned = turn_over(steps)
        expander = expander_ref[...]
        inject = inject_ref[span, :]
        readout = read_ref[span, :]
        scores = jnp.where(i >= j, dot(readout, inject, ((1,), (1,))), 0.0)
        per = LANES // dim
        lane = lax.broadcasted_iota(jnp.int32, (BLOCK, LANES), 1)
        for k in range(heads // per):
            cut = slice(k * LANES, (k + 1) * LANES)
            pair = values_ref[span, cut]
            mixes, parts = [], []
            for q in range(per):
                h = k * per + q
                gap = jnp.minimum(running_t[:, h : h + 1] - running[h : h + 1, :], 0.0)
                mixes.append((scores * jnp.exp(gap) * steps[h : h + 1, :]).astype(BF16))
                parts.append(jnp.where(lane // dim == q, pair, jnp.zeros_like(pair)))
            part_ref[:, cut] = dot(jnp.concatenate(mixes, axis=1), jnp.concatenate(parts, axis=0))
        decay = spread(jnp.exp(running_t), expander)
        values = values_ref[span, :].astype(F32)
        opened = silu(gate_ref[span, :].astype(F32))
        total = part_ref[...] + skip_ref[0:1, :] * values
        total = total + dot(readout, state_ref[...].astype(BF16)) * decay
        local_ref[span, :] = (total * opened).astype(BF16)
        offset = offset_ref[0:1, :]
        gain_ref[span, :] = (opened * spread(jnp.exp(running_t + offset), expander)).astype(BF16)
        offset_ref[0:1, :] = offset + running_t[BLOCK - 1 : BLOCK, :]
        scaled = (spread(jnp.exp(after) * turned, expander) * values).astype(BF16)
        state_ref[...] = state_ref[...] * decay[BLOCK - 1 : BLOCK, :] + dot(
            inject, scaled, ((0,), (0,))
        )

    last_round = chunks + 2 * (levels - 1)

    def small_copy(q, src, dst):
        return remote(src, dst, small_ssems.at[q], small_rsems.at[q], {"ctx": mate(0)})

    picked_copy = small_copy(0, picked_ref, picked_got)
    reply_copy = small_copy(1, reply_ref, reply_got)

    def round_of(t, carry):
        @pl.when(t < blocks)
        def _():
            block_local(t)

        @pl.when(t == blocks)
        def _():
            sample_local()
            picked_copy.start()

        for s in range(1, levels + 1):
            c = t - 2 * (s - 1)

            @pl.when((c >= 0) & (c < chunks))
            def _():
                scan_step(s, c)

        return carry

    lax.fori_loop(0, max(last_round, blocks + 1), round_of, 0)
    for c in range(chunks):
        swap_copy(c, other_rows).wait_recv()
    for d in range(n):
        tile_copy(d).wait()

    def share(rows, d):
        return dot(normed_ref[rows, :], tiles_ref[d])

    def hop_up(d, b):
        return remote(
            sent.at[d, b],
            landing.at[d + 1, b],
            sent_sems.at[d, b],
            land_sems.at[d + 1, b],
            {"head": place + 1},
        )

    def hop_down(d, b):
        return remote(
            sent.at[d, b],
            landing.at[d, b],
            sent_sems.at[d, b],
            land_sems.at[d, b],
            {"head": place - 1},
        )

    def shop_up(d):
        return remote(
            ssent.at[d],
            slanding.at[d + 1],
            ssent_sems.at[d],
            sland_sems.at[d + 1],
            {"head": place + 1},
        )

    def shop_down(d):
        return remote(
            ssent.at[d], slanding.at[d], ssent_sems.at[d], sland_sems.at[d], {"head": place - 1}
        )

    def rows_of(b):
        return pl.ds(pl.multiple_of(b * BLOCK, BLOCK), BLOCK)

    def pass_on(d, b, slot, move, fed):
        acc_ref[...] = share(rows_of(b), d)

        @pl.when(fed)
        def _():
            move(d, b).wait_recv()
            acc_ref[...] = acc_ref[...] + landing[slot, b].astype(F32)

        sent[d, b] = acc_ref[...].astype(BF16)
        move(d, b).start()

    def finish_block(b):
        span = rows_of(b)
        readout = read_ref[span, :]
        pieces = []
        for c in range(chunks):
            arrival = dot(readout, enter_ref[c])
            piece = local_ref[span, lanes_of(c)].astype(F32)
            pieces.append(piece + arrival * gain_ref[span, lanes_of(c)].astype(F32))
        normed_ref[span, :] = finish_rows(jnp.concatenate(pieces, axis=1), norm_ref[...])

    def send_turn(k, b):
        up, down = n - 1 - k, k

        @pl.when(place < up)
        def _():
            pass_on(up, b, up + 1, hop_up, place > 0)

        @pl.when(place > down)
        def _():
            pass_on(down, b, down, hop_down, place < n - 1)

    def first_turn(b, carry):
        finish_block(b)
        send_turn(0, b)
        return carry

    lax.fori_loop(0, blocks, first_turn, 0)

    def half_of(ref):
        return jnp.where(odd, ref[:, half:].astype(F32), ref[:, :half].astype(F32)).astype(BF16)

    picked_copy.wait_recv()
    asked, answered = half_of(picked_got), half_of(picked_ref)
    arrivals = []
    for c in range(chunks):
        reply_ref[:, lanes_of(c)] = dot(asked, totals[levels, c])
        arrivals.append(dot(answered, totals[levels, c]))
    reply_copy.start()
    reply_copy.wait_recv()
    arrival = jnp.concatenate(arrivals, axis=1) + reply_got[...]
    padded = slocal_ref.shape[0]
    srows = pl.ds(tokens, padded)
    normed_ref[srows, :] = finish_rows(slocal_ref[...] + arrival * sgain_ref[...], norm_ref[...])

    def spass_on(d, slot, move, fed):
        sown_ref[...] = share(srows, d)

        @pl.when(fed)
        def _():
            move(d).wait_recv()
            sown_ref[...] = sown_ref[...] + slanding[slot].astype(F32)

        ssent[d] = sown_ref[...].astype(BF16)
        move(d).start()

    def sample_turn(k, carry):
        up, down = n - 1 - k, k

        @pl.when(place < up)
        def _():
            spass_on(up, up + 1, shop_up, place > 0)

        @pl.when(place > down)
        def _():
            spass_on(down, down, shop_down, place < n - 1)

        return carry

    lax.fori_loop(0, n - 1, sample_turn, 0)
    sown_ref[...] = share(srows, place)

    def later_turn(t, carry):
        send_turn(t // blocks, t % blocks)
        return carry

    lax.fori_loop(blocks, (n - 1) * blocks, later_turn, 0)

    def own(b, carry):
        own_ref[b] = share(rows_of(b), place)
        return carry

    lax.fori_loop(0, blocks, own, 0)

    @pl.when(place < n - 1)
    def _():
        shop_down(place).wait_recv()
        sown_ref[...] = sown_ref[...] + slanding[place].astype(F32)

    @pl.when(place > 0)
    def _():
        shop_up(place).wait_recv()
        sown_ref[...] = sown_ref[...] + slanding[place + 1].astype(F32)

    sout_ref[...] = sown_ref[...].astype(BF16)

    def out_copy(b):
        return pltpu.make_async_copy(
            result_ref.at[b], out_hbm.at[pl.ds(pl.multiple_of(b * BLOCK, BLOCK), BLOCK)], out_sems.at[b]
        )

    def gather(b, carry):
        @pl.when(place < n - 1)
        def _():
            hop_down(place, b).wait_recv()
            own_ref[b] = own_ref[b] + landing[place, b].astype(F32)

        @pl.when(place > 0)
        def _():
            hop_up(place, b).wait_recv()
            own_ref[b] = own_ref[b] + landing[place + 1, b].astype(F32)

        result_ref[b] = own_ref[b].astype(BF16)
        out_copy(b).start()
        return carry

    lax.fori_loop(0, blocks, gather, 0)

    def drain(t, carry):
        d, b = t // blocks, t % blocks

        @pl.when(d > place)
        def _():
            hop_up(d, b).wait_send()

        @pl.when(d < place)
        def _():
            hop_down(d, b).wait_send()

        return carry

    lax.fori_loop(0, n * blocks, drain, 0)

    def sdrain(d, carry):
        @pl.when(d > place)
        def _():
            shop_up(d).wait_send()

        @pl.when(d < place)
        def _():
            shop_down(d).wait_send()

        return carry

    lax.fori_loop(0, n, sdrain, 0)
    for c in range(chunks):
        pair_copy(c).wait_send()
        swap_copy(c, own_rows).wait_send()
        for s in range(1, levels + 1):
            scan_copy(s, c).wait_send()
    picked_copy.wait_send()
    reply_copy.wait_send()
    for b in range(blocks):
        out_copy(b).wait()


def per_device(
    prompt_values,
    prompt_gate,
    prompt_inject,
    prompt_read,
    prompt_step,
    decay_log,
    skip_gain,
    norm_weight,
    out_weight,
    sample_values,
    sample_gate,
    sample_inject,
    sample_read,
    sample_step,
    sample_length,
):
    n, peers = lax.axis_size("head"), lax.axis_size("ctx")
    levels = peers.bit_length() - 2
    tokens, channels = prompt_values.shape
    heads = prompt_step.shape[0]
    dim = channels // heads
    entries = prompt_inject.shape[2]
    half = entries // 2
    samples, length = sample_values.shape[:2]
    padded = -(-samples // (2 * PAD)) * 2 * PAD
    cols = out_weight.shape[1] // n
    blocks, chunks = tokens // BLOCK, channels // CHUNK
    vmem = pl.BlockSpec(memory_space=pltpu.VMEM)
    hbm = pl.BlockSpec(memory_space=pl.ANY)
    dma = pltpu.SemaphoreType.DMA
    shape = jax.ShapeDtypeStruct
    V = pltpu.VMEM
    mixed, smixed = pl.pallas_call(
        functools.partial(layer_kernel, dim, n, peers),
        out_shape=(shape((tokens, cols), BF16), shape((padded, cols), BF16)),
        in_specs=[
            pl.BlockSpec(memory_space=pltpu.SMEM),
            hbm,
            hbm,
            vmem,
            vmem,
            vmem,
            vmem,
            vmem,
            vmem,
            hbm,
            vmem,
            vmem,
            vmem,
            vmem,
            vmem,
        ],
        out_specs=(hbm, vmem),
        scratch_shapes=[
            V((tokens, channels), BF16),
            V((tokens, channels), BF16),
            V((n, channels, cols), BF16),
            V((blocks, heads, BLOCK), F32),
            V((blocks, heads, BLOCK), F32),
            V((tokens, 2 * heads), BF16),
            V((2 * heads, channels), BF16),
            V((entries, tokens), BF16),
            V((PAD, channels), F32),
            V((chunks, entries, CHUNK), BF16),
            V((chunks, half, CHUNK), BF16),
            V((levels + 1, chunks, half, CHUNK), BF16),
            V((levels, chunks, half, CHUNK), BF16),
            V((chunks, half, CHUNK), F32),
            V((chunks, half, CHUNK), BF16),
            V((chunks, entries, CHUNK), BF16),
            V((levels + 1, PAD, heads), F32),
            V((levels + 1, PAD, heads), F32),
            V((PAD, channels), F32),
            V((levels, PAD, channels), F32),
            V((entries, channels), F32),
            V((PAD, heads), F32),
            V((BLOCK, channels), F32),
            V((tokens, channels), BF16),
            V((tokens, channels), BF16),
            V((tokens + padded, channels), BF16),
            V((padded, channels), F32),
            V((padded, channels), F32),
            V((padded, entries), BF16),
            V((padded, entries), BF16),
            V((padded, channels), F32),
            V((padded, channels), F32),
            V((BLOCK, cols), F32),
            V((blocks, BLOCK, cols), F32),
            V((n, blocks, BLOCK, cols), BF16),
            V((n + 1, blocks, BLOCK, cols), BF16),
            V((n, padded, cols), BF16),
            V((n + 1, padded, cols), BF16),
            V((padded, cols), F32),
            V((blocks, BLOCK, cols), BF16),
            dma((chunks,)),
            dma((1,)),
            dma((n,)),
            dma((blocks,)),
            dma((levels + 1,)),
            dma((levels + 1,)),
            dma((chunks,)),
            dma((chunks,)),
            dma((levels, chunks)),
            dma((levels, chunks)),
            dma((chunks,)),
            dma((chunks,)),
            dma((2,)),
            dma((2,)),
            dma((n, blocks)),
            dma((n + 1, blocks)),
            dma((n,)),
            dma((n + 1,)),
        ],
        compiler_params=pltpu.CompilerParams(
            collective_id=0, has_side_effects=True, vmem_limit_bytes=VMEM_LIMIT
        ),
    )(
        sample_length,
        prompt_values,
        prompt_gate,
        prompt_inject.reshape(tokens, entries),
        prompt_read.reshape(tokens, entries),
        prompt_step,
        decay_log[None],
        skip_gain[None],
        norm_weight[None],
        out_weight,
        sample_values,
        sample_gate,
        sample_inject.reshape(samples, length, entries),
        sample_read.reshape(samples, length, entries),
        sample_step.transpose(1, 2, 0),
    )
    return mixed.T, smixed[:samples].T


def solution(mesh):
    in_specs = (
        P("ctx", "head"),
        P("ctx", "head"),
        P("ctx", "head", None),
        P("ctx", "head", None),
        P("head", "ctx"),
        P("head"),
        P("head"),
        P("head"),
        P("head", None),
        P("ctx", None, "head"),
        P("ctx", None, "head"),
        P("ctx", None, "head", None),
        P("ctx", None, "head", None),
        P("head", "ctx", None),
        P("ctx"),
    )
    out_specs = (P("head", "ctx"), P("head", "ctx"))
    return jax.shard_map(
        per_device, mesh=mesh, in_specs=in_specs, out_specs=out_specs, check_vma=False
    )
```

```python
import functools

import jax
import jax.numpy as jnp
from jax import lax
from jax.experimental import pallas as pl
from jax.experimental.pallas import tpu as pltpu
from jax.sharding import PartitionSpec as P

BLOCK = 128
LANES = 128
PAD = 8
F32 = jnp.float32
BF16 = jnp.bfloat16
EXACT = lax.Precision.HIGHEST
VMEM_LIMIT = 60 * 1024 * 1024


def dot(a, b, dims=((1,), (0,)), precision=None):
    return lax.dot_general(a, b, (dims, ((), ())), precision=precision, preferred_element_type=F32)


def softplus(v):
    return jnp.maximum(v, 0.0) + jnp.log1p(jnp.exp(-jnp.abs(v)))


def silu(v):
    return v / (1.0 + jnp.exp(-v))


def spread(w, expander):
    high = w.astype(BF16)
    low = (w - high.astype(F32)).astype(BF16)
    return dot(jnp.concatenate([high, low], axis=1), expander)


def expander_of(heads, dim):
    row = lax.broadcasted_iota(jnp.int32, (2 * heads, heads * dim), 0)
    lane = lax.broadcasted_iota(jnp.int32, (2 * heads, heads * dim), 1)
    head = lane // dim
    return jnp.where((row == head) | (row == head + heads), 1.0, 0.0).astype(BF16)


def square(n):
    return (
        lax.broadcasted_iota(jnp.int32, (n, n), 0),
        lax.broadcasted_iota(jnp.int32, (n, n), 1),
    )


def finish_rows(total, weight):
    mean = jnp.mean(total * total, axis=1, keepdims=True)
    return (total * lax.rsqrt(mean + 1e-05) * weight).astype(BF16)


CHUNK = 2 * LANES
LAG = 3


def turn_over(w):
    return jnp.transpose(w, (1, 0))


def layer_kernel(
    dim,
    n,
    peers,
    length_ref,
    values_hbm,
    gate_hbm,
    inject_ref,
    read_ref,
    step_ref,
    decay_ref,
    gain_in_ref,
    norm_ref,
    weight_hbm,
    svalues_ref,
    sgate_ref,
    sinject_ref,
    sread_ref,
    sstep_ref,
    out_hbm,
    sout_ref,
    values_ref,
    gate_ref,
    tiles_ref,
    steps_ref,
    logs_ref,
    wide_ref,
    expander_ref,
    turned_ref,
    skip_ref,
    mine_state,
    pair_state,
    totals,
    arrived,
    before_ref,
    swap_ref,
    enter_ref,
    log_sent,
    log_got,
    before_logs,
    pair_scale,
    scale_ref,
    state_ref,
    offset_ref,
    part_ref,
    local_ref,
    gain_ref,
    normed_ref,
    slocal_ref,
    sgain_ref,
    picked_ref,
    picked_got,
    reply_ref,
    reply_got,
    acc_ref,
    own_ref,
    sent,
    landing,
    ssent,
    slanding,
    sown_ref,
    result_ref,
    value_sems,
    gate_sem,
    tile_sems,
    out_sems,
    log_ssems,
    log_rsems,
    pair_ssems,
    pair_rsems,
    scan_ssems,
    scan_rsems,
    swap_ssems,
    swap_rsems,
    small_ssems,
    small_rsems,
    sent_sems,
    land_sems,
    ssent_sems,
    sland_sems,
):
    tokens, channels = values_ref.shape
    heads = step_ref.shape[0]
    entries = inject_ref.shape[1]
    half = entries // 2
    cols = acc_ref.shape[1]
    chunks = channels // CHUNK
    blocks = tokens // BLOCK
    levels = totals.shape[0] - 1
    place = lax.axis_index("head")
    seat = lax.axis_index("ctx")
    side = seat % 2
    odd = side == 1
    own_rows = pl.ds(pl.multiple_of(side * half, half), half)
    other_rows = pl.ds(pl.multiple_of((1 - side) * half, half), half)

    def lanes_of(c):
        return slice(c * CHUNK, (c + 1) * CHUNK)

    def some_lanes(c):
        return pl.ds(pl.multiple_of(c * CHUNK, CHUNK), CHUNK)

    def value_copy(c):
        return pltpu.make_async_copy(
            values_hbm.at[:, lanes_of(c)], values_ref.at[:, lanes_of(c)], value_sems.at[c]
        )

    gate_copy = pltpu.make_async_copy(gate_hbm, gate_ref, gate_sem.at[0])

    def tile_copy(d):
        return pltpu.make_async_copy(
            weight_hbm.at[:, pl.ds(d * cols, cols)], tiles_ref.at[d], tile_sems.at[d]
        )

    for c in range(chunks):
        value_copy(c).start()
    gate_copy.start()
    for k in range((n + 1) // 2):
        for d in sorted({n - 1 - k, k}, reverse=True):
            tile_copy(d).start()

    def digit(s):
        return (seat // (1 << s)) % 2

    def mate(s):
        return seat + (1 << s) - (2 << s) * digit(s)

    barrier = pltpu.get_barrier_semaphore()

    def greet(device):
        pl.semaphore_signal(
            barrier, inc=1, device_id=device, device_id_type=pl.DeviceIdType.MESH
        )

    for s in range(levels + 1):
        greet({"ctx": mate(s)})

    @pl.when(place > 0)
    def _():
        greet({"head": place - 1})

    @pl.when(place < n - 1)
    def _():
        greet({"head": place + 1})

    rows, lanes = square(heads)
    rate_row = -jnp.exp(decay_ref[...])
    rate = jnp.sum(jnp.where(rows == lanes, rate_row, 0.0), axis=1, keepdims=True)
    steps = softplus(step_ref[...])
    logs = steps * rate
    i, j = square(BLOCK)
    expander_ref[...] = expander_of(heads, dim)
    later = jnp.zeros((heads, 1), F32)
    for b in reversed(range(blocks)):
        span = slice(b * BLOCK, (b + 1) * BLOCK)
        steps_ref[b] = steps[:, span]
        logs_ref[b] = logs[:, span]
        after = dot(logs[:, span], jnp.where(i > j, 1.0, 0.0), precision=EXACT) + later
        later = later + jnp.sum(logs[:, span], axis=1, keepdims=True)
        w = turn_over(jnp.exp(after) * steps[:, span])
        high = w.astype(BF16)
        low = (w - high.astype(F32)).astype(BF16)
        wide_ref[span, :] = jnp.concatenate([high, low], axis=1)
    total_logs = jnp.sum(jnp.where(rows == lanes, later, 0.0), axis=0, keepdims=True)
    total_logs = jnp.broadcast_to(total_logs, (PAD, heads))
    turned_ref[...] = turn_over(inject_ref[...].astype(F32)).astype(BF16)
    top = lax.broadcasted_iota(jnp.int32, (PAD, heads), 0) == 0

    inside = (place > 0) & (place < n - 1)
    log_sent[0] = total_logs
    before_logs[...] = jnp.zeros_like(before_logs)

    def state_of(c):
        value_copy(c).wait()
        wide = dot(wide_ref[...], expander_ref[:, lanes_of(c)])
        scaled = (wide * values_ref[:, lanes_of(c)].astype(F32)).astype(BF16)
        mine_state[c] = dot(turned_ref[...], scaled).astype(BF16)

    state_of(0)

    @pl.when(inside)
    def _():
        pl.semaphore_wait(barrier, levels + 3)

    @pl.when(jnp.logical_not(inside))
    def _():
        pl.semaphore_wait(barrier, levels + 2)

    def remote(src, dst, ssem, rsem, device):
        return pltpu.make_async_remote_copy(
            src_ref=src,
            dst_ref=dst,
            send_sem=ssem,
            recv_sem=rsem,
            device_id=device,
            device_id_type=pl.DeviceIdType.MESH,
        )

    def log_copy(s):
        return remote(
            log_sent.at[s], log_got.at[s], log_ssems.at[s], log_rsems.at[s], {"ctx": mate(s)}
        )

    def pair_copy(c):
        return remote(
            mine_state.at[c, other_rows],
            pair_state.at[c],
            pair_ssems.at[c],
            pair_rsems.at[c],
            {"ctx": mate(0)},
        )

    def scan_copy(s, c):
        return remote(
            totals.at[s - 1, c],
            arrived.at[s - 1, c],
            scan_ssems.at[s - 1, c],
            scan_rsems.at[s - 1, c],
            {"ctx": mate(s)},
        )

    def swap_copy(c, where):
        return remote(
            swap_ref.at[c],
            enter_ref.at[c, where],
            swap_ssems.at[c],
            swap_rsems.at[c],
            {"ctx": mate(0)},
        )

    log_copy(0).start()

    def exchange_logs(s):
        log_copy(s).wait_recv()
        got, own = log_got[s], log_sent[s]
        upper = digit(s) == 1
        above = jnp.where(upper, own, got)
        if s == 0:
            pair = jnp.where(top, above, jnp.where(odd, got, own))
            pair_scale[...] = spread(jnp.exp(pair), expander_ref[...])
        else:
            held = before_logs[...]
            scale_ref[s - 1] = spread(jnp.exp(jnp.where(top, above, held)), expander_ref[...])
            before_logs[...] = held + jnp.where(upper, got, 0.0)
        if s < levels:
            log_sent[s + 1] = own + got
            log_copy(s + 1).start()

    def pair_up(c):
        pair_copy(c).wait_recv()
        mine = mine_state[c, own_rows].astype(F32)
        theirs = pair_state[c].astype(F32)
        first, second = jnp.where(odd, theirs, mine), jnp.where(odd, mine, theirs)
        totals[0, c] = (first * pair_scale[0:1, lanes_of(c)] + second).astype(BF16)
        scan_copy(1, c).start()

    pair_copy(0).start()
    for c in range(1, chunks):
        state_of(c)
        pair_copy(c).start()
        if c == 2:
            exchange_logs(0)
        if c > 2:
            pair_up(c - 3)
    for c in range(chunks - 3, chunks):
        pair_up(c)

    def scan_step(s, c):
        scan_copy(s, c).wait_recv()
        upper = digit(s) == 1
        far = arrived[s - 1, c].astype(F32)
        near = totals[s - 1, c].astype(F32)
        first, second = jnp.where(upper, far, near), jnp.where(upper, near, far)
        total_scale = scale_ref[s - 1, 0:1, some_lanes(c)]
        totals[s, c] = (first * total_scale + second).astype(BF16)
        if s == 1:
            before = jnp.where(upper, far, 0.0)
        else:
            held = before_ref[c]
            before = jnp.where(upper, far * scale_ref[s - 1, 1:2, some_lanes(c)] + held, held)
        if s < levels:
            before_ref[c] = before
            scan_copy(s + 1, c).start()
        else:
            even_state = jnp.where(odd, pair_state[c].astype(F32), mine_state[c, own_rows].astype(F32))
            moved = before * pair_scale[1:2, some_lanes(c)] + even_state
            enter_ref[c, own_rows] = jnp.where(odd, moved, before).astype(BF16)
            swap_ref[c] = jnp.where(odd, before, moved).astype(BF16)
            swap_copy(c, own_rows).start()

    skip_ref[...] = spread(jnp.broadcast_to(gain_in_ref[...], (PAD, heads)), expander_ref[...])

    def sample_local():
        samples, length = svalues_ref.shape[:2]
        slocal_ref[...] = jnp.zeros_like(slocal_ref)
        sgain_ref[...] = jnp.zeros_like(sgain_ref)
        picked_ref[...] = jnp.zeros_like(picked_ref)
        u, s = square(length)
        own = lax.broadcasted_iota(jnp.int32, (heads, channels), 1) // dim == (
            lax.broadcasted_iota(jnp.int32, (heads, channels), 0)
        )
        at = lax.broadcasted_iota(jnp.int32, (1, length), 1)
        for k in range(samples):
            last = length_ref[k] - 1
            hot = jnp.where(
                lax.broadcasted_iota(jnp.int32, (PAD, length), 1) == last, 1.0, 0.0
            ).astype(BF16)
            tall = softplus(sstep_ref[k])
            tall_logs = tall * rate_row
            flip = ((0,), (0,))
            gap = dot(tall_logs, jnp.where((u > s) & (u <= last), 1.0, 0.0), flip, EXACT)
            running = dot(tall_logs, jnp.where(u <= last, 1.0, 0.0), flip, EXACT)[:, 0:1]
            wide_steps = dot(tall, jnp.where(u == s, 1.0, 0.0), flip, EXACT)
            row = dot(hot, sread_ref[k])
            score = dot(row.astype(BF16), sinject_ref[k], ((1,), (1,)))[0:1]
            mixing = jnp.where(at <= last, score * jnp.exp(gap) * wide_steps, 0.0).astype(BF16)
            values = svalues_ref[k]
            local = jnp.sum(jnp.where(own, dot(mixing, values), 0.0), axis=0, keepdims=True)
            decay = jnp.sum(jnp.where(own, jnp.exp(running), 0.0), axis=0, keepdims=True)
            value = dot(hot, values)[0:1]
            opened = silu(dot(hot, sgate_ref[k])[0:1])
            slocal_ref[k : k + 1, :] = (local + skip_ref[0:1, :] * value) * opened
            sgain_ref[k : k + 1, :] = decay * opened
            picked_ref[k : k + 1, :] = row[0:1].astype(BF16)

    state_ref[...] = jnp.zeros_like(state_ref)
    offset_ref[...] = jnp.zeros_like(offset_ref)
    gate_copy.wait()

    def block_local(b, hook):
        span = pl.ds(pl.multiple_of(b * BLOCK, BLOCK), BLOCK)
        steps, logs = steps_ref[b], logs_ref[b]
        i, j = square(BLOCK)
        lower = jnp.where(i >= j, 1.0, 0.0)
        running = dot(logs, lower, ((1,), (1,)), EXACT)
        running_t = turn_over(running)
        after = turn_over(dot(logs, jnp.where(i > j, 1.0, 0.0), precision=EXACT))
        turned = turn_over(steps)
        expander = expander_ref[...]
        inject = inject_ref[span, :]
        readout = read_ref[span, :]
        scores = jnp.where(i >= j, dot(readout, inject, ((1,), (1,))), 0.0)
        per = LANES // dim
        lane = lax.broadcasted_iota(jnp.int32, (BLOCK, LANES), 1)
        for k in range(heads // per):
            cut = slice(k * LANES, (k + 1) * LANES)
            pair = values_ref[span, cut]
            mixes, parts = [], []
            for q in range(per):
                h = k * per + q
                gap = jnp.minimum(running_t[:, h : h + 1] - running[h : h + 1, :], 0.0)
                mixes.append((scores * jnp.exp(gap) * steps[h : h + 1, :]).astype(BF16))
                parts.append(jnp.where(lane // dim == q, pair, jnp.zeros_like(pair)))
            part_ref[:, cut] = dot(jnp.concatenate(mixes, axis=1), jnp.concatenate(parts, axis=0))
            if 2 * (k + 1) == heads // per:
                hook(2 * b)
        decay = spread(jnp.exp(running_t), expander)
        values = values_ref[span, :].astype(F32)
        opened = silu(gate_ref[span, :].astype(F32))
        total = part_ref[...] + skip_ref[0:1, :] * values
        total = total + dot(readout, state_ref[...].astype(BF16)) * decay
        local_ref[span, :] = (total * opened).astype(BF16)
        offset = offset_ref[0:1, :]
        gain_ref[span, :] = (opened * spread(jnp.exp(running_t + offset), expander)).astype(BF16)
        offset_ref[0:1, :] = offset + running_t[BLOCK - 1 : BLOCK, :]
        scaled = (spread(jnp.exp(after) * turned, expander) * values).astype(BF16)
        state_ref[...] = state_ref[...] * decay[BLOCK - 1 : BLOCK, :] + dot(
            inject, scaled, ((0,), (0,))
        )
        hook(2 * b + 1)

    def hook(g):
        for s in range(1, levels + 1):

            @pl.when(g == s - 1)
            def _():
                exchange_logs(s)

        for s in range(1, levels + 1):
            c = g - LAG * (s - 1)

            @pl.when((c >= 0) & (c < chunks))
            def _():
                scan_step(s, c)

    def small_copy(q, src, dst):
        return remote(src, dst, small_ssems.at[q], small_rsems.at[q], {"ctx": mate(0)})

    picked_copy = small_copy(0, picked_ref, picked_got)
    reply_copy = small_copy(1, reply_ref, reply_got)

    def round_of(t, carry):
        block_local(t, hook)
        return carry

    def late_round(g, carry):
        hook(g)
        return carry

    lax.fori_loop(0, blocks, round_of, 0)
    sample_local()
    picked_copy.start()
    lax.fori_loop(2 * blocks, max(chunks + LAG * (levels - 1), 2 * blocks), late_round, 0)
    for c in range(chunks):
        swap_copy(c, other_rows).wait_recv()
    for d in range(n):
        tile_copy(d).wait()

    def share(rows, d):
        return dot(normed_ref[rows, :], tiles_ref[d])

    def hop_up(d, b):
        return remote(
            sent.at[d, b],
            landing.at[d + 1, b],
            sent_sems.at[d, b],
            land_sems.at[d + 1, b],
            {"head": place + 1},
        )

    def hop_down(d, b):
        return remote(
            sent.at[d, b],
            landing.at[d, b],
            sent_sems.at[d, b],
            land_sems.at[d, b],
            {"head": place - 1},
        )

    def shop_up(d):
        return remote(
            ssent.at[d],
            slanding.at[d + 1],
            ssent_sems.at[d],
            sland_sems.at[d + 1],
            {"head": place + 1},
        )

    def shop_down(d):
        return remote(
            ssent.at[d], slanding.at[d], ssent_sems.at[d], sland_sems.at[d], {"head": place - 1}
        )

    def rows_of(b):
        return pl.ds(pl.multiple_of(b * BLOCK, BLOCK), BLOCK)

    def pass_on(d, b, slot, move, fed):
        acc_ref[...] = share(rows_of(b), d)

        @pl.when(fed)
        def _():
            move(d, b).wait_recv()
            acc_ref[...] = acc_ref[...] + landing[slot, b].astype(F32)

        sent[d, b] = acc_ref[...].astype(BF16)
        move(d, b).start()

    def finish_block(b):
        span = rows_of(b)
        readout = read_ref[span, :]
        pieces = []
        for c in range(chunks):
            arrival = dot(readout, enter_ref[c])
            piece = local_ref[span, lanes_of(c)].astype(F32)
            pieces.append(piece + arrival * gain_ref[span, lanes_of(c)].astype(F32))
        normed_ref[span, :] = finish_rows(jnp.concatenate(pieces, axis=1), norm_ref[...])

    def half_of(ref):
        return jnp.where(odd, ref[:, half:].astype(F32), ref[:, :half].astype(F32)).astype(BF16)

    padded = slocal_ref.shape[0]
    srows = pl.ds(tokens, padded)

    def answer():
        picked_copy.wait_recv()
        asked = half_of(picked_got)
        for c in range(chunks):
            reply_ref[:, lanes_of(c)] = dot(asked, totals[levels, c])
        reply_copy.start()

    def finish_samples():
        reply_copy.wait_recv()
        answered = half_of(picked_ref)
        arrivals = [dot(answered, totals[levels, c]) for c in range(chunks)]
        arrival = jnp.concatenate(arrivals, axis=1) + reply_got[...]
        total = slocal_ref[...] + arrival * sgain_ref[...]
        normed_ref[srows, :] = finish_rows(total, norm_ref[...])

    def spass_on(d, slot, move, fed):
        sown_ref[...] = share(srows, d)

        @pl.when(fed)
        def _():
            move(d).wait_recv()
            sown_ref[...] = sown_ref[...] + slanding[slot].astype(F32)

        ssent[d] = sown_ref[...].astype(BF16)
        move(d).start()

    def step(t, carry):
        @pl.when(t < blocks)
        def _():
            finish_block(t)

        @pl.when(t == min(1, blocks - 1))
        def _():
            answer()

        @pl.when(t == blocks - 1)
        def _():
            finish_samples()

        rising, falling = t - place, t - (n - 1 - place)
        up, down = n - 1 - rising // blocks, falling // blocks

        @pl.when((rising >= 0) & (up > place))
        def _():
            pass_on(up, rising % blocks, up + 1, hop_up, place > 0)

        @pl.when((falling >= 0) & (down < place))
        def _():
            pass_on(down, falling % blocks, down, hop_down, place < n - 1)

        srising, sfalling = rising - (blocks - 1), falling - (blocks - 1)
        sup, sdown = n - 1 - srising, sfalling

        @pl.when((srising >= 0) & (sup > place))
        def _():
            spass_on(sup, sup + 1, shop_up, place > 0)

        @pl.when((sfalling >= 0) & (sdown < place))
        def _():
            spass_on(sdown, sdown, shop_down, place < n - 1)

        return carry

    lax.fori_loop(0, (n - 1) * max(blocks, 2), step, 0)
    sown_ref[...] = share(srows, place)

    def own(b, carry):
        own_ref[b] = share(rows_of(b), place)
        return carry

    lax.fori_loop(0, blocks, own, 0)

    @pl.when(place < n - 1)
    def _():
        shop_down(place).wait_recv()
        sown_ref[...] = sown_ref[...] + slanding[place].astype(F32)

    @pl.when(place > 0)
    def _():
        shop_up(place).wait_recv()
        sown_ref[...] = sown_ref[...] + slanding[place + 1].astype(F32)

    sout_ref[...] = sown_ref[0 : sout_ref.shape[0], :].astype(BF16)

    def out_copy(b):
        return pltpu.make_async_copy(
            result_ref.at[b],
            out_hbm.at[:, pl.ds(pl.multiple_of(b * BLOCK, BLOCK), BLOCK)],
            out_sems.at[b],
        )

    def gather(b, carry):
        @pl.when(place < n - 1)
        def _():
            hop_down(place, b).wait_recv()
            own_ref[b] = own_ref[b] + landing[place, b].astype(F32)

        @pl.when(place > 0)
        def _():
            hop_up(place, b).wait_recv()
            own_ref[b] = own_ref[b] + landing[place + 1, b].astype(F32)

        result_ref[b] = turn_over(own_ref[b]).astype(BF16)
        out_copy(b).start()
        return carry

    lax.fori_loop(0, blocks, gather, 0)

    def drain(t, carry):
        d, b = t // blocks, t % blocks

        @pl.when(d > place)
        def _():
            hop_up(d, b).wait_send()

        @pl.when(d < place)
        def _():
            hop_down(d, b).wait_send()

        return carry

    lax.fori_loop(0, n * blocks, drain, 0)

    def sdrain(d, carry):
        @pl.when(d > place)
        def _():
            shop_up(d).wait_send()

        @pl.when(d < place)
        def _():
            shop_down(d).wait_send()

        return carry

    lax.fori_loop(0, n, sdrain, 0)
    for c in range(chunks):
        pair_copy(c).wait_send()
        swap_copy(c, own_rows).wait_send()
        for s in range(1, levels + 1):
            scan_copy(s, c).wait_send()
    for s in range(levels + 1):
        log_copy(s).wait_send()
    picked_copy.wait_send()
    reply_copy.wait_send()
    for b in range(blocks):
        out_copy(b).wait()


def per_device(
    prompt_values,
    prompt_gate,
    prompt_inject,
    prompt_read,
    prompt_step,
    decay_log,
    skip_gain,
    norm_weight,
    out_weight,
    sample_values,
    sample_gate,
    sample_inject,
    sample_read,
    sample_step,
    sample_length,
):
    n, peers = lax.axis_size("head"), lax.axis_size("ctx")
    levels = peers.bit_length() - 2
    tokens, channels = prompt_values.shape
    heads = prompt_step.shape[0]
    dim = channels // heads
    entries = prompt_inject.shape[2]
    half = entries // 2
    samples, length = sample_values.shape[:2]
    padded = -(-samples // (2 * PAD)) * 2 * PAD
    cols = out_weight.shape[1] // n
    blocks, chunks = tokens // BLOCK, channels // CHUNK
    vmem = pl.BlockSpec(memory_space=pltpu.VMEM)
    hbm = pl.BlockSpec(memory_space=pl.ANY)
    dma = pltpu.SemaphoreType.DMA
    shape = jax.ShapeDtypeStruct
    V = pltpu.VMEM
    mixed, smixed = pl.pallas_call(
        functools.partial(layer_kernel, dim, n, peers),
        out_shape=(shape((cols, tokens), BF16), shape((samples, cols), BF16)),
        in_specs=[
            pl.BlockSpec(memory_space=pltpu.SMEM),
            hbm,
            hbm,
            vmem,
            vmem,
            vmem,
            vmem,
            vmem,
            vmem,
            hbm,
            vmem,
            vmem,
            vmem,
            vmem,
            vmem,
        ],
        out_specs=(hbm, vmem),
        scratch_shapes=[
            V((tokens, channels), BF16),
            V((tokens, channels), BF16),
            V((n, channels, cols), BF16),
            V((blocks, heads, BLOCK), F32),
            V((blocks, heads, BLOCK), F32),
            V((tokens, 2 * heads), BF16),
            V((2 * heads, channels), BF16),
            V((entries, tokens), BF16),
            V((PAD, channels), F32),
            V((chunks, entries, CHUNK), BF16),
            V((chunks, half, CHUNK), BF16),
            V((levels + 1, chunks, half, CHUNK), BF16),
            V((levels, chunks, half, CHUNK), BF16),
            V((chunks, half, CHUNK), F32),
            V((chunks, half, CHUNK), BF16),
            V((chunks, entries, CHUNK), BF16),
            V((levels + 1, PAD, heads), F32),
            V((levels + 1, PAD, heads), F32),
            V((PAD, heads), F32),
            V((PAD, channels), F32),
            V((levels, PAD, channels), F32),
            V((entries, channels), F32),
            V((PAD, heads), F32),
            V((BLOCK, channels), F32),
            V((tokens, channels), BF16),
            V((tokens, channels), BF16),
            V((tokens + padded, channels), BF16),
            V((padded, channels), F32),
            V((padded, channels), F32),
            V((padded, entries), BF16),
            V((padded, entries), BF16),
            V((padded, channels), F32),
            V((padded, channels), F32),
            V((BLOCK, cols), F32),
            V((blocks, BLOCK, cols), F32),
            V((n, blocks, BLOCK, cols), BF16),
            V((n + 1, blocks, BLOCK, cols), BF16),
            V((n, padded, cols), BF16),
            V((n + 1, padded, cols), BF16),
            V((padded, cols), F32),
            V((blocks, cols, BLOCK), BF16),
            dma((chunks,)),
            dma((1,)),
            dma((n,)),
            dma((blocks,)),
            dma((levels + 1,)),
            dma((levels + 1,)),
            dma((chunks,)),
            dma((chunks,)),
            dma((levels, chunks)),
            dma((levels, chunks)),
            dma((chunks,)),
            dma((chunks,)),
            dma((2,)),
            dma((2,)),
            dma((n, blocks)),
            dma((n + 1, blocks)),
            dma((n,)),
            dma((n + 1,)),
        ],
        compiler_params=pltpu.CompilerParams(
            collective_id=0, has_side_effects=True, vmem_limit_bytes=VMEM_LIMIT
        ),
    )(
        sample_length,
        prompt_values,
        prompt_gate,
        prompt_inject.reshape(tokens, entries),
        prompt_read.reshape(tokens, entries),
        prompt_step,
        decay_log[None],
        skip_gain[None],
        norm_weight[None],
        out_weight,
        sample_values,
        sample_gate,
        sample_inject.reshape(samples, length, entries),
        sample_read.reshape(samples, length, entries),
        sample_step.transpose(1, 2, 0),
    )
    return mixed, smixed.T


def solution(mesh):
    in_specs = (
        P("ctx", "head"),
        P("ctx", "head"),
        P("ctx", "head", None),
        P("ctx", "head", None),
        P("head", "ctx"),
        P("head"),
        P("head"),
        P("head"),
        P("head", None),
        P("ctx", None, "head"),
        P("ctx", None, "head"),
        P("ctx", None, "head", None),
        P("ctx", None, "head", None),
        P("head", "ctx", None),
        P("ctx"),
    )
    out_specs = (P("head", "ctx"), P("head", "ctx"))
    return jax.shard_map(
        per_device, mesh=mesh, in_specs=in_specs, out_specs=out_specs, check_vma=False
    )
```

```python
import functools

import jax
import jax.numpy as jnp
from jax import lax
from jax.experimental import pallas as pl
from jax.experimental.pallas import tpu as pltpu
from jax.sharding import PartitionSpec as P

BLOCK = 128
LANES = 128
PAD = 8
F32 = jnp.float32
BF16 = jnp.bfloat16
EXACT = lax.Precision.HIGHEST
VMEM_LIMIT = 60 * 1024 * 1024


def dot(a, b, dims=((1,), (0,)), precision=None):
    return lax.dot_general(a, b, (dims, ((), ())), precision=precision, preferred_element_type=F32)


def softplus(v):
    return jnp.maximum(v, 0.0) + jnp.log1p(jnp.exp(-jnp.abs(v)))


def silu(v):
    return v / (1.0 + jnp.exp(-v))


def spread(w, expander):
    high = w.astype(BF16)
    low = (w - high.astype(F32)).astype(BF16)
    return dot(jnp.concatenate([high, low], axis=1), expander)


def expander_of(heads, dim):
    row = lax.broadcasted_iota(jnp.int32, (2 * heads, heads * dim), 0)
    lane = lax.broadcasted_iota(jnp.int32, (2 * heads, heads * dim), 1)
    head = lane // dim
    return jnp.where((row == head) | (row == head + heads), 1.0, 0.0).astype(BF16)


def square(n):
    return (
        lax.broadcasted_iota(jnp.int32, (n, n), 0),
        lax.broadcasted_iota(jnp.int32, (n, n), 1),
    )


def finish_rows(total, weight):
    mean = jnp.mean(total * total, axis=1, keepdims=True)
    return (total * lax.rsqrt(mean + 1e-05) * weight).astype(BF16)


CHUNK = 2 * LANES
LAG = 3
EARLY = 2


def turn_over(w):
    return jnp.transpose(w, (1, 0))


def layer_kernel(
    dim,
    n,
    peers,
    length_ref,
    values_hbm,
    gate_hbm,
    inject_ref,
    read_ref,
    step_ref,
    decay_ref,
    gain_in_ref,
    norm_ref,
    weight_hbm,
    svalues_ref,
    sgate_ref,
    sinject_ref,
    sread_ref,
    sstep_ref,
    out_hbm,
    sout_hbm,
    values_ref,
    gate_ref,
    tiles_ref,
    steps_ref,
    logs_ref,
    wide_ref,
    expander_ref,
    turned_ref,
    skip_ref,
    mine_state,
    pair_state,
    totals,
    arrived,
    before_ref,
    swap_ref,
    enter_ref,
    log_sent,
    log_got,
    before_logs,
    pair_scale,
    scale_ref,
    state_ref,
    offset_ref,
    part_ref,
    local_ref,
    gain_ref,
    normed_ref,
    slocal_ref,
    sgain_ref,
    picked_ref,
    picked_got,
    reply_ref,
    reply_got,
    acc_ref,
    own_ref,
    sent,
    landing,
    ssent,
    slanding,
    sown_ref,
    result_ref,
    sresult_ref,
    value_sems,
    gate_sem,
    tile_sems,
    out_sems,
    log_ssems,
    log_rsems,
    pair_ssems,
    pair_rsems,
    scan_ssems,
    scan_rsems,
    swap_ssems,
    swap_rsems,
    small_ssems,
    small_rsems,
    sent_sems,
    land_sems,
    ssent_sems,
    sland_sems,
):
    tokens, channels = values_ref.shape
    heads = step_ref.shape[0]
    entries = inject_ref.shape[1]
    half = entries // 2
    cols = acc_ref.shape[1]
    chunks = channels // CHUNK
    blocks = tokens // BLOCK
    levels = totals.shape[0] - 1
    place = lax.axis_index("head")
    seat = lax.axis_index("ctx")
    side = seat % 2
    odd = side == 1
    own_rows = pl.ds(pl.multiple_of(side * half, half), half)
    other_rows = pl.ds(pl.multiple_of((1 - side) * half, half), half)

    def lanes_of(c):
        return slice(c * CHUNK, (c + 1) * CHUNK)

    def some_lanes(c):
        return pl.ds(pl.multiple_of(c * CHUNK, CHUNK), CHUNK)

    def value_copy(c):
        return pltpu.make_async_copy(
            values_hbm.at[:, lanes_of(c)], values_ref.at[:, lanes_of(c)], value_sems.at[c]
        )

    gate_copy = pltpu.make_async_copy(gate_hbm, gate_ref, gate_sem.at[0])

    def tile_copy(d):
        return pltpu.make_async_copy(
            weight_hbm.at[:, pl.ds(d * cols, cols)], tiles_ref.at[d], tile_sems.at[d]
        )

    for c in range(chunks):
        value_copy(c).start()
    gate_copy.start()

    def digit(s):
        return (seat // (1 << s)) % 2

    def mate(s):
        return seat + (1 << s) - (2 << s) * digit(s)

    barrier = pltpu.get_barrier_semaphore()

    def greet(device):
        pl.semaphore_signal(
            barrier, inc=1, device_id=device, device_id_type=pl.DeviceIdType.MESH
        )

    for s in range(levels + 1):
        greet({"ctx": mate(s)})

    @pl.when(place > 0)
    def _():
        greet({"head": place - 1})

    @pl.when(place < n - 1)
    def _():
        greet({"head": place + 1})

    rows, lanes = square(heads)
    rate_row = -jnp.exp(decay_ref[...])
    rate = jnp.sum(jnp.where(rows == lanes, rate_row, 0.0), axis=1, keepdims=True)
    steps = softplus(step_ref[...])
    logs = steps * rate
    i, j = square(BLOCK)

    def fill_expander():
        expander_ref[...] = expander_of(heads, dim)

    fill_expander()
    later = jnp.zeros((heads, 1), F32)
    for b in reversed(range(blocks)):
        span = slice(b * BLOCK, (b + 1) * BLOCK)
        steps_ref[b] = steps[:, span]
        logs_ref[b] = logs[:, span]
        after = dot(logs[:, span], jnp.where(i > j, 1.0, 0.0), precision=EXACT) + later
        later = later + jnp.sum(logs[:, span], axis=1, keepdims=True)
        w = turn_over(jnp.exp(after) * steps[:, span])
        high = w.astype(BF16)
        low = (w - high.astype(F32)).astype(BF16)
        wide_ref[span, :] = jnp.concatenate([high, low], axis=1)
    total_logs = jnp.sum(jnp.where(rows == lanes, later, 0.0), axis=0, keepdims=True)
    total_logs = jnp.broadcast_to(total_logs, (PAD, heads))

    def turn_inject():
        turned_ref[...] = turn_over(inject_ref[...].astype(F32)).astype(BF16)

    turn_inject()
    top = lax.broadcasted_iota(jnp.int32, (PAD, heads), 0) == 0

    inside = (place > 0) & (place < n - 1)
    log_sent[0] = total_logs
    before_logs[...] = jnp.zeros_like(before_logs)

    def state_of(c):
        value_copy(c).wait()
        wide = dot(wide_ref[...], expander_ref[:, lanes_of(c)])
        scaled = (wide * values_ref[:, lanes_of(c)].astype(F32)).astype(BF16)
        mine_state[c] = dot(turned_ref[...], scaled).astype(BF16)

    state_of(0)

    @pl.when(inside)
    def _():
        pl.semaphore_wait(barrier, levels + 3)

    @pl.when(jnp.logical_not(inside))
    def _():
        pl.semaphore_wait(barrier, levels + 2)

    def remote(src, dst, ssem, rsem, device):
        return pltpu.make_async_remote_copy(
            src_ref=src,
            dst_ref=dst,
            send_sem=ssem,
            recv_sem=rsem,
            device_id=device,
            device_id_type=pl.DeviceIdType.MESH,
        )

    def log_copy(s):
        return remote(
            log_sent.at[s], log_got.at[s], log_ssems.at[s], log_rsems.at[s], {"ctx": mate(s)}
        )

    def pair_copy(c):
        return remote(
            mine_state.at[c, other_rows],
            pair_state.at[c],
            pair_ssems.at[c],
            pair_rsems.at[c],
            {"ctx": mate(0)},
        )

    def scan_copy(s, c):
        return remote(
            totals.at[s - 1, c],
            arrived.at[s - 1, c],
            scan_ssems.at[s - 1, c],
            scan_rsems.at[s - 1, c],
            {"ctx": mate(s)},
        )

    def swap_copy(c, where):
        return remote(
            swap_ref.at[c],
            enter_ref.at[c, where],
            swap_ssems.at[c],
            swap_rsems.at[c],
            {"ctx": mate(0)},
        )

    log_copy(0).start()

    def exchange_logs(s):
        log_copy(s).wait_recv()
        got, own = log_got[s], log_sent[s]
        upper = digit(s) == 1
        above = jnp.where(upper, own, got)
        if s == 0:
            pair = jnp.where(top, above, jnp.where(odd, got, own))
            pair_scale[...] = spread(jnp.exp(pair), expander_ref[...])
        else:
            held = before_logs[...]
            scale_ref[s - 1] = spread(jnp.exp(jnp.where(top, above, held)), expander_ref[...])
            before_logs[...] = held + jnp.where(upper, got, 0.0)
        if s < levels:
            log_sent[s + 1] = own + got
            log_copy(s + 1).start()

    def pair_up(c):
        pair_copy(c).wait_recv()
        mine = mine_state[c, own_rows].astype(F32)
        theirs = pair_state[c].astype(F32)
        first, second = jnp.where(odd, theirs, mine), jnp.where(odd, mine, theirs)
        totals[0, c] = (first * pair_scale[0:1, lanes_of(c)] + second).astype(BF16)
        scan_copy(1, c).start()

    pair_copy(0).start()
    for c in range(1, chunks):
        state_of(c)
        pair_copy(c).start()
        if c == 2:
            exchange_logs(0)
        if c > 2:
            pair_up(c - 3)
    for c in range(chunks - 3, chunks):
        if c == chunks - 1:
            exchange_logs(1)
        pair_up(c)

    def scan_step(s, c):
        scan_copy(s, c).wait_recv()
        upper = digit(s) == 1
        far = arrived[s - 1, c].astype(F32)
        near = totals[s - 1, c].astype(F32)
        first, second = jnp.where(upper, far, near), jnp.where(upper, near, far)
        total_scale = scale_ref[s - 1, 0:1, some_lanes(c)]
        totals[s, c] = (first * total_scale + second).astype(BF16)
        if s == 1:
            before = jnp.where(upper, far, 0.0)
        else:
            held = before_ref[c]
            before = jnp.where(upper, far * scale_ref[s - 1, 1:2, some_lanes(c)] + held, held)
        if s < levels:
            before_ref[c] = before
            scan_copy(s + 1, c).start()
        else:
            even_state = jnp.where(odd, pair_state[c].astype(F32), mine_state[c, own_rows].astype(F32))
            moved = before * pair_scale[1:2, some_lanes(c)] + even_state
            enter_ref[c, own_rows] = jnp.where(odd, moved, before).astype(BF16)
            swap_ref[c] = jnp.where(odd, before, moved).astype(BF16)
            swap_copy(c, own_rows).start()

    skip_ref[...] = spread(jnp.broadcast_to(gain_in_ref[...], (PAD, heads)), expander_ref[...])

    def sample_local():
        samples, length = svalues_ref.shape[:2]
        slocal_ref[...] = jnp.zeros_like(slocal_ref)
        sgain_ref[...] = jnp.zeros_like(sgain_ref)
        picked_ref[...] = jnp.zeros_like(picked_ref)
        u, s = square(length)
        own = lax.broadcasted_iota(jnp.int32, (heads, channels), 1) // dim == (
            lax.broadcasted_iota(jnp.int32, (heads, channels), 0)
        )
        at = lax.broadcasted_iota(jnp.int32, (1, length), 1)
        for k in range(samples):
            last = length_ref[k] - 1
            hot = jnp.where(
                lax.broadcasted_iota(jnp.int32, (PAD, length), 1) == last, 1.0, 0.0
            ).astype(BF16)
            tall = softplus(sstep_ref[k])
            tall_logs = tall * rate_row
            flip = ((0,), (0,))
            gap = dot(tall_logs, jnp.where((u > s) & (u <= last), 1.0, 0.0), flip, EXACT)
            running = dot(tall_logs, jnp.where(u <= last, 1.0, 0.0), flip, EXACT)[:, 0:1]
            wide_steps = dot(tall, jnp.where(u == s, 1.0, 0.0), flip, EXACT)
            row = dot(hot, sread_ref[k])
            score = dot(row.astype(BF16), sinject_ref[k], ((1,), (1,)))[0:1]
            mixing = jnp.where(at <= last, score * jnp.exp(gap) * wide_steps, 0.0).astype(BF16)
            values = svalues_ref[k]
            local = jnp.sum(jnp.where(own, dot(mixing, values), 0.0), axis=0, keepdims=True)
            decay = jnp.sum(jnp.where(own, jnp.exp(running), 0.0), axis=0, keepdims=True)
            value = dot(hot, values)[0:1]
            opened = silu(dot(hot, sgate_ref[k])[0:1])
            slocal_ref[k : k + 1, :] = (local + skip_ref[0:1, :] * value) * opened
            sgain_ref[k : k + 1, :] = decay * opened
            picked_ref[k : k + 1, :] = row[0:1].astype(BF16)

    state_ref[...] = jnp.zeros_like(state_ref)
    offset_ref[...] = jnp.zeros_like(offset_ref)
    gate_copy.wait()
    for k in range((n + 1) // 2):
        for d in sorted({n - 1 - k, k}, reverse=True):
            tile_copy(d).start()

    def block_local(b, hook):
        span = pl.ds(pl.multiple_of(b * BLOCK, BLOCK), BLOCK)
        steps, logs = steps_ref[b], logs_ref[b]
        i, j = square(BLOCK)
        lower = jnp.where(i >= j, 1.0, 0.0)
        running = dot(logs, lower, ((1,), (1,)), EXACT)
        running_t = turn_over(running)
        after = turn_over(dot(logs, jnp.where(i > j, 1.0, 0.0), precision=EXACT))
        turned = turn_over(steps)
        expander = expander_ref[...]
        inject = inject_ref[span, :]
        readout = read_ref[span, :]
        scores = jnp.where(i >= j, dot(readout, inject, ((1,), (1,))), 0.0)
        per = LANES // dim
        lane = lax.broadcasted_iota(jnp.int32, (BLOCK, LANES), 1)
        for k in range(heads // per):
            cut = slice(k * LANES, (k + 1) * LANES)
            pair = values_ref[span, cut]
            mixes, parts = [], []
            for q in range(per):
                h = k * per + q
                gap = jnp.minimum(running_t[:, h : h + 1] - running[h : h + 1, :], 0.0)
                mixes.append((scores * jnp.exp(gap) * steps[h : h + 1, :]).astype(BF16))
                parts.append(jnp.where(lane // dim == q, pair, jnp.zeros_like(pair)))
            part_ref[:, cut] = dot(jnp.concatenate(mixes, axis=1), jnp.concatenate(parts, axis=0))
            if hook is not None and 2 * (k + 1) == heads // per:
                hook(2 * b)
        decay = spread(jnp.exp(running_t), expander)
        values = values_ref[span, :].astype(F32)
        opened = silu(gate_ref[span, :].astype(F32))
        total = part_ref[...] + skip_ref[0:1, :] * values
        total = total + dot(readout, state_ref[...].astype(BF16)) * decay
        local_ref[span, :] = (total * opened).astype(BF16)
        offset = offset_ref[0:1, :]
        gain_ref[span, :] = (opened * spread(jnp.exp(running_t + offset), expander)).astype(BF16)
        offset_ref[0:1, :] = offset + running_t[BLOCK - 1 : BLOCK, :]
        scaled = (spread(jnp.exp(after) * turned, expander) * values).astype(BF16)
        state_ref[...] = state_ref[...] * decay[BLOCK - 1 : BLOCK, :] + dot(
            inject, scaled, ((0,), (0,))
        )
        if hook is not None:
            hook(2 * b + 1)

    def hook(g):
        for s in range(2, levels + 1):

            @pl.when(g == s - 1)
            def _():
                exchange_logs(s)

        for s in range(1, levels + 1):
            c = g - LAG * (s - 1)

            @pl.when((c >= 0) & (c < chunks))
            def _():
                scan_step(s, c)

    def small_copy(q, src, dst):
        return remote(src, dst, small_ssems.at[q], small_rsems.at[q], {"ctx": mate(0)})

    picked_copy = small_copy(0, picked_ref, picked_got)
    reply_copy = small_copy(1, reply_ref, reply_got)

    def round_of(t, carry):
        block_local(t, hook)
        return carry

    def late_round(g, carry):
        hook(g)
        return carry

    early = min(EARLY, blocks)
    lax.fori_loop(0, early, round_of, 0)
    lax.fori_loop(2 * early, max(chunks + LAG * (levels - 1), 2 * early), late_round, 0)
    for c in range(chunks):
        swap_copy(c, other_rows).wait_recv()
    for d in range(n):
        tile_copy(d).wait()

    def share(rows, d):
        return dot(normed_ref[rows, :], tiles_ref[d])

    def hop_up(d, b):
        return remote(
            sent.at[d, b],
            landing.at[d + 1, b],
            sent_sems.at[d, b],
            land_sems.at[d + 1, b],
            {"head": place + 1},
        )

    def hop_down(d, b):
        return remote(
            sent.at[d, b],
            landing.at[d, b],
            sent_sems.at[d, b],
            land_sems.at[d, b],
            {"head": place - 1},
        )

    def shop_up(d):
        return remote(
            ssent.at[d],
            slanding.at[d + 1],
            ssent_sems.at[d],
            sland_sems.at[d + 1],
            {"head": place + 1},
        )

    def shop_down(d):
        return remote(
            ssent.at[d], slanding.at[d], ssent_sems.at[d], sland_sems.at[d], {"head": place - 1}
        )

    def rows_of(b):
        return pl.ds(pl.multiple_of(b * BLOCK, BLOCK), BLOCK)

    def pass_on(d, b, slot, move, fed):
        acc_ref[...] = share(rows_of(b), d)

        @pl.when(fed)
        def _():
            move(d, b).wait_recv()
            acc_ref[...] = acc_ref[...] + landing[slot, b].astype(F32)

        sent[d, b] = acc_ref[...].astype(BF16)
        move(d, b).start()

    def finish_block(b):
        span = rows_of(b)
        readout = read_ref[span, :]
        pieces = []
        for c in range(chunks):
            arrival = dot(readout, enter_ref[c])
            piece = local_ref[span, lanes_of(c)].astype(F32)
            pieces.append(piece + arrival * gain_ref[span, lanes_of(c)].astype(F32))
        normed_ref[span, :] = finish_rows(jnp.concatenate(pieces, axis=1), norm_ref[...])

    def half_of(ref):
        return jnp.where(odd, ref[:, half:].astype(F32), ref[:, :half].astype(F32)).astype(BF16)

    padded = slocal_ref.shape[0]
    srows = pl.ds(tokens, padded)

    def answer():
        picked_copy.wait_recv()
        asked = half_of(picked_got)
        for c in range(chunks):
            reply_ref[:, lanes_of(c)] = dot(asked, totals[levels, c])
        reply_copy.start()

    def finish_samples():
        reply_copy.wait_recv()
        answered = half_of(picked_ref)
        arrivals = [dot(answered, totals[levels, c]) for c in range(chunks)]
        arrival = jnp.concatenate(arrivals, axis=1) + reply_got[...]
        total = slocal_ref[...] + arrival * sgain_ref[...]
        normed_ref[srows, :] = finish_rows(total, norm_ref[...])

    few = sresult_ref.shape[0]

    def sshare(d):
        wide = share(srows, d)
        return jnp.concatenate([wide[:few, q * LANES : (q + 1) * LANES] for q in range(cols // LANES)], axis=0)

    def spass_on(d, slot, move, fed):
        sown_ref[...] = sshare(d)

        @pl.when(fed)
        def _():
            move(d).wait_recv()
            sown_ref[...] = sown_ref[...] + slanding[slot].astype(F32)

        ssent[d] = sown_ref[...].astype(BF16)
        move(d).start()

    def step(t, carry):
        @pl.when(t < blocks)
        def _():
            finish_block(t)

        @pl.when(t == blocks)
        def _():
            finish_samples()

        rising, falling = t - place, t - (n - 1 - place)
        up, down = n - 1 - rising // blocks, falling // blocks

        @pl.when((rising >= 0) & (up > place))
        def _():
            pass_on(up, rising % blocks, up + 1, hop_up, place > 0)

        @pl.when((falling >= 0) & (down < place))
        def _():
            pass_on(down, falling % blocks, down, hop_down, place < n - 1)

        srising, sfalling = rising - blocks, falling - blocks
        sup, sdown = n - 1 - srising, sfalling

        @pl.when((srising >= 0) & (sup > place))
        def _():
            spass_on(sup, sup + 1, shop_up, place > 0)

        @pl.when((sfalling >= 0) & (sdown < place))
        def _():
            spass_on(sdown, sdown, shop_down, place < n - 1)

        @pl.when(t + early < blocks)
        def _():
            block_local(t + early, None)

        @pl.when(t == blocks - 2)
        def _():
            sample_local()
            picked_copy.start()

        @pl.when(t == blocks - 1)
        def _():
            answer()

        return carry

    lax.fori_loop(0, (n - 1) * blocks, step, 0)
    sown_ref[...] = sshare(place)

    def own(b, carry):
        own_ref[b] = share(rows_of(b), place)
        return carry

    lax.fori_loop(0, blocks, own, 0)

    @pl.when(place < n - 1)
    def _():
        shop_down(place).wait_recv()
        sown_ref[...] = sown_ref[...] + slanding[place].astype(F32)

    @pl.when(place > 0)
    def _():
        shop_up(place).wait_recv()
        sown_ref[...] = sown_ref[...] + slanding[place + 1].astype(F32)

    for q in range(cols // LANES):
        sresult_ref[:, q * LANES : (q + 1) * LANES] = sown_ref[q * few : (q + 1) * few, :].astype(BF16)
    sout_copy = pltpu.make_async_copy(sresult_ref, sout_hbm, gate_sem.at[1])
    sout_copy.start()

    def drain(t, carry):
        d, b = t // blocks, t % blocks

        @pl.when(d > place)
        def _():
            hop_up(d, b).wait_send()

        @pl.when(d < place)
        def _():
            hop_down(d, b).wait_send()

        return carry

    lax.fori_loop(0, n * blocks, drain, 0)

    def sdrain(d, carry):
        @pl.when(d > place)
        def _():
            shop_up(d).wait_send()

        @pl.when(d < place)
        def _():
            shop_down(d).wait_send()

        return carry

    lax.fori_loop(0, n, sdrain, 0)
    for c in range(chunks):
        pair_copy(c).wait_send()
        swap_copy(c, own_rows).wait_send()
        for s in range(1, levels + 1):
            scan_copy(s, c).wait_send()
    for s in range(levels + 1):
        log_copy(s).wait_send()
    picked_copy.wait_send()
    reply_copy.wait_send()
    def out_copy(b):
        return pltpu.make_async_copy(
            result_ref.at[b],
            out_hbm.at[:, pl.ds(pl.multiple_of(b * BLOCK, BLOCK), BLOCK)],
            out_sems.at[b],
        )

    def gather(b, carry):
        @pl.when(place < n - 1)
        def _():
            hop_down(place, b).wait_recv()
            own_ref[b] = own_ref[b] + landing[place, b].astype(F32)

        @pl.when(place > 0)
        def _():
            hop_up(place, b).wait_recv()
            own_ref[b] = own_ref[b] + landing[place + 1, b].astype(F32)

        result_ref[b] = turn_over(own_ref[b]).astype(BF16)
        out_copy(b).start()
        return carry

    lax.fori_loop(0, blocks, gather, 0)

    sout_copy.wait()
    for b in range(blocks):
        out_copy(b).wait()


def per_device(
    prompt_values,
    prompt_gate,
    prompt_inject,
    prompt_read,
    prompt_step,
    decay_log,
    skip_gain,
    norm_weight,
    out_weight,
    sample_values,
    sample_gate,
    sample_inject,
    sample_read,
    sample_step,
    sample_length,
):
    n, peers = lax.axis_size("head"), lax.axis_size("ctx")
    levels = peers.bit_length() - 2
    tokens, channels = prompt_values.shape
    heads = prompt_step.shape[0]
    dim = channels // heads
    entries = prompt_inject.shape[2]
    half = entries // 2
    samples, length = sample_values.shape[:2]
    padded = -(-samples // (2 * PAD)) * 2 * PAD
    cols = out_weight.shape[1] // n
    blocks, chunks = tokens // BLOCK, channels // CHUNK
    vmem = pl.BlockSpec(memory_space=pltpu.VMEM)
    hbm = pl.BlockSpec(memory_space=pl.ANY)
    dma = pltpu.SemaphoreType.DMA
    shape = jax.ShapeDtypeStruct
    V = pltpu.VMEM
    mixed, smixed = pl.pallas_call(
        functools.partial(layer_kernel, dim, n, peers),
        out_shape=(shape((cols, tokens), BF16), shape((samples, cols), BF16)),
        in_specs=[
            pl.BlockSpec(memory_space=pltpu.SMEM),
            hbm,
            hbm,
            vmem,
            vmem,
            vmem,
            vmem,
            vmem,
            vmem,
            hbm,
            vmem,
            vmem,
            vmem,
            vmem,
            vmem,
        ],
        out_specs=(hbm, hbm),
        scratch_shapes=[
            V((tokens, channels), BF16),
            V((tokens, channels), BF16),
            V((n, channels, cols), BF16),
            V((blocks, heads, BLOCK), F32),
            V((blocks, heads, BLOCK), F32),
            V((tokens, 2 * heads), BF16),
            V((2 * heads, channels), BF16),
            V((entries, tokens), BF16),
            V((PAD, channels), F32),
            V((chunks, entries, CHUNK), BF16),
            V((chunks, half, CHUNK), BF16),
            V((levels + 1, chunks, half, CHUNK), BF16),
            V((levels, chunks, half, CHUNK), BF16),
            V((chunks, half, CHUNK), F32),
            V((chunks, half, CHUNK), BF16),
            V((chunks, entries, CHUNK), BF16),
            V((levels + 1, PAD, heads), F32),
            V((levels + 1, PAD, heads), F32),
            V((PAD, heads), F32),
            V((PAD, channels), F32),
            V((levels, PAD, channels), F32),
            V((entries, channels), F32),
            V((PAD, heads), F32),
            V((BLOCK, channels), F32),
            V((tokens, channels), BF16),
            V((tokens, channels), BF16),
            V((tokens + padded, channels), BF16),
            V((padded, channels), F32),
            V((padded, channels), F32),
            V((padded, entries), BF16),
            V((padded, entries), BF16),
            V((padded, channels), F32),
            V((padded, channels), F32),
            V((BLOCK, cols), F32),
            V((blocks, BLOCK, cols), F32),
            V((n, blocks, BLOCK, cols), BF16),
            V((n + 1, blocks, BLOCK, cols), BF16),
            V((n, samples * cols // LANES, LANES), BF16),
            V((n + 1, samples * cols // LANES, LANES), BF16),
            V((samples * cols // LANES, LANES), F32),
            V((blocks, cols, BLOCK), BF16),
            V((samples, cols), BF16),
            dma((chunks,)),
            dma((2,)),
            dma((n,)),
            dma((blocks,)),
            dma((levels + 1,)),
            dma((levels + 1,)),
            dma((chunks,)),
            dma((chunks,)),
            dma((levels, chunks)),
            dma((levels, chunks)),
            dma((chunks,)),
            dma((chunks,)),
            dma((2,)),
            dma((2,)),
            dma((n, blocks)),
            dma((n + 1, blocks)),
            dma((n,)),
            dma((n + 1,)),
        ],
        compiler_params=pltpu.CompilerParams(
            collective_id=0, has_side_effects=True, vmem_limit_bytes=VMEM_LIMIT
        ),
    )(
        sample_length,
        prompt_values,
        prompt_gate,
        prompt_inject.reshape(tokens, entries),
        prompt_read.reshape(tokens, entries),
        prompt_step,
        decay_log[None],
        skip_gain[None],
        norm_weight[None],
        out_weight,
        sample_values,
        sample_gate,
        sample_inject.reshape(samples, length, entries),
        sample_read.reshape(samples, length, entries),
        sample_step.transpose(1, 2, 0),
    )
    return mixed, smixed.T


def solution(mesh):
    in_specs = (
        P("ctx", "head"),
        P("ctx", "head"),
        P("ctx", "head", None),
        P("ctx", "head", None),
        P("head", "ctx"),
        P("head"),
        P("head"),
        P("head"),
        P("head", None),
        P("ctx", None, "head"),
        P("ctx", None, "head"),
        P("ctx", None, "head", None),
        P("ctx", None, "head", None),
        P("head", "ctx", None),
        P("ctx"),
    )
    out_specs = (P("head", "ctx"), P("head", "ctx"))
    return jax.shard_map(
        per_device, mesh=mesh, in_specs=in_specs, out_specs=out_specs, check_vma=False
    )
```

```python
import functools

import jax
import jax.numpy as jnp
from jax import lax
from jax.experimental import pallas as pl
from jax.experimental.pallas import tpu as pltpu
from jax.sharding import PartitionSpec as P

BLOCK = 128
LANES = 128
PAD = 8
F32 = jnp.float32
BF16 = jnp.bfloat16
EXACT = lax.Precision.HIGHEST
VMEM_LIMIT = 60 * 1024 * 1024


def dot(a, b, dims=((1,), (0,)), precision=None):
    return lax.dot_general(a, b, (dims, ((), ())), precision=precision, preferred_element_type=F32)


def softplus(v):
    return jnp.maximum(v, 0.0) + jnp.log1p(jnp.exp(-jnp.abs(v)))


def silu(v):
    return v / (1.0 + jnp.exp(-v))


def spread(w, expander):
    high = w.astype(BF16)
    low = (w - high.astype(F32)).astype(BF16)
    return dot(jnp.concatenate([high, low], axis=1), expander)


def expander_of(heads, dim):
    row = lax.broadcasted_iota(jnp.int32, (2 * heads, heads * dim), 0)
    lane = lax.broadcasted_iota(jnp.int32, (2 * heads, heads * dim), 1)
    head = lane // dim
    return jnp.where((row == head) | (row == head + heads), 1.0, 0.0).astype(BF16)


def square(n):
    return (
        lax.broadcasted_iota(jnp.int32, (n, n), 0),
        lax.broadcasted_iota(jnp.int32, (n, n), 1),
    )


def finish_rows(total, weight):
    mean = jnp.mean(total * total, axis=1, keepdims=True)
    return (total * lax.rsqrt(mean + 1e-05) * weight).astype(BF16)


CHUNK = 2 * LANES
LAG = 3
HOOKS = 4


def turn_over(w):
    return jnp.transpose(w, (1, 0))


def layer_kernel(
    dim,
    n,
    peers,
    length_ref,
    values_hbm,
    gate_hbm,
    inject_ref,
    read_hbm,
    step_ref,
    decay_ref,
    gain_in_ref,
    norm_ref,
    weight_hbm,
    svalues_hbm,
    sgate_hbm,
    sinject_hbm,
    sread_hbm,
    sstep_hbm,
    out_hbm,
    sout_hbm,
    values_ref,
    gate_ref,
    read_ref,
    svalues_ref,
    sgate_ref,
    sinject_ref,
    sread_ref,
    sstep_ref,
    tiles_ref,
    steps_ref,
    logs_ref,
    wide_ref,
    expander_ref,
    turned_ref,
    skip_ref,
    mine_state,
    pair_state,
    totals,
    arrived,
    before_ref,
    swap_ref,
    enter_ref,
    log_sent,
    log_got,
    before_logs,
    pair_scale,
    scale_ref,
    state_ref,
    offset_ref,
    part_ref,
    gain_ref,
    normed_ref,
    slocal_ref,
    sgain_ref,
    picked_ref,
    picked_all,
    reply_ref,
    reply_got,
    acc_ref,
    own_ref,
    sent,
    landing,
    ssent,
    slanding,
    sown_ref,
    result_ref,
    sresult_ref,
    value_sems,
    late_sems,
    tile_sems,
    out_sems,
    log_ssems,
    log_rsems,
    pair_ssems,
    pair_rsems,
    scan_ssems,
    scan_rsems,
    swap_ssems,
    swap_rsems,
    small_ssems,
    small_rsems,
    picked_sems,
    reply_sems,
    sent_sems,
    land_sems,
    ssent_sems,
    sland_sems,
):
    tokens, channels = values_ref.shape
    heads = step_ref.shape[0]
    entries = inject_ref.shape[1]
    half = entries // 2
    cols = acc_ref.shape[1]
    chunks = channels // CHUNK
    blocks = tokens // BLOCK
    levels = peers.bit_length() - 2
    squared = levels == 2
    log_steps = 2 if squared else levels + 1
    scan_steps = arrived.shape[0]
    place = lax.axis_index("head")
    seat = lax.axis_index("ctx")
    side = seat % 2
    odd = side == 1
    own_rows = pl.ds(pl.multiple_of(side * half, half), half)
    other_rows = pl.ds(pl.multiple_of((1 - side) * half, half), half)

    def lanes_of(c):
        return slice(c * CHUNK, (c + 1) * CHUNK)

    def some_lanes(c):
        return pl.ds(pl.multiple_of(c * CHUNK, CHUNK), CHUNK)

    def value_copy(q):
        lanes = slice(2 * q * CHUNK, 2 * (q + 1) * CHUNK)
        return pltpu.make_async_copy(values_hbm.at[:, lanes], values_ref.at[:, lanes], value_sems.at[q])

    late = [
        (gate_hbm, gate_ref),
        (read_hbm, read_ref),
        (svalues_hbm, svalues_ref),
        (sgate_hbm, sgate_ref),
        (sinject_hbm, sinject_ref),
        (sread_hbm, sread_ref),
        (sstep_hbm, sstep_ref),
    ]
    late_copies = [pltpu.make_async_copy(*refs, late_sems.at[q]) for q, refs in enumerate(late)]

    def tile_copy(d):
        return pltpu.make_async_copy(
            weight_hbm.at[:, pl.ds(d * cols, cols)], tiles_ref.at[d], tile_sems.at[d]
        )

    for q in range(chunks // 2):
        value_copy(q).start()
    for copy in late_copies:
        copy.start()

    def digit(s):
        return (seat // (1 << s)) % 2

    def mate(s):
        return seat + (1 << s) - (2 << s) * digit(s)

    barrier = pltpu.get_barrier_semaphore()

    def greet(device):
        pl.semaphore_signal(
            barrier, inc=1, device_id=device, device_id_type=pl.DeviceIdType.MESH
        )

    for s in range(levels + 1):
        greet({"ctx": mate(s)})

    last_seat = peers - 1
    holds_final = seat == last_seat

    @pl.when(holds_final)
    def _():
        for p in range(peers - 1):
            greet({"ctx": p})

    @pl.when(jnp.logical_not(holds_final))
    def _():
        greet({"ctx": last_seat})

    @pl.when(place > 0)
    def _():
        greet({"head": place - 1})

    @pl.when(place < n - 1)
    def _():
        greet({"head": place + 1})

    rows, lanes = square(heads)
    rate_row = -jnp.exp(decay_ref[...])
    rate = jnp.sum(jnp.where(rows == lanes, rate_row, 0.0), axis=1, keepdims=True)
    steps = softplus(step_ref[...])
    logs = steps * rate
    i, j = square(BLOCK)

    def fill_expander():
        expander_ref[...] = expander_of(heads, dim)

    fill_expander()
    later = jnp.zeros((heads, 1), F32)
    for b in reversed(range(blocks)):
        span = slice(b * BLOCK, (b + 1) * BLOCK)
        steps_ref[b] = steps[:, span]
        logs_ref[b] = logs[:, span]
        after = dot(logs[:, span], jnp.where(i > j, 1.0, 0.0), precision=EXACT) + later
        later = later + jnp.sum(logs[:, span], axis=1, keepdims=True)
        w = turn_over(jnp.exp(after) * steps[:, span])
        high = w.astype(BF16)
        low = (w - high.astype(F32)).astype(BF16)
        wide_ref[span, :] = jnp.concatenate([high, low], axis=1)
    total_logs = jnp.sum(jnp.where(rows == lanes, later, 0.0), axis=0, keepdims=True)
    total_logs = jnp.broadcast_to(total_logs, (PAD, heads))

    def turn_inject():
        turned_ref[...] = turn_over(inject_ref[...].astype(F32)).astype(BF16)

    turn_inject()
    top = lax.broadcasted_iota(jnp.int32, (PAD, heads), 0) == 0

    inside = (place > 0) & (place < n - 1)
    log_sent[0] = total_logs
    before_logs[...] = jnp.zeros_like(before_logs)

    def state_of(q):
        lanes = slice(2 * q * CHUNK, 2 * (q + 1) * CHUNK)
        value_copy(q).wait()
        wide = dot(wide_ref[...], expander_ref[:, lanes])
        scaled = (wide * values_ref[:, lanes].astype(F32)).astype(BF16)
        state = dot(turned_ref[...], scaled).astype(BF16)
        mine_state[2 * q] = state[:, :CHUNK]
        mine_state[2 * q + 1] = state[:, CHUNK:]

    state_of(0)

    for middle in (False, True):
        for final in (False, True):

            @pl.when((inside == middle) & (holds_final == final))
            def _():
                pl.semaphore_wait(barrier, levels + 2 + middle + (peers - 1 if final else 1))

    def remote(src, dst, ssem, rsem, device):
        return pltpu.make_async_remote_copy(
            src_ref=src,
            dst_ref=dst,
            send_sem=ssem,
            recv_sem=rsem,
            device_id=device,
            device_id_type=pl.DeviceIdType.MESH,
        )

    def log_copy(s):
        return remote(
            log_sent.at[s], log_got.at[s], log_ssems.at[s], log_rsems.at[s], {"ctx": mate(s)}
        )

    def pair_copy(c):
        return remote(
            mine_state.at[c, other_rows],
            pair_state.at[c],
            pair_ssems.at[c],
            pair_rsems.at[c],
            {"ctx": mate(0)},
        )

    def scan_copy(s, c):
        return remote(
            totals.at[s - 1, c],
            arrived.at[s - 1, c],
            scan_ssems.at[s - 1, c],
            scan_rsems.at[s - 1, c],
            {"ctx": mate(1 if squared and s == 3 else s)},
        )

    def swap_copy(c, where):
        return remote(
            swap_ref.at[c],
            enter_ref.at[c, where],
            swap_ssems.at[c],
            swap_rsems.at[c],
            {"ctx": mate(0)},
        )

    log_copy(0).start()

    def exchange_logs(s):
        log_copy(s).wait_recv()
        got, own = log_got[s], log_sent[s]
        upper = digit(s) == 1
        above = jnp.where(upper, own, got)
        if s == 0:
            pair = jnp.where(top, above, jnp.where(odd, got, own))
            pair_scale[...] = spread(jnp.exp(pair), expander_ref[...])
        else:
            held = before_logs[...]
            crossed = jnp.where(digit(2) == 1, jnp.where(upper, got, own), above) if squared else above
            scale_ref[s - 1] = spread(jnp.exp(jnp.where(top, crossed, held)), expander_ref[...])
            before_logs[...] = held + jnp.where(upper, got, 0.0)
        if s < log_steps - 1:
            log_sent[s + 1] = own + got
            log_copy(s + 1).start()

    column, row = digit(1), digit(2)

    def at_once(c):
        if not squared:
            return seat >= 0
        if c % 2:
            return column == 0
        return (column == 1) & (row == 0)

    def sends(s, c):
        if not squared:
            return seat >= 0
        if s == 1:
            return column == 0 if c % 2 else row == 0
        return (column == c % 2) & (row == s - 2)

    def pair_up(c):
        pair_copy(c).wait_recv()
        mine = mine_state[c, own_rows].astype(F32)
        theirs = pair_state[c].astype(F32)
        first, second = jnp.where(odd, theirs, mine), jnp.where(odd, mine, theirs)
        totals[0, c] = (first * pair_scale[0:1, lanes_of(c)] + second).astype(BF16)

        @pl.when(at_once(c))
        def _():
            scan_copy(1, c).start()

    pairs = chunks // 2
    for q in range(pairs):
        if q:
            state_of(q)
        pair_copy(2 * q + 1).start()
        pair_copy(2 * q).start()
        if q == 1:
            exchange_logs(0)
        if q > 1:
            pair_up(2 * q - 3)
            pair_up(2 * q - 4)
    for q in range(pairs - 2, pairs):
        pair_up(2 * q + 1)
        pair_up(2 * q)
    if squared:
        for c in range(0, chunks, 2):

            @pl.when((column == 0) & (row == 0))
            def _():
                scan_copy(1, c).start()

    def enter(c, before):
        even_state = jnp.where(odd, pair_state[c].astype(F32), mine_state[c, own_rows].astype(F32))
        moved = before * pair_scale[1:2, some_lanes(c)] + even_state
        enter_ref[c, own_rows] = jnp.where(odd, moved, before).astype(BF16)
        swap_ref[c] = jnp.where(odd, before, moved).astype(BF16)
        swap_copy(c, own_rows).start()

    def cross_row(q):
        c = 2 * q + column
        scan_copy(1, c).wait_recv()
        far, near = arrived[0, c].astype(F32), totals[0, c].astype(F32)
        right = column == 1
        first, second = jnp.where(right, far, near), jnp.where(right, near, far)
        totals[1, c] = (first * scale_ref[0, 0:1, some_lanes(c)] + second).astype(BF16)
        scan_copy(2, c).start()
        enter(c, jnp.where(right, far, 0.0))

        @pl.when(column == 0)
        def _():
            enter(c + 1, jnp.zeros((half, CHUNK), F32))

    def end_row(q):
        @pl.when(column == 1)
        def _():
            scan_copy(1, 2 * q).wait_recv()
            enter(2 * q, arrived[0, 2 * q].astype(F32))

    def next_row(q):
        c = 2 * q + column
        right = column == 1

        @pl.when(right)
        def _():
            scan_copy(1, c).wait_recv()
            totals[0, c] = arrived[0, c]

        scan_copy(2, c).wait_recv()
        far = arrived[1, c].astype(F32)
        joined = far * scale_ref[0, 0:1, some_lanes(c)] + totals[0, c].astype(F32)
        totals[2, c] = jnp.where(right, far, joined).astype(BF16)
        scan_copy(3, c).start()
        enter(c, jnp.where(right, joined, far))

    def last_column(q):
        c = 2 * q + 1 - column
        scan_copy(3, c).wait_recv()
        enter(c, arrived[2, c].astype(F32))

    def square_events():
        first = [(q, cross_row, q) for q in range(pairs)]
        first += [(q + pairs, end_row, q) for q in range(pairs)]
        second = [(q, next_row, q) for q in range(pairs)]
        second += [(q + 2.5, last_column, q) for q in range(pairs)]
        return [sorted(events, key=lambda event: event[0]) for events in (first, second)]

    def run_events(here, events):
        @pl.when(here)
        def _():
            for _, work, q in events:
                work(q)

    def scan_step(s, c):
        scan_copy(s, c).wait_recv()
        upper = digit(s) == 1
        far = arrived[s - 1, c].astype(F32)
        near = totals[s - 1, c].astype(F32)
        first, second = jnp.where(upper, far, near), jnp.where(upper, near, far)
        total_scale = scale_ref[s - 1, 0:1, some_lanes(c)]
        totals[s, c] = (first * total_scale + second).astype(BF16)
        if s == 1:
            before = jnp.where(upper, far, 0.0)
        else:
            held = before_ref[c]
            before = jnp.where(upper, far * scale_ref[s - 1, 1:2, some_lanes(c)] + held, held)
        if s < levels:
            before_ref[c] = before
            scan_copy(s + 1, c).start()
        else:
            enter(c, before)

    exchange_logs(1)

    skip_ref[...] = spread(jnp.broadcast_to(gain_in_ref[...], (PAD, heads)), expander_ref[...])

    def sample_local():
        samples, length = svalues_ref.shape[:2]
        slocal_ref[...] = jnp.zeros_like(slocal_ref)
        sgain_ref[...] = jnp.zeros_like(sgain_ref)
        picked_ref[...] = jnp.zeros_like(picked_ref)
        u, s = square(length)
        own = lax.broadcasted_iota(jnp.int32, (heads, channels), 1) // dim == (
            lax.broadcasted_iota(jnp.int32, (heads, channels), 0)
        )
        at = lax.broadcasted_iota(jnp.int32, (1, length), 1)
        for k in range(samples):
            last = length_ref[k] - 1
            hot = jnp.where(
                lax.broadcasted_iota(jnp.int32, (PAD, length), 1) == last, 1.0, 0.0
            ).astype(BF16)
            tall = softplus(sstep_ref[k])
            tall_logs = tall * rate_row
            flip = ((0,), (0,))
            gap = dot(tall_logs, jnp.where((u > s) & (u <= last), 1.0, 0.0), flip, EXACT)
            running = dot(tall_logs, jnp.where(u <= last, 1.0, 0.0), flip, EXACT)[:, 0:1]
            wide_steps = dot(tall, jnp.where(u == s, 1.0, 0.0), flip, EXACT)
            row = dot(hot, sread_ref[k])
            score = dot(row.astype(BF16), sinject_ref[k], ((1,), (1,)))[0:1]
            mixing = jnp.where(at <= last, score * jnp.exp(gap) * wide_steps, 0.0).astype(BF16)
            values = svalues_ref[k]
            local = jnp.sum(jnp.where(own, dot(mixing, values), 0.0), axis=0, keepdims=True)
            decay = jnp.sum(jnp.where(own, jnp.exp(running), 0.0), axis=0, keepdims=True)
            value = dot(hot, values)[0:1]
            opened = silu(dot(hot, sgate_ref[k])[0:1])
            slocal_ref[k : k + 1, :] = (local + skip_ref[0:1, :] * value) * opened
            sgain_ref[k : k + 1, :] = decay * opened
            picked_ref[k : k + 1, :] = row[0:1].astype(BF16)

    state_ref[...] = jnp.zeros_like(state_ref)
    offset_ref[...] = jnp.zeros_like(offset_ref)
    for copy in late_copies:
        copy.wait()
    for k in range((n + 1) // 2):
        for d in sorted({n - 1 - k, k}, reverse=True):
            tile_copy(d).start()

    def block_local(b, hook):
        span = pl.ds(pl.multiple_of(b * BLOCK, BLOCK), BLOCK)
        steps, logs = steps_ref[b], logs_ref[b]
        i, j = square(BLOCK)
        lower = jnp.where(i >= j, 1.0, 0.0)
        running = dot(logs, lower, ((1,), (1,)), EXACT)
        running_t = turn_over(running)
        after = turn_over(dot(logs, jnp.where(i > j, 1.0, 0.0), precision=EXACT))
        turned = turn_over(steps)
        expander = expander_ref[...]
        inject = inject_ref[span, :]
        readout = read_ref[span, :]
        scores = jnp.where(i >= j, dot(readout, inject, ((1,), (1,))), 0.0)
        per = LANES // dim
        lane = lax.broadcasted_iota(jnp.int32, (BLOCK, LANES), 1)
        for k in range(heads // per):
            cut = slice(k * LANES, (k + 1) * LANES)
            pair = values_ref[span, cut]
            mixes, parts = [], []
            for q in range(per):
                h = k * per + q
                gap = jnp.minimum(running_t[:, h : h + 1] - running[h : h + 1, :], 0.0)
                mixes.append((scores * jnp.exp(gap) * steps[h : h + 1, :]).astype(BF16))
                parts.append(jnp.where(lane // dim == q, pair, jnp.zeros_like(pair)))
            part_ref[:, cut] = dot(jnp.concatenate(mixes, axis=1), jnp.concatenate(parts, axis=0))
            if hook is not None and 2 * (k + 1) == heads // per:
                hook(HOOKS * b)
        if hook is not None:
            hook(HOOKS * b + 1)
        decay = spread(jnp.exp(running_t), expander)
        values = values_ref[span, :].astype(F32)
        opened = silu(gate_ref[span, :].astype(F32))
        total = part_ref[...] + skip_ref[0:1, :] * values
        total = total + dot(readout, state_ref[...].astype(BF16)) * decay
        normed_ref[span, :] = (total * opened).astype(BF16)
        if hook is not None:
            hook(HOOKS * b + 2)
        offset = offset_ref[0:1, :]
        gain_ref[span, :] = (opened * spread(jnp.exp(running_t + offset), expander)).astype(BF16)
        offset_ref[0:1, :] = offset + running_t[BLOCK - 1 : BLOCK, :]
        scaled = (spread(jnp.exp(after) * turned, expander) * values).astype(BF16)
        state_ref[...] = state_ref[...] * decay[BLOCK - 1 : BLOCK, :] + dot(
            inject, scaled, ((0,), (0,))
        )
        if hook is not None:
            hook(HOOKS * b + 3)

    def hook(g):
        if squared:
            if g in (0, 1, 3):
                run_events(row == 0, square_events()[0][g - g // 3 : g - g // 3 + 1])
            return

        for s in range(2, levels + 1):

            @pl.when(g == s - 1)
            def _():
                exchange_logs(s)

        for s in range(1, levels + 1):
            c = g - LAG * (s - 1)

            @pl.when((c >= 0) & (c < chunks))
            def _():
                scan_step(s, c)

    def picked_copy(p):
        return remote(
            picked_ref, picked_all.at[p], small_ssems.at[0], picked_sems.at[p], {"ctx": last_seat}
        )

    def reply_copy(p):
        return remote(
            reply_ref.at[p], reply_got, reply_sems.at[p], small_rsems.at[0], {"ctx": p}
        )

    def late_round(g, carry):
        hook(g)
        return carry

    block_local(0, hook)
    if squared:
        first, second = square_events()
        run_events(row == 0, first[HOOKS - 1 :])
        run_events(row == 1, second)
    else:
        lax.fori_loop(HOOKS, max(chunks + LAG * (levels - 1), HOOKS), late_round, 0)
    for c in range(chunks):
        swap_copy(c, other_rows).wait_recv()
    for d in range(n):
        tile_copy(d).wait()

    def share(rows, d):
        return dot(normed_ref[rows, :], tiles_ref[d])

    def hop_up(d, b):
        return remote(
            sent.at[d, b],
            landing.at[d + 1, b],
            sent_sems.at[d, b],
            land_sems.at[d + 1, b],
            {"head": place + 1},
        )

    def hop_down(d, b):
        return remote(
            sent.at[d, b],
            landing.at[d, b],
            sent_sems.at[d, b],
            land_sems.at[d, b],
            {"head": place - 1},
        )

    def shop_up(d):
        return remote(
            ssent.at[d],
            slanding.at[d + 1],
            ssent_sems.at[d],
            sland_sems.at[d + 1],
            {"head": place + 1},
        )

    def shop_down(d):
        return remote(
            ssent.at[d], slanding.at[d], ssent_sems.at[d], sland_sems.at[d], {"head": place - 1}
        )

    def rows_of(b):
        return pl.ds(pl.multiple_of(b * BLOCK, BLOCK), BLOCK)

    def pass_on(d, b, slot, move, fed):
        acc_ref[...] = share(rows_of(b), d)

        @pl.when(fed)
        def _():
            move(d, b).wait_recv()
            acc_ref[...] = acc_ref[...] + landing[slot, b].astype(F32)

        sent[d, b] = acc_ref[...].astype(BF16)
        move(d, b).start()

    def finish_block(b):
        span = rows_of(b)
        readout = read_ref[span, :]
        pieces = []
        for c in range(chunks):
            arrival = dot(readout, enter_ref[c])
            piece = normed_ref[span, lanes_of(c)].astype(F32)
            pieces.append(piece + arrival * gain_ref[span, lanes_of(c)].astype(F32))
        normed_ref[span, :] = finish_rows(jnp.concatenate(pieces, axis=1), norm_ref[...])

    padded = slocal_ref.shape[0]
    few_rows = reply_got.shape[0]
    srows = pl.ds(tokens, padded)

    def answer():
        picked_all[last_seat] = picked_ref[...]
        for p in range(peers - 1):
            picked_copy(p).wait_recv()
        asked = picked_all[...].reshape(peers * padded, entries)
        for c in range(chunks):
            final = enter_ref[c].astype(F32) * pair_scale[0:1, lanes_of(c)] + mine_state[c].astype(F32)
            told = dot(asked, final.astype(BF16))
            for p in range(peers - 1):
                reply_ref[p, :, lanes_of(c)] = told[p * padded : p * padded + few_rows]
            own = told[last_seat * padded : last_seat * padded + few_rows]
            reply_got[:, lanes_of(c)] = own
        for p in range(peers - 1):
            reply_copy(p).start()

    def finish_samples():
        @pl.when(jnp.logical_not(holds_final))
        def _():
            reply_copy(0).wait_recv()

        total = slocal_ref[:few_rows] + reply_got[...] * sgain_ref[:few_rows]
        normed = finish_rows(total, norm_ref[...])
        if few_rows < padded:
            normed = jnp.concatenate([normed, jnp.zeros((padded - few_rows, channels), BF16)], axis=0)
        normed_ref[srows, :] = normed

    few = sresult_ref.shape[0]

    def sshare(d):
        wide = share(srows, d)
        return jnp.concatenate([wide[:few, q * LANES : (q + 1) * LANES] for q in range(cols // LANES)], axis=0)

    def spass_on(d, slot, move, fed):
        sown_ref[...] = sshare(d)

        @pl.when(fed)
        def _():
            move(d).wait_recv()
            sown_ref[...] = sown_ref[...] + slanding[slot].astype(F32)

        ssent[d] = sown_ref[...].astype(BF16)
        move(d).start()

    def step(t, carry):
        @pl.when(t < blocks)
        def _():
            finish_block(t)

        @pl.when(t == blocks + 1)
        def _():
            finish_samples()

        rising, falling = t - place, t - (n - 1 - place)
        up, down = n - 1 - rising // blocks, falling // blocks

        @pl.when((rising >= 0) & (up > place))
        def _():
            pass_on(up, rising % blocks, up + 1, hop_up, place > 0)

        @pl.when((falling >= 0) & (down < place))
        def _():
            pass_on(down, falling % blocks, down, hop_down, place < n - 1)

        srising, sfalling = rising - (blocks + 1), falling - (blocks + 1)
        sup, sdown = n - 1 - srising, sfalling

        @pl.when((srising >= 0) & (sup > place))
        def _():
            spass_on(sup, sup + 1, shop_up, place > 0)

        @pl.when((sfalling >= 0) & (sdown < place))
        def _():
            spass_on(sdown, sdown, shop_down, place < n - 1)

        @pl.when(t + 1 < blocks)
        def _():
            block_local(t + 1, None)

        @pl.when(t == blocks - 2)
        def _():
            sample_local()

            @pl.when(jnp.logical_not(holds_final))
            def _():
                picked_copy(seat).start()

        @pl.when((t == blocks - 1) & holds_final)
        def _():
            answer()

        return carry

    lax.fori_loop(0, (n - 1) * blocks, step, 0)
    sown_ref[...] = sshare(place)

    def own(b, carry):
        own_ref[b] = share(rows_of(b), place)
        return carry

    lax.fori_loop(0, blocks, own, 0)

    @pl.when(place < n - 1)
    def _():
        shop_down(place).wait_recv()
        sown_ref[...] = sown_ref[...] + slanding[place].astype(F32)

    @pl.when(place > 0)
    def _():
        shop_up(place).wait_recv()
        sown_ref[...] = sown_ref[...] + slanding[place + 1].astype(F32)

    for q in range(cols // LANES):
        sresult_ref[:, q * LANES : (q + 1) * LANES] = sown_ref[q * few : (q + 1) * few, :].astype(BF16)
    sout_copy = pltpu.make_async_copy(sresult_ref, sout_hbm, late_sems.at[len(late)])
    sout_copy.start()

    def drain(t, carry):
        d, b = t // blocks, t % blocks

        @pl.when(d > place)
        def _():
            hop_up(d, b).wait_send()

        @pl.when(d < place)
        def _():
            hop_down(d, b).wait_send()

        return carry

    lax.fori_loop(0, n * blocks, drain, 0)

    def sdrain(d, carry):
        @pl.when(d > place)
        def _():
            shop_up(d).wait_send()

        @pl.when(d < place)
        def _():
            shop_down(d).wait_send()

        return carry

    lax.fori_loop(0, n, sdrain, 0)
    for c in range(chunks):
        pair_copy(c).wait_send()
        swap_copy(c, own_rows).wait_send()
        for s in range(1, scan_steps + 1):

            @pl.when(sends(s, c))
            def _():
                scan_copy(s, c).wait_send()
    for s in range(log_steps):
        log_copy(s).wait_send()

    @pl.when(holds_final)
    def _():
        for p in range(peers - 1):
            reply_copy(p).wait_send()

    @pl.when(jnp.logical_not(holds_final))
    def _():
        picked_copy(seat).wait_send()
    def out_copy(b):
        return pltpu.make_async_copy(
            result_ref.at[b],
            out_hbm.at[:, pl.ds(pl.multiple_of(b * BLOCK, BLOCK), BLOCK)],
            out_sems.at[b],
        )

    def gather(b, carry):
        @pl.when(place < n - 1)
        def _():
            hop_down(place, b).wait_recv()
            own_ref[b] = own_ref[b] + landing[place, b].astype(F32)

        @pl.when(place > 0)
        def _():
            hop_up(place, b).wait_recv()
            own_ref[b] = own_ref[b] + landing[place + 1, b].astype(F32)

        result_ref[b] = turn_over(own_ref[b]).astype(BF16)
        out_copy(b).start()
        return carry

    lax.fori_loop(0, blocks, gather, 0)

    sout_copy.wait()
    for b in range(blocks):
        out_copy(b).wait()


def per_device(
    prompt_values,
    prompt_gate,
    prompt_inject,
    prompt_read,
    prompt_step,
    decay_log,
    skip_gain,
    norm_weight,
    out_weight,
    sample_values,
    sample_gate,
    sample_inject,
    sample_read,
    sample_step,
    sample_length,
):
    n, peers = lax.axis_size("head"), lax.axis_size("ctx")
    levels = peers.bit_length() - 2
    scan_steps = 3 if levels == 2 else levels
    tokens, channels = prompt_values.shape
    heads = prompt_step.shape[0]
    dim = channels // heads
    entries = prompt_inject.shape[2]
    half = entries // 2
    samples, length = sample_values.shape[:2]
    padded = -(-samples // (2 * PAD)) * 2 * PAD
    cols = out_weight.shape[1] // n
    blocks, chunks = tokens // BLOCK, channels // CHUNK
    vmem = pl.BlockSpec(memory_space=pltpu.VMEM)
    hbm = pl.BlockSpec(memory_space=pl.ANY)
    dma = pltpu.SemaphoreType.DMA
    shape = jax.ShapeDtypeStruct
    V = pltpu.VMEM
    mixed, smixed = pl.pallas_call(
        functools.partial(layer_kernel, dim, n, peers),
        out_shape=(shape((cols, tokens), BF16), shape((samples, cols), BF16)),
        in_specs=[
            pl.BlockSpec(memory_space=pltpu.SMEM),
            hbm,
            hbm,
            vmem,
            hbm,
            vmem,
            vmem,
            vmem,
            vmem,
            hbm,
            hbm,
            hbm,
            hbm,
            hbm,
            hbm,
        ],
        out_specs=(hbm, hbm),
        scratch_shapes=[
            V((tokens, channels), BF16),
            V((tokens, channels), BF16),
            V((tokens, entries), BF16),
            V(sample_values.shape, BF16),
            V(sample_gate.shape, BF16),
            V((samples, length, entries), BF16),
            V((samples, length, entries), BF16),
            V((samples, length, heads), F32),
            V((n, channels, cols), BF16),
            V((blocks, heads, BLOCK), F32),
            V((blocks, heads, BLOCK), F32),
            V((tokens, 2 * heads), BF16),
            V((2 * heads, channels), BF16),
            V((entries, tokens), BF16),
            V((PAD, channels), F32),
            V((chunks, entries, CHUNK), BF16),
            V((chunks, half, CHUNK), BF16),
            V((levels + 1, chunks, half, CHUNK), BF16),
            V((scan_steps, chunks, half, CHUNK), BF16),
            V((chunks, half, CHUNK), F32),
            V((chunks, half, CHUNK), BF16),
            V((chunks, entries, CHUNK), BF16),
            V((levels + 1, PAD, heads), F32),
            V((levels + 1, PAD, heads), F32),
            V((PAD, heads), F32),
            V((PAD, channels), F32),
            V((levels, PAD, channels), F32),
            V((entries, channels), F32),
            V((PAD, heads), F32),
            V((BLOCK, channels), F32),
            V((tokens, channels), BF16),
            V((tokens + padded, channels), BF16),
            V((padded, channels), F32),
            V((padded, channels), F32),
            V((padded, entries), BF16),
            V((peers, padded, entries), BF16),
            V((peers - 1, -(-samples // PAD) * PAD, channels), F32),
            V((-(-samples // PAD) * PAD, channels), F32),
            V((BLOCK, cols), F32),
            V((blocks, BLOCK, cols), F32),
            V((n, blocks, BLOCK, cols), BF16),
            V((n + 1, blocks, BLOCK, cols), BF16),
            V((n, samples * cols // LANES, LANES), BF16),
            V((n + 1, samples * cols // LANES, LANES), BF16),
            V((samples * cols // LANES, LANES), F32),
            V((blocks, cols, BLOCK), BF16),
            V((samples, cols), BF16),
            dma((chunks,)),
            dma((8,)),
            dma((n,)),
            dma((blocks,)),
            dma((levels + 1,)),
            dma((levels + 1,)),
            dma((chunks,)),
            dma((chunks,)),
            dma((scan_steps, chunks)),
            dma((scan_steps, chunks)),
            dma((chunks,)),
            dma((chunks,)),
            dma((1,)),
            dma((1,)),
            dma((peers,)),
            dma((peers,)),
            dma((n, blocks)),
            dma((n + 1, blocks)),
            dma((n,)),
            dma((n + 1,)),
        ],
        compiler_params=pltpu.CompilerParams(
            collective_id=0, has_side_effects=True, vmem_limit_bytes=VMEM_LIMIT
        ),
    )(
        sample_length,
        prompt_values,
        prompt_gate,
        prompt_inject.reshape(tokens, entries),
        prompt_read.reshape(tokens, entries),
        prompt_step,
        decay_log[None],
        skip_gain[None],
        norm_weight[None],
        out_weight,
        sample_values,
        sample_gate,
        sample_inject.reshape(samples, length, entries),
        sample_read.reshape(samples, length, entries),
        sample_step.transpose(1, 2, 0),
    )
    return mixed, smixed.T


def solution(mesh):
    in_specs = (
        P("ctx", "head"),
        P("ctx", "head"),
        P("ctx", "head", None),
        P("ctx", "head", None),
        P("head", "ctx"),
        P("head"),
        P("head"),
        P("head"),
        P("head", None),
        P("ctx", None, "head"),
        P("ctx", None, "head"),
        P("ctx", None, "head", None),
        P("ctx", None, "head", None),
        P("head", "ctx", None),
        P("ctx"),
    )
    out_specs = (P("head", "ctx"), P("head", "ctx"))
    return jax.shard_map(
        per_device, mesh=mesh, in_specs=in_specs, out_specs=out_specs, check_vma=False
    )
```

```python
import functools

import jax
import jax.numpy as jnp
from jax import lax
from jax.experimental import pallas as pl
from jax.experimental.pallas import tpu as pltpu
from jax.sharding import PartitionSpec as P

BLOCK = 128
LANES = 128
PAD = 8
F32 = jnp.float32
BF16 = jnp.bfloat16
EXACT = lax.Precision.HIGHEST
VMEM_LIMIT = 60 * 1024 * 1024


def dot(a, b, dims=((1,), (0,)), precision=None):
    return lax.dot_general(a, b, (dims, ((), ())), precision=precision, preferred_element_type=F32)


def softplus(v):
    return jnp.maximum(v, 0.0) + jnp.log1p(jnp.exp(-jnp.abs(v)))


def silu(v):
    return v / (1.0 + jnp.exp(-v))


def spread(w, expander):
    high = w.astype(BF16)
    low = (w - high.astype(F32)).astype(BF16)
    return dot(jnp.concatenate([high, low], axis=1), expander)


def expander_of(heads, dim):
    row = lax.broadcasted_iota(jnp.int32, (2 * heads, heads * dim), 0)
    lane = lax.broadcasted_iota(jnp.int32, (2 * heads, heads * dim), 1)
    head = lane // dim
    return jnp.where((row == head) | (row == head + heads), 1.0, 0.0).astype(BF16)


def square(n):
    return (
        lax.broadcasted_iota(jnp.int32, (n, n), 0),
        lax.broadcasted_iota(jnp.int32, (n, n), 1),
    )


def finish_rows(total, weight):
    mean = jnp.mean(total * total, axis=1, keepdims=True)
    return (total * lax.rsqrt(mean + 1e-05) * weight).astype(BF16)


CHUNK = LANES
GROUP = 4
PARTS = 2
LAG = 3
HOOKS = 4


def turn_over(w):
    return jnp.transpose(w, (1, 0))


def layer_kernel(
    dim,
    n,
    peers,
    length_ref,
    values_hbm,
    gate_hbm,
    inject_ref,
    read_hbm,
    step_ref,
    decay_ref,
    gain_in_ref,
    norm_ref,
    weight_hbm,
    svalues_hbm,
    sgate_hbm,
    sinject_hbm,
    sread_hbm,
    sstep_hbm,
    out_hbm,
    sout_hbm,
    values_ref,
    gate_ref,
    read_ref,
    svalues_ref,
    sgate_ref,
    sinject_ref,
    sread_ref,
    sstep_ref,
    tiles_ref,
    steps_ref,
    logs_ref,
    wide_ref,
    expander_ref,
    turned_ref,
    skip_ref,
    mine_state,
    pair_state,
    totals,
    arrived,
    before_ref,
    swap_ref,
    enter_ref,
    log_sent,
    log_got,
    before_logs,
    pair_scale,
    scale_ref,
    state_ref,
    offset_ref,
    part_ref,
    normed_ref,
    slocal_ref,
    sgain_ref,
    picked_ref,
    picked_all,
    reply_ref,
    reply_got,
    acc_ref,
    sent,
    landing,
    ssent,
    slanding,
    sown_ref,
    result_ref,
    sresult_ref,
    value_sems,
    late_sems,
    tile_sems,
    out_sems,
    log_ssems,
    log_rsems,
    pair_ssems,
    pair_rsems,
    scan_ssems,
    scan_rsems,
    swap_ssems,
    swap_rsems,
    small_ssems,
    small_rsems,
    picked_sems,
    reply_sems,
    sent_sems,
    land_sems,
    ssent_sems,
    sland_sems,
):
    tokens, channels = values_ref.shape
    heads = step_ref.shape[0]
    entries = inject_ref.shape[1]
    half = entries // 2
    cols = weight_hbm.shape[1] // n
    part = acc_ref.shape[1]
    per = sent.shape[1]
    chunks = channels // CHUNK
    blocks = tokens // BLOCK
    levels = peers.bit_length() - 2
    squared = levels == 2
    log_steps = 2 if squared else levels + 1
    scan_steps = arrived.shape[0]
    place = lax.axis_index("head")
    seat = lax.axis_index("ctx")
    side = seat % 2
    odd = side == 1
    own_rows = pl.ds(pl.multiple_of(side * half, half), half)
    other_rows = pl.ds(pl.multiple_of((1 - side) * half, half), half)

    def lanes_of(c):
        return slice(c * CHUNK, (c + 1) * CHUNK)

    def some_lanes(c):
        return pl.ds(pl.multiple_of(c * CHUNK, CHUNK), CHUNK)

    groups = chunks // GROUP

    def group_lanes(q):
        return slice(q * GROUP * CHUNK, (q + 1) * GROUP * CHUNK)

    def value_copy(q):
        lanes = group_lanes(q)
        return pltpu.make_async_copy(values_hbm.at[:, lanes], values_ref.at[:, lanes], value_sems.at[q])

    late = [
        (gate_hbm, gate_ref),
        (read_hbm, read_ref),
        (svalues_hbm, svalues_ref),
        (sgate_hbm, sgate_ref),
        (sinject_hbm, sinject_ref),
        (sread_hbm, sread_ref),
        (sstep_hbm, sstep_ref),
    ]
    late_copies = [pltpu.make_async_copy(*refs, late_sems.at[q]) for q, refs in enumerate(late)]

    def tile_copy(d):
        return pltpu.make_async_copy(
            weight_hbm.at[:, pl.ds(d * cols, cols)], tiles_ref.at[d], tile_sems.at[d]
        )

    for q in range(groups):
        value_copy(q).start()
    for copy in late_copies:
        copy.start()

    def digit(s):
        return (seat // (1 << s)) % 2

    def mate(s):
        return seat + (1 << s) - (2 << s) * digit(s)

    barrier = pltpu.get_barrier_semaphore()

    def greet(device):
        pl.semaphore_signal(
            barrier, inc=1, device_id=device, device_id_type=pl.DeviceIdType.MESH
        )

    for s in range(levels + 1):
        greet({"ctx": mate(s)})

    last_seat = peers - 1
    holds_final = seat == last_seat

    @pl.when(holds_final)
    def _():
        for p in range(peers - 1):
            greet({"ctx": p})

    @pl.when(jnp.logical_not(holds_final))
    def _():
        greet({"ctx": last_seat})

    @pl.when(place > 0)
    def _():
        greet({"head": place - 1})

    @pl.when(place < n - 1)
    def _():
        greet({"head": place + 1})

    rows, lanes = square(heads)
    rate_row = -jnp.exp(decay_ref[...])
    rate = jnp.sum(jnp.where(rows == lanes, rate_row, 0.0), axis=1, keepdims=True)
    steps = softplus(step_ref[...])
    logs = steps * rate
    i, j = square(BLOCK)

    def fill_expander():
        expander_ref[...] = expander_of(heads, dim)

    fill_expander()
    later = jnp.zeros((heads, 1), F32)
    for b in reversed(range(blocks)):
        span = slice(b * BLOCK, (b + 1) * BLOCK)
        steps_ref[b] = steps[:, span]
        logs_ref[b] = logs[:, span]
        after = dot(logs[:, span], jnp.where(i > j, 1.0, 0.0), precision=EXACT) + later
        later = later + jnp.sum(logs[:, span], axis=1, keepdims=True)
        w = turn_over(jnp.exp(after) * steps[:, span])
        high = w.astype(BF16)
        low = (w - high.astype(F32)).astype(BF16)
        wide_ref[span, :] = jnp.concatenate([high, low], axis=1)
    total_logs = jnp.sum(jnp.where(rows == lanes, later, 0.0), axis=0, keepdims=True)
    total_logs = jnp.broadcast_to(total_logs, (PAD, heads))

    def turn_inject():
        turned_ref[...] = turn_over(inject_ref[...].astype(F32)).astype(BF16)

    turn_inject()
    top = lax.broadcasted_iota(jnp.int32, (PAD, heads), 0) == 0

    inside = (place > 0) & (place < n - 1)
    log_sent[0] = total_logs
    before_logs[...] = jnp.zeros_like(before_logs)

    def state_of(q):
        lanes = group_lanes(q)
        value_copy(q).wait()
        wide = dot(wide_ref[...], expander_ref[:, lanes])
        scaled = (wide * values_ref[:, lanes].astype(F32)).astype(BF16)
        mine_state[:, lanes] = dot(turned_ref[...], scaled).astype(BF16)

    state_of(0)

    for middle in (False, True):
        for final in (False, True):

            @pl.when((inside == middle) & (holds_final == final))
            def _():
                pl.semaphore_wait(barrier, levels + 2 + middle + (peers - 1 if final else 1))

    def remote(src, dst, ssem, rsem, device):
        return pltpu.make_async_remote_copy(
            src_ref=src,
            dst_ref=dst,
            send_sem=ssem,
            recv_sem=rsem,
            device_id=device,
            device_id_type=pl.DeviceIdType.MESH,
        )

    def log_copy(s):
        return remote(
            log_sent.at[s], log_got.at[s], log_ssems.at[s], log_rsems.at[s], {"ctx": mate(s)}
        )

    def pair_copy(c):
        return remote(
            mine_state.at[other_rows, some_lanes(c)],
            pair_state.at[c],
            pair_ssems.at[c],
            pair_rsems.at[c],
            {"ctx": mate(0)},
        )

    def scan_copy(s, c):
        return remote(
            totals.at[s - 1, c],
            arrived.at[s - 1, c],
            scan_ssems.at[s - 1, c],
            scan_rsems.at[s - 1, c],
            {"ctx": mate(1 if squared and s == 3 else s)},
        )

    def swap_copy(c, where):
        return remote(
            swap_ref.at[c],
            enter_ref.at[where, some_lanes(c)],
            swap_ssems.at[c],
            swap_rsems.at[c],
            {"ctx": mate(0)},
        )

    log_copy(0).start()

    def exchange_logs(s):
        log_copy(s).wait_recv()
        got, own = log_got[s], log_sent[s]
        upper = digit(s) == 1
        above = jnp.where(upper, own, got)
        if s == 0:
            pair = jnp.where(top, above, jnp.where(odd, got, own))
            pair_scale[...] = spread(jnp.exp(pair), expander_ref[...])
        else:
            held = before_logs[...]
            crossed = jnp.where(digit(2) == 1, jnp.where(upper, got, own), above) if squared else above
            scale_ref[s - 1] = spread(jnp.exp(jnp.where(top, crossed, held)), expander_ref[...])
            before_logs[...] = held + jnp.where(upper, got, 0.0)
        if s < log_steps - 1:
            log_sent[s + 1] = own + got
            log_copy(s + 1).start()

    column, row = digit(1), digit(2)

    def at_once(c):
        if not squared:
            return seat >= 0
        if c % 2:
            return column == 0
        return (column == 1) & (row == 0)

    def sends(s, c):
        if not squared:
            return seat >= 0
        if s == 1:
            return column == 0 if c % 2 else row == 0
        return (column == c % 2) & (row == s - 2)

    def pair_up(c):
        pair_copy(c).wait_recv()
        mine = mine_state[own_rows, lanes_of(c)].astype(F32)
        theirs = pair_state[c].astype(F32)
        first, second = jnp.where(odd, theirs, mine), jnp.where(odd, mine, theirs)
        totals[0, c] = (first * pair_scale[0:1, lanes_of(c)] + second).astype(BF16)

        @pl.when(at_once(c))
        def _():
            scan_copy(1, c).start()

    pairs = chunks // 2

    def group_order(q):
        return sorted(range(q * GROUP, (q + 1) * GROUP), key=lambda c: 1 - c % 2)

    for q in range(groups):
        if q:
            state_of(q)
        for c in group_order(q):
            pair_copy(c).start()
        if q == 1:
            exchange_logs(0)
        if q > 1:
            for c in group_order(q - 2):
                pair_up(c)
    for q in range(groups - 2, groups):
        for c in group_order(q):
            pair_up(c)
    if squared:
        for c in range(0, chunks, 2):

            @pl.when((column == 0) & (row == 0))
            def _():
                scan_copy(1, c).start()

    def enter(c, before):
        even_state = jnp.where(odd, pair_state[c].astype(F32), mine_state[own_rows, some_lanes(c)].astype(F32))
        moved = before * pair_scale[1:2, some_lanes(c)] + even_state
        enter_ref[own_rows, some_lanes(c)] = jnp.where(odd, moved, before).astype(BF16)
        swap_ref[c] = jnp.where(odd, before, moved).astype(BF16)
        swap_copy(c, own_rows).start()

    def cross_row(q):
        c = 2 * q + column
        scan_copy(1, c).wait_recv()
        far, near = arrived[0, c].astype(F32), totals[0, c].astype(F32)
        right = column == 1
        first, second = jnp.where(right, far, near), jnp.where(right, near, far)
        totals[1, c] = (first * scale_ref[0, 0:1, some_lanes(c)] + second).astype(BF16)
        scan_copy(2, c).start()
        enter(c, jnp.where(right, far, 0.0))

        @pl.when(column == 0)
        def _():
            enter(c + 1, jnp.zeros((half, CHUNK), F32))

    def end_row(q):
        @pl.when(column == 1)
        def _():
            scan_copy(1, 2 * q).wait_recv()
            enter(2 * q, arrived[0, 2 * q].astype(F32))

    def next_row(q):
        c = 2 * q + column
        right = column == 1

        @pl.when(right)
        def _():
            scan_copy(1, c).wait_recv()
            totals[0, c] = arrived[0, c]

        scan_copy(2, c).wait_recv()
        far = arrived[1, c].astype(F32)
        joined = far * scale_ref[0, 0:1, some_lanes(c)] + totals[0, c].astype(F32)
        totals[2, c] = jnp.where(right, far, joined).astype(BF16)
        scan_copy(3, c).start()
        enter(c, jnp.where(right, joined, far))

    def last_column(q):
        c = 2 * q + 1 - column
        scan_copy(3, c).wait_recv()
        enter(c, arrived[2, c].astype(F32))

    def square_events():
        first = [(q, cross_row, q) for q in range(pairs)]
        first += [(q + pairs, end_row, q) for q in range(pairs)]
        second = [(q, next_row, q) for q in range(pairs)]
        second += [(q + 4.5, last_column, q) for q in range(pairs)]
        return [sorted(events, key=lambda event: event[0]) for events in (first, second)]

    def run_events(here, events):
        @pl.when(here)
        def _():
            for _, work, q in events:
                work(q)

    def scan_step(s, c):
        scan_copy(s, c).wait_recv()
        upper = digit(s) == 1
        far = arrived[s - 1, c].astype(F32)
        near = totals[s - 1, c].astype(F32)
        first, second = jnp.where(upper, far, near), jnp.where(upper, near, far)
        total_scale = scale_ref[s - 1, 0:1, some_lanes(c)]
        totals[s, c] = (first * total_scale + second).astype(BF16)
        if s == 1:
            before = jnp.where(upper, far, 0.0)
        else:
            held = before_ref[c]
            before = jnp.where(upper, far * scale_ref[s - 1, 1:2, some_lanes(c)] + held, held)
        if s < levels:
            before_ref[c] = before
            scan_copy(s + 1, c).start()
        else:
            enter(c, before)

    exchange_logs(1)

    skip_ref[...] = spread(jnp.broadcast_to(gain_in_ref[...], (PAD, heads)), expander_ref[...])

    def sample_local():
        samples, length = svalues_ref.shape[:2]
        slocal_ref[...] = jnp.zeros_like(slocal_ref)
        sgain_ref[...] = jnp.zeros_like(sgain_ref)
        picked_ref[...] = jnp.zeros_like(picked_ref)
        u, s = square(length)
        own = lax.broadcasted_iota(jnp.int32, (heads, channels), 1) // dim == (
            lax.broadcasted_iota(jnp.int32, (heads, channels), 0)
        )
        at = lax.broadcasted_iota(jnp.int32, (1, length), 1)
        for k in range(samples):
            last = length_ref[k] - 1
            hot = jnp.where(
                lax.broadcasted_iota(jnp.int32, (PAD, length), 1) == last, 1.0, 0.0
            ).astype(BF16)
            tall = softplus(sstep_ref[k])
            tall_logs = tall * rate_row
            flip = ((0,), (0,))
            gap = dot(tall_logs, jnp.where((u > s) & (u <= last), 1.0, 0.0), flip, EXACT)
            running = dot(tall_logs, jnp.where(u <= last, 1.0, 0.0), flip, EXACT)[:, 0:1]
            wide_steps = dot(tall, jnp.where(u == s, 1.0, 0.0), flip, EXACT)
            row = dot(hot, sread_ref[k])
            score = dot(row.astype(BF16), sinject_ref[k], ((1,), (1,)))[0:1]
            mixing = jnp.where(at <= last, score * jnp.exp(gap) * wide_steps, 0.0).astype(BF16)
            values = svalues_ref[k]
            local = jnp.sum(jnp.where(own, dot(mixing, values), 0.0), axis=0, keepdims=True)
            decay = jnp.sum(jnp.where(own, jnp.exp(running), 0.0), axis=0, keepdims=True)
            value = dot(hot, values)[0:1]
            opened = silu(dot(hot, sgate_ref[k])[0:1])
            slocal_ref[k : k + 1, :] = (local + skip_ref[0:1, :] * value) * opened
            sgain_ref[k : k + 1, :] = decay * opened
            picked_ref[k : k + 1, :] = row[0:1].astype(BF16)

    state_ref[...] = jnp.zeros_like(state_ref)
    offset_ref[...] = jnp.zeros_like(offset_ref)
    for copy in late_copies:
        copy.wait()
    for k in range((n + 1) // 2):
        for d in sorted({n - 1 - k, k}, reverse=True):
            tile_copy(d).start()

    def block_local(b, hook):
        span = pl.ds(pl.multiple_of(b * BLOCK, BLOCK), BLOCK)
        steps, logs = steps_ref[b], logs_ref[b]
        i, j = square(BLOCK)
        lower = jnp.where(i >= j, 1.0, 0.0)
        running = dot(logs, lower, ((1,), (1,)), EXACT)
        running_t = turn_over(running)
        after = turn_over(dot(logs, jnp.where(i > j, 1.0, 0.0), precision=EXACT))
        turned = turn_over(steps)
        expander = expander_ref[...]
        inject = inject_ref[span, :]
        readout = read_ref[span, :]
        scores = jnp.where(i >= j, dot(readout, inject, ((1,), (1,))), 0.0)
        per = LANES // dim
        lane = lax.broadcasted_iota(jnp.int32, (BLOCK, LANES), 1)
        for k in range(heads // per):
            cut = slice(k * LANES, (k + 1) * LANES)
            pair = values_ref[span, cut]
            mixes, parts = [], []
            for q in range(per):
                h = k * per + q
                gap = jnp.minimum(running_t[:, h : h + 1] - running[h : h + 1, :], 0.0)
                mixes.append((scores * jnp.exp(gap) * steps[h : h + 1, :]).astype(BF16))
                parts.append(jnp.where(lane // dim == q, pair, jnp.zeros_like(pair)))
            part_ref[:, cut] = dot(jnp.concatenate(mixes, axis=1), jnp.concatenate(parts, axis=0))
            if hook is not None and 2 * (k + 1) == heads // per:
                hook(HOOKS * b)
        if hook is not None:
            hook(HOOKS * b + 1)
        decay = spread(jnp.exp(running_t), expander)
        values = values_ref[span, :].astype(F32)
        opened = silu(gate_ref[span, :].astype(F32))
        total = part_ref[...] + skip_ref[0:1, :] * values
        total = total + dot(readout, state_ref[...].astype(BF16)) * decay
        normed_ref[span, :] = (total * opened).astype(BF16)
        if hook is not None:
            hook(HOOKS * b + 2)
        offset = offset_ref[0:1, :]
        gate_ref[span, :] = (opened * spread(jnp.exp(running_t + offset), expander)).astype(BF16)
        offset_ref[0:1, :] = offset + running_t[BLOCK - 1 : BLOCK, :]
        scaled = (spread(jnp.exp(after) * turned, expander) * values).astype(BF16)
        state_ref[...] = state_ref[...] * decay[BLOCK - 1 : BLOCK, :] + dot(
            inject, scaled, ((0,), (0,))
        )
        if hook is not None:
            hook(HOOKS * b + 3)

    def hook(g):
        if squared:
            run_events(row == 0, square_events()[0][g : g + 1])
            return

        for s in range(2, levels + 1):

            @pl.when(g == s - 1)
            def _():
                exchange_logs(s)

        for s in range(1, levels + 1):
            c = g - LAG * (s - 1)

            @pl.when((c >= 0) & (c < chunks))
            def _():
                scan_step(s, c)

    def picked_copy(p):
        return remote(
            picked_ref, picked_all.at[p], small_ssems.at[0], picked_sems.at[p], {"ctx": last_seat}
        )

    def reply_copy(p):
        return remote(
            reply_ref.at[p], reply_got, reply_sems.at[p], small_rsems.at[0], {"ctx": p}
        )

    def late_round(g, carry):
        hook(g)
        return carry

    block_local(0, hook)
    if squared:
        first, second = square_events()
        run_events(row == 0, first[HOOKS:])
        run_events(row == 1, second)
    else:
        lax.fori_loop(HOOKS, max(chunks + LAG * (levels - 1), HOOKS), late_round, 0)
    for c in range(chunks):
        swap_copy(c, other_rows).wait_recv()
    for d in range(n):
        tile_copy(d).wait()

    def share(d, q):
        rows = rows_of(q // PARTS)
        return dot(normed_ref[rows, :], tiles_ref[d, :, pl.ds(pl.multiple_of(q % PARTS * part, part), part)])

    def hop_up(d, b):
        return remote(
            sent.at[d, b],
            landing.at[d + 1, b],
            sent_sems.at[d, b],
            land_sems.at[d + 1, b],
            {"head": place + 1},
        )

    def hop_down(d, b):
        return remote(
            sent.at[d, b],
            landing.at[d, b],
            sent_sems.at[d, b],
            land_sems.at[d, b],
            {"head": place - 1},
        )

    def shop_up(d):
        return remote(
            ssent.at[d],
            slanding.at[d + 1],
            ssent_sems.at[d],
            sland_sems.at[d + 1],
            {"head": place + 1},
        )

    def shop_down(d):
        return remote(
            ssent.at[d], slanding.at[d], ssent_sems.at[d], sland_sems.at[d], {"head": place - 1}
        )

    def rows_of(b):
        return pl.ds(pl.multiple_of(b * BLOCK, BLOCK), BLOCK)

    def pass_on(d, b, slot, move, fed):
        acc_ref[...] = share(d, b)

        @pl.when(fed)
        def _():
            move(d, b).wait_recv()
            acc_ref[...] = acc_ref[...] + landing[slot, b].astype(F32)

        sent[d, b] = acc_ref[...].astype(BF16)
        move(d, b).start()

    def finish_block(b):
        span = rows_of(b)
        readout = read_ref[span, :]
        pieces = []
        for q in range(groups):
            lanes = group_lanes(q)
            arrival = dot(readout, enter_ref[:, lanes])
            piece = normed_ref[span, lanes].astype(F32)
            pieces.append(piece + arrival * gate_ref[span, lanes].astype(F32))
        normed_ref[span, :] = finish_rows(jnp.concatenate(pieces, axis=1), norm_ref[...])

    padded = slocal_ref.shape[0]
    few_rows = reply_got.shape[0]
    srows = pl.ds(tokens, padded)

    def answer():
        picked_all[last_seat] = picked_ref[...]
        for p in range(peers - 1):
            picked_copy(p).wait_recv()
        asked = picked_all[...].reshape(peers * padded, entries)
        for q in range(groups):
            lanes = group_lanes(q)
            entered = enter_ref[:, lanes].astype(F32) * pair_scale[0:1, lanes]
            final = entered + mine_state[:, lanes].astype(F32)
            told = dot(asked, final.astype(BF16))
            for p in range(peers - 1):
                reply_ref[p, :, lanes] = told[p * padded : p * padded + few_rows]
            reply_got[:, lanes] = told[last_seat * padded : last_seat * padded + few_rows]
        for p in range(peers - 1):
            reply_copy(p).start()

    def finish_samples():
        @pl.when(jnp.logical_not(holds_final))
        def _():
            reply_copy(0).wait_recv()

        total = slocal_ref[:few_rows] + reply_got[...] * sgain_ref[:few_rows]
        normed = finish_rows(total, norm_ref[...])
        if few_rows < padded:
            normed = jnp.concatenate([normed, jnp.zeros((padded - few_rows, channels), BF16)], axis=0)
        normed_ref[srows, :] = normed

    few = sresult_ref.shape[0]

    def sshare(d):
        wide = dot(normed_ref[srows, :], tiles_ref[d])
        return jnp.concatenate([wide[:few, q * LANES : (q + 1) * LANES] for q in range(cols // LANES)], axis=0)

    def spass_on(d, slot, move, fed):
        sown_ref[...] = sshare(d)

        @pl.when(fed)
        def _():
            move(d).wait_recv()
            sown_ref[...] = sown_ref[...] + slanding[slot].astype(F32)

        ssent[d] = sown_ref[...].astype(BF16)
        move(d).start()

    sample_start = PARTS * (blocks + 1)

    def step(t, carry):
        block, first_part, last_part = t // PARTS, t % PARTS == 0, t % PARTS == PARTS - 1

        @pl.when((block < blocks) & first_part)
        def _():
            finish_block(block)

        @pl.when(t == sample_start)
        def _():
            finish_samples()

        rising, falling = t - place, t - (n - 1 - place)
        up, down = n - 1 - rising // per, falling // per

        @pl.when((rising >= 0) & (up > place))
        def _():
            pass_on(up, rising % per, up + 1, hop_up, place > 0)

        @pl.when((falling >= 0) & (down < place))
        def _():
            pass_on(down, falling % per, down, hop_down, place < n - 1)

        srising, sfalling = rising - sample_start, falling - sample_start
        sup, sdown = n - 1 - srising, sfalling

        @pl.when((srising >= 0) & (sup > place))
        def _():
            spass_on(sup, sup + 1, shop_up, place > 0)

        @pl.when((sfalling >= 0) & (sdown < place))
        def _():
            spass_on(sdown, sdown, shop_down, place < n - 1)

        @pl.when((block + 1 < blocks) & last_part)
        def _():
            block_local(block + 1, None)

        @pl.when((block == blocks - 2) & last_part)
        def _():
            sample_local()

            @pl.when(jnp.logical_not(holds_final))
            def _():
                picked_copy(seat).start()

        @pl.when((block == blocks - 1) & last_part & holds_final)
        def _():
            answer()

        return carry

    lax.fori_loop(0, (n - 1) * per, step, 0)
    sown_ref[...] = sshare(place)

    @pl.when(place < n - 1)
    def _():
        shop_down(place).wait_recv()
        sown_ref[...] = sown_ref[...] + slanding[place].astype(F32)

    @pl.when(place > 0)
    def _():
        shop_up(place).wait_recv()
        sown_ref[...] = sown_ref[...] + slanding[place + 1].astype(F32)

    for q in range(cols // LANES):
        sresult_ref[:, q * LANES : (q + 1) * LANES] = sown_ref[q * few : (q + 1) * few, :].astype(BF16)
    sout_copy = pltpu.make_async_copy(sresult_ref, sout_hbm, late_sems.at[len(late)])
    sout_copy.start()

    for c in range(chunks):
        pair_copy(c).wait_send()
        swap_copy(c, own_rows).wait_send()
        for s in range(1, scan_steps + 1):

            @pl.when(sends(s, c))
            def _():
                scan_copy(s, c).wait_send()
    for s in range(log_steps):
        log_copy(s).wait_send()

    @pl.when(holds_final)
    def _():
        for p in range(peers - 1):
            reply_copy(p).wait_send()

    @pl.when(jnp.logical_not(holds_final))
    def _():
        picked_copy(seat).wait_send()

    def out_copy(b):
        return pltpu.make_async_copy(
            result_ref.at[b],
            out_hbm.at[pl.ds(pl.multiple_of(b % PARTS * part, part), part), rows_of(b // PARTS)],
            out_sems.at[b],
        )

    def gather(b, carry):
        acc_ref[...] = share(place, b)

        @pl.when(place < n - 1)
        def _():
            hop_down(place, b).wait_recv()
            acc_ref[...] = acc_ref[...] + landing[place, b].astype(F32)

        @pl.when(place > 0)
        def _():
            hop_up(place, b).wait_recv()
            acc_ref[...] = acc_ref[...] + landing[place + 1, b].astype(F32)

        result_ref[b] = turn_over(acc_ref[...]).astype(BF16)
        out_copy(b).start()
        for d in range(n):

            @pl.when(d > place)
            def _():
                hop_up(d, b).wait_send()

            @pl.when(d < place)
            def _():
                hop_down(d, b).wait_send()

        return carry

    lax.fori_loop(0, per, gather, 0)
    for d in range(n):

        @pl.when(d > place)
        def _():
            shop_up(d).wait_send()

        @pl.when(d < place)
        def _():
            shop_down(d).wait_send()

    sout_copy.wait()
    for b in range(per):
        out_copy(b).wait()


def hand_over_kernel(bands, mixed_hbm, smixed_hbm, out_hbm, sout_hbm, bands_ref, few_ref, sems):
    rows = mixed_hbm.shape[0] // bands
    moves = [(smixed_hbm, few_ref, sout_hbm)]
    for q in range(bands):
        part = pl.ds(q * rows, rows)
        moves.append((mixed_hbm.at[part], bands_ref.at[q], out_hbm.at[part]))
    ins = [pltpu.make_async_copy(a, b, sems.at[0, q]) for q, (a, b, _) in enumerate(moves)]
    outs = [pltpu.make_async_copy(b, c, sems.at[1, q]) for q, (_, b, c) in enumerate(moves)]
    for copy in ins:
        copy.start()
    for into, out in zip(ins, outs):
        into.wait()
        out.start()
    for copy in outs:
        copy.wait()


def per_device(
    prompt_values,
    prompt_gate,
    prompt_inject,
    prompt_read,
    prompt_step,
    decay_log,
    skip_gain,
    norm_weight,
    out_weight,
    sample_values,
    sample_gate,
    sample_inject,
    sample_read,
    sample_step,
    sample_length,
):
    n, peers = lax.axis_size("head"), lax.axis_size("ctx")
    levels = peers.bit_length() - 2
    scan_steps = 3 if levels == 2 else levels
    tokens, channels = prompt_values.shape
    heads = prompt_step.shape[0]
    dim = channels // heads
    entries = prompt_inject.shape[2]
    half = entries // 2
    samples, length = sample_values.shape[:2]
    padded = -(-samples // (2 * PAD)) * 2 * PAD
    cols = out_weight.shape[1] // n
    blocks, chunks = tokens // BLOCK, channels // CHUNK
    part, per = cols // PARTS, blocks * PARTS
    vmem = pl.BlockSpec(memory_space=pltpu.VMEM)
    hbm = pl.BlockSpec(memory_space=pl.ANY)
    dma = pltpu.SemaphoreType.DMA
    shape = jax.ShapeDtypeStruct
    V = pltpu.VMEM
    mixed, smixed = pl.pallas_call(
        functools.partial(layer_kernel, dim, n, peers),
        out_shape=(shape((cols, tokens), BF16), shape((samples, cols), BF16)),
        in_specs=[
            pl.BlockSpec(memory_space=pltpu.SMEM),
            hbm,
            hbm,
            vmem,
            hbm,
            vmem,
            vmem,
            vmem,
            vmem,
            hbm,
            hbm,
            hbm,
            hbm,
            hbm,
            hbm,
        ],
        out_specs=(hbm, hbm),
        scratch_shapes=[
            V((tokens, channels), BF16),
            V((tokens, channels), BF16),
            V((tokens, entries), BF16),
            V(sample_values.shape, BF16),
            V(sample_gate.shape, BF16),
            V((samples, length, entries), BF16),
            V((samples, length, entries), BF16),
            V((samples, length, heads), F32),
            V((n, channels, cols), BF16),
            V((blocks, heads, BLOCK), F32),
            V((blocks, heads, BLOCK), F32),
            V((tokens, 2 * heads), BF16),
            V((2 * heads, channels), BF16),
            V((entries, tokens), BF16),
            V((PAD, channels), F32),
            V((entries, channels), BF16),
            V((chunks, half, CHUNK), BF16),
            V((levels + 1, chunks, half, CHUNK), BF16),
            V((scan_steps, chunks, half, CHUNK), BF16),
            V((chunks, half, CHUNK), F32),
            V((chunks, half, CHUNK), BF16),
            V((entries, channels), BF16),
            V((levels + 1, PAD, heads), F32),
            V((levels + 1, PAD, heads), F32),
            V((PAD, heads), F32),
            V((PAD, channels), F32),
            V((levels, PAD, channels), F32),
            V((entries, channels), F32),
            V((PAD, heads), F32),
            V((BLOCK, channels), F32),
            V((tokens + padded, channels), BF16),
            V((padded, channels), F32),
            V((padded, channels), F32),
            V((padded, entries), BF16),
            V((peers, padded, entries), BF16),
            V((peers - 1, -(-samples // PAD) * PAD, channels), F32),
            V((-(-samples // PAD) * PAD, channels), F32),
            V((BLOCK, part), F32),
            V((n, per, BLOCK, part), BF16),
            V((n + 1, per, BLOCK, part), BF16),
            V((n, samples * cols // LANES, LANES), BF16),
            V((n + 1, samples * cols // LANES, LANES), BF16),
            V((samples * cols // LANES, LANES), F32),
            V((per, part, BLOCK), BF16),
            V((samples, cols), BF16),
            dma((chunks,)),
            dma((8,)),
            dma((n,)),
            dma((per,)),
            dma((levels + 1,)),
            dma((levels + 1,)),
            dma((chunks,)),
            dma((chunks,)),
            dma((scan_steps, chunks)),
            dma((scan_steps, chunks)),
            dma((chunks,)),
            dma((chunks,)),
            dma((1,)),
            dma((1,)),
            dma((peers,)),
            dma((peers,)),
            dma((n, per)),
            dma((n + 1, per)),
            dma((n,)),
            dma((n + 1,)),
        ],
        compiler_params=pltpu.CompilerParams(
            collective_id=0, has_side_effects=True, vmem_limit_bytes=VMEM_LIMIT
        ),
    )(
        sample_length,
        prompt_values,
        prompt_gate,
        prompt_inject.reshape(tokens, entries),
        prompt_read.reshape(tokens, entries),
        prompt_step,
        decay_log[None],
        skip_gain[None],
        norm_weight[None],
        out_weight,
        sample_values,
        sample_gate,
        sample_inject.reshape(samples, length, entries),
        sample_read.reshape(samples, length, entries),
        sample_step.transpose(1, 2, 0),
    )
    bands = 4
    band = (cols // bands, tokens)
    mixed, smixed = pl.pallas_call(
        functools.partial(hand_over_kernel, bands),
        out_shape=(shape((cols, tokens), BF16), shape((samples, cols), BF16)),
        in_specs=[hbm, hbm],
        out_specs=(hbm, hbm),
        scratch_shapes=[
            V((bands, *band), BF16),
            V((samples, cols), BF16),
            dma((2, bands + 1)),
        ],
    )(mixed, smixed)
    return mixed, smixed.T


def solution(mesh):
    in_specs = (
        P("ctx", "head"),
        P("ctx", "head"),
        P("ctx", "head", None),
        P("ctx", "head", None),
        P("head", "ctx"),
        P("head"),
        P("head"),
        P("head"),
        P("head", None),
        P("ctx", None, "head"),
        P("ctx", None, "head"),
        P("ctx", None, "head", None),
        P("ctx", None, "head", None),
        P("head", "ctx", None),
        P("ctx"),
    )
    out_specs = (P("head", "ctx"), P("head", "ctx"))
    return jax.shard_map(
        per_device, mesh=mesh, in_specs=in_specs, out_specs=out_specs, check_vma=False
    )
```

```python
import functools

import jax
import jax.numpy as jnp
from jax import lax
from jax.experimental import pallas as pl
from jax.experimental.pallas import tpu as pltpu
from jax.sharding import PartitionSpec as P

BLOCK = 128
LANES = 128
PAD = 8
F32 = jnp.float32
BF16 = jnp.bfloat16
EXACT = lax.Precision.HIGHEST
VMEM_LIMIT = 60 * 1024 * 1024


def dot(a, b, dims=((1,), (0,)), precision=None):
    return lax.dot_general(a, b, (dims, ((), ())), precision=precision, preferred_element_type=F32)


def softplus(v):
    return jnp.maximum(v, 0.0) + jnp.log1p(jnp.exp(-jnp.abs(v)))


def silu(v):
    return v / (1.0 + jnp.exp(-v))


def spread(w, expander):
    high = w.astype(BF16)
    low = (w - high.astype(F32)).astype(BF16)
    return dot(jnp.concatenate([high, low], axis=1), expander)


def expander_of(heads, dim):
    row = lax.broadcasted_iota(jnp.int32, (2 * heads, heads * dim), 0)
    lane = lax.broadcasted_iota(jnp.int32, (2 * heads, heads * dim), 1)
    head = lane // dim
    return jnp.where((row == head) | (row == head + heads), 1.0, 0.0).astype(BF16)


def square(n):
    return (
        lax.broadcasted_iota(jnp.int32, (n, n), 0),
        lax.broadcasted_iota(jnp.int32, (n, n), 1),
    )


def finish_rows(total, weight):
    mean = jnp.mean(total * total, axis=1, keepdims=True)
    return (total * lax.rsqrt(mean + 1e-05) * weight).astype(BF16)


CHUNK = LANES
GROUP = 4
PARTS = 2
LAG = 3
HOOKS = 4


def turn_over(w):
    return jnp.transpose(w, (1, 0))


def layer_kernel(
    dim,
    n,
    peers,
    length_ref,
    values_hbm,
    gate_hbm,
    inject_ref,
    read_hbm,
    step_ref,
    decay_ref,
    gain_in_ref,
    norm_ref,
    weight_hbm,
    svalues_hbm,
    sgate_hbm,
    sinject_hbm,
    sread_hbm,
    sstep_hbm,
    out_hbm,
    sout_hbm,
    values_ref,
    gate_ref,
    read_ref,
    svalues_ref,
    sgate_ref,
    sinject_ref,
    sread_ref,
    sstep_ref,
    tiles_ref,
    steps_ref,
    logs_ref,
    wide_ref,
    expander_ref,
    turned_ref,
    skip_ref,
    mine_state,
    pair_state,
    totals,
    arrived,
    before_ref,
    swap_ref,
    enter_ref,
    log_sent,
    log_got,
    before_logs,
    pair_scale,
    scale_ref,
    state_ref,
    offset_ref,
    part_ref,
    normed_ref,
    slocal_ref,
    sgain_ref,
    picked_ref,
    picked_all,
    reply_ref,
    reply_got,
    acc_ref,
    sent,
    landing,
    ssent,
    slanding,
    sown_ref,
    result_ref,
    sresult_ref,
    value_sems,
    late_sems,
    tile_sems,
    out_sems,
    log_ssems,
    log_rsems,
    pair_ssems,
    pair_rsems,
    scan_ssems,
    scan_rsems,
    swap_ssems,
    swap_rsems,
    small_ssems,
    small_rsems,
    picked_sems,
    reply_sems,
    sent_sems,
    land_sems,
    ssent_sems,
    sland_sems,
):
    tokens, channels = values_ref.shape
    heads = step_ref.shape[0]
    entries = inject_ref.shape[1]
    half = entries // 2
    cols = weight_hbm.shape[1] // n
    part = acc_ref.shape[1]
    per = sent.shape[1]
    chunks = channels // CHUNK
    blocks = tokens // BLOCK
    levels = peers.bit_length() - 2
    squared = levels == 2
    log_steps = 2 if squared else levels + 1
    scan_steps = arrived.shape[0]
    place = lax.axis_index("head")
    seat = lax.axis_index("ctx")
    side = seat % 2
    odd = side == 1
    own_rows = pl.ds(pl.multiple_of(side * half, half), half)
    other_rows = pl.ds(pl.multiple_of((1 - side) * half, half), half)

    def lanes_of(c):
        return slice(c * CHUNK, (c + 1) * CHUNK)

    def some_lanes(c):
        return pl.ds(pl.multiple_of(c * CHUNK, CHUNK), CHUNK)

    groups = chunks // GROUP

    def group_lanes(q):
        return slice(q * GROUP * CHUNK, (q + 1) * GROUP * CHUNK)

    def value_copy(q):
        lanes = group_lanes(q)
        return pltpu.make_async_copy(values_hbm.at[:, lanes], values_ref.at[:, lanes], value_sems.at[q])

    late = [
        (gate_hbm, gate_ref),
        (read_hbm, read_ref),
        (svalues_hbm, svalues_ref),
        (sgate_hbm, sgate_ref),
        (sinject_hbm, sinject_ref),
        (sread_hbm, sread_ref),
        (sstep_hbm, sstep_ref),
    ]
    late_copies = [pltpu.make_async_copy(*refs, late_sems.at[q]) for q, refs in enumerate(late)]

    tile_copy = pltpu.make_async_copy(weight_hbm, tiles_ref, tile_sems.at[0])

    for q in range(groups):
        value_copy(q).start()
    for copy in late_copies:
        copy.start()

    def digit(s):
        return (seat // (1 << s)) % 2

    def mate(s):
        return seat + (1 << s) - (2 << s) * digit(s)

    barrier = pltpu.get_barrier_semaphore()

    def greet(device):
        pl.semaphore_signal(
            barrier, inc=1, device_id=device, device_id_type=pl.DeviceIdType.MESH
        )

    for s in range(levels + 1):
        greet({"ctx": mate(s)})

    last_seat = peers - 1
    holds_final = seat == last_seat

    @pl.when(holds_final)
    def _():
        for p in range(peers - 1):
            greet({"ctx": p})

    @pl.when(jnp.logical_not(holds_final))
    def _():
        greet({"ctx": last_seat})

    @pl.when(place > 0)
    def _():
        greet({"head": place - 1})

    @pl.when(place < n - 1)
    def _():
        greet({"head": place + 1})

    rows, lanes = square(heads)
    rate_row = -jnp.exp(decay_ref[...])
    rate = jnp.sum(jnp.where(rows == lanes, rate_row, 0.0), axis=1, keepdims=True)
    steps = softplus(step_ref[...])
    logs = steps * rate
    i, j = square(BLOCK)

    def fill_expander():
        expander_ref[...] = expander_of(heads, dim)

    fill_expander()
    later = jnp.zeros((heads, 1), F32)
    for b in reversed(range(blocks)):
        span = slice(b * BLOCK, (b + 1) * BLOCK)
        steps_ref[b] = steps[:, span]
        logs_ref[b] = logs[:, span]
        after = dot(logs[:, span], jnp.where(i > j, 1.0, 0.0), precision=EXACT) + later
        later = later + jnp.sum(logs[:, span], axis=1, keepdims=True)
        w = turn_over(jnp.exp(after) * steps[:, span])
        high = w.astype(BF16)
        low = (w - high.astype(F32)).astype(BF16)
        wide_ref[span, :] = jnp.concatenate([high, low], axis=1)
    total_logs = jnp.sum(jnp.where(rows == lanes, later, 0.0), axis=0, keepdims=True)
    total_logs = jnp.broadcast_to(total_logs, (PAD, heads))

    def turn_inject():
        turned_ref[...] = turn_over(inject_ref[...].astype(F32)).astype(BF16)

    turn_inject()
    top = lax.broadcasted_iota(jnp.int32, (PAD, heads), 0) == 0

    inside = (place > 0) & (place < n - 1)
    log_sent[0] = total_logs
    before_logs[...] = jnp.zeros_like(before_logs)

    def state_of(q):
        lanes = group_lanes(q)
        value_copy(q).wait()
        wide = dot(wide_ref[...], expander_ref[:, lanes])
        scaled = (wide * values_ref[:, lanes].astype(F32)).astype(BF16)
        mine_state[:, lanes] = dot(turned_ref[...], scaled).astype(BF16)

    state_of(0)

    for middle in (False, True):
        for final in (False, True):

            @pl.when((inside == middle) & (holds_final == final))
            def _():
                pl.semaphore_wait(barrier, levels + 2 + middle + (peers - 1 if final else 1))

    def remote(src, dst, ssem, rsem, device):
        return pltpu.make_async_remote_copy(
            src_ref=src,
            dst_ref=dst,
            send_sem=ssem,
            recv_sem=rsem,
            device_id=device,
            device_id_type=pl.DeviceIdType.MESH,
        )

    def log_copy(s):
        return remote(
            log_sent.at[s], log_got.at[s], log_ssems.at[s], log_rsems.at[s], {"ctx": mate(s)}
        )

    def pair_copy(q):
        return remote(
            mine_state.at[other_rows, group_lanes(q)],
            pair_state.at[:, group_lanes(q)],
            pair_ssems.at[0],
            pair_rsems.at[q],
            {"ctx": mate(0)},
        )

    def scan_copy(s, c):
        return remote(
            totals.at[s - 1, c],
            arrived.at[s - 1, c],
            scan_ssems.at[s - 1],
            scan_rsems.at[s - 1, c],
            {"ctx": mate(1 if squared and s == 3 else s)},
        )

    def swap_copy(lanes, where):
        return remote(
            swap_ref.at[:, lanes],
            enter_ref.at[where, lanes],
            swap_ssems.at[0],
            swap_rsems.at[0],
            {"ctx": mate(0)},
        )

    log_copy(0).start()

    def exchange_logs(s):
        log_copy(s).wait_recv()
        got, own = log_got[s], log_sent[s]
        upper = digit(s) == 1
        above = jnp.where(upper, own, got)
        if s == 0:
            pair = jnp.where(top, above, jnp.where(odd, got, own))
            pair_scale[...] = spread(jnp.exp(pair), expander_ref[...])
        else:
            held = before_logs[...]
            crossed = jnp.where(digit(2) == 1, jnp.where(upper, got, own), above) if squared else above
            scale_ref[s - 1] = spread(jnp.exp(jnp.where(top, crossed, held)), expander_ref[...])
            before_logs[...] = held + jnp.where(upper, got, 0.0)
        if s < log_steps - 1:
            log_sent[s + 1] = own + got
            log_copy(s + 1).start()

    column, row = digit(1), digit(2)

    def at_once(c):
        if not squared:
            return seat >= 0
        if c % 2:
            return column == 0
        return (column == 1) & (row == 0)

    def pair_up(c):
        mine = mine_state[own_rows, lanes_of(c)].astype(F32)
        theirs = pair_state[:, lanes_of(c)].astype(F32)
        first, second = jnp.where(odd, theirs, mine), jnp.where(odd, mine, theirs)
        totals[0, c] = (first * pair_scale[0:1, lanes_of(c)] + second).astype(BF16)

        @pl.when(at_once(c))
        def _():
            scan_copy(1, c).start()

    pairs = chunks // 2

    def pair_group(q):
        pair_copy(q).wait_recv()
        for c in sorted(range(q * GROUP, (q + 1) * GROUP), key=lambda c: 1 - c % 2):
            pair_up(c)

    for q in range(groups):
        if q:
            state_of(q)
        pair_copy(q).start()
        if q == 1:
            exchange_logs(0)
        if q > 1:
            pair_group(q - 2)
    for q in range(groups - 2, groups):
        pair_group(q)
    if squared:
        for c in range(0, chunks, 2):

            @pl.when((column == 0) & (row == 0))
            def _():
                scan_copy(1, c).start()

    def enter(c, before):
        even_state = jnp.where(odd, pair_state[:, some_lanes(c)].astype(F32), mine_state[own_rows, some_lanes(c)].astype(F32))
        moved = before * pair_scale[1:2, some_lanes(c)] + even_state
        enter_ref[own_rows, some_lanes(c)] = jnp.where(odd, moved, before).astype(BF16)
        swap_ref[:, some_lanes(c)] = jnp.where(odd, before, moved).astype(BF16)
        swap_copy(some_lanes(c), own_rows).start()

    def cross_row(q):
        c = 2 * q + column
        scan_copy(1, c).wait_recv()
        far, near = arrived[0, c].astype(F32), totals[0, c].astype(F32)
        right = column == 1
        first, second = jnp.where(right, far, near), jnp.where(right, near, far)
        totals[1, c] = (first * scale_ref[0, 0:1, some_lanes(c)] + second).astype(BF16)
        scan_copy(2, c).start()
        enter(c, jnp.where(right, far, 0.0))

        @pl.when(column == 0)
        def _():
            enter(c + 1, jnp.zeros((half, CHUNK), F32))

    def end_row(q):
        @pl.when(column == 1)
        def _():
            scan_copy(1, 2 * q).wait_recv()
            enter(2 * q, arrived[0, 2 * q].astype(F32))

    def next_row(q):
        c = 2 * q + column
        right = column == 1

        @pl.when(right)
        def _():
            scan_copy(1, c).wait_recv()
            totals[0, c] = arrived[0, c]

        scan_copy(2, c).wait_recv()
        far = arrived[1, c].astype(F32)
        joined = far * scale_ref[0, 0:1, some_lanes(c)] + totals[0, c].astype(F32)
        totals[2, c] = jnp.where(right, far, joined).astype(BF16)
        scan_copy(3, c).start()
        enter(c, jnp.where(right, joined, far))

    def last_column(q):
        c = 2 * q + 1 - column
        scan_copy(3, c).wait_recv()
        enter(c, arrived[2, c].astype(F32))

    def square_events():
        first = [(q, cross_row, q) for q in range(pairs)]
        first += [(q + pairs, end_row, q) for q in range(pairs)]
        second = [(q, next_row, q) for q in range(pairs)]
        second += [(q + 4.5, last_column, q) for q in range(pairs)]
        return [sorted(events, key=lambda event: event[0]) for events in (first, second)]

    def run_events(here, events):
        @pl.when(here)
        def _():
            for _, work, q in events:
                work(q)

    def scan_step(s, c):
        scan_copy(s, c).wait_recv()
        upper = digit(s) == 1
        far = arrived[s - 1, c].astype(F32)
        near = totals[s - 1, c].astype(F32)
        first, second = jnp.where(upper, far, near), jnp.where(upper, near, far)
        total_scale = scale_ref[s - 1, 0:1, some_lanes(c)]
        totals[s, c] = (first * total_scale + second).astype(BF16)
        if s == 1:
            before = jnp.where(upper, far, 0.0)
        else:
            held = before_ref[c]
            before = jnp.where(upper, far * scale_ref[s - 1, 1:2, some_lanes(c)] + held, held)
        if s < levels:
            before_ref[c] = before
            scan_copy(s + 1, c).start()
        else:
            enter(c, before)

    exchange_logs(1)

    skip_ref[...] = spread(jnp.broadcast_to(gain_in_ref[...], (PAD, heads)), expander_ref[...])

    def sample_local():
        samples, length = svalues_ref.shape[:2]
        slocal_ref[...] = jnp.zeros_like(slocal_ref)
        sgain_ref[...] = jnp.zeros_like(sgain_ref)
        picked_ref[...] = jnp.zeros_like(picked_ref)
        u, s = square(length)
        own = lax.broadcasted_iota(jnp.int32, (heads, channels), 1) // dim == (
            lax.broadcasted_iota(jnp.int32, (heads, channels), 0)
        )
        at = lax.broadcasted_iota(jnp.int32, (1, length), 1)
        for k in range(samples):
            last = length_ref[k] - 1
            hot = jnp.where(
                lax.broadcasted_iota(jnp.int32, (PAD, length), 1) == last, 1.0, 0.0
            ).astype(BF16)
            tall = softplus(sstep_ref[k])
            tall_logs = tall * rate_row
            flip = ((0,), (0,))
            gap = dot(tall_logs, jnp.where((u > s) & (u <= last), 1.0, 0.0), flip, EXACT)
            running = dot(tall_logs, jnp.where(u <= last, 1.0, 0.0), flip, EXACT)[:, 0:1]
            wide_steps = dot(tall, jnp.where(u == s, 1.0, 0.0), flip, EXACT)
            row = dot(hot, sread_ref[k])
            score = dot(row.astype(BF16), sinject_ref[k], ((1,), (1,)))[0:1]
            mixing = jnp.where(at <= last, score * jnp.exp(gap) * wide_steps, 0.0).astype(BF16)
            values = svalues_ref[k]
            local = jnp.sum(jnp.where(own, dot(mixing, values), 0.0), axis=0, keepdims=True)
            decay = jnp.sum(jnp.where(own, jnp.exp(running), 0.0), axis=0, keepdims=True)
            value = dot(hot, values)[0:1]
            opened = silu(dot(hot, sgate_ref[k])[0:1])
            slocal_ref[k : k + 1, :] = (local + skip_ref[0:1, :] * value) * opened
            sgain_ref[k : k + 1, :] = decay * opened
            picked_ref[k : k + 1, :] = row[0:1].astype(BF16)

    state_ref[...] = jnp.zeros_like(state_ref)
    offset_ref[...] = jnp.zeros_like(offset_ref)
    for copy in late_copies:
        copy.wait()
    tile_copy.start()

    def block_local(b, hook):
        span = pl.ds(pl.multiple_of(b * BLOCK, BLOCK), BLOCK)
        steps, logs = steps_ref[b], logs_ref[b]
        i, j = square(BLOCK)
        lower = jnp.where(i >= j, 1.0, 0.0)
        running = dot(logs, lower, ((1,), (1,)), EXACT)
        running_t = turn_over(running)
        after = turn_over(dot(logs, jnp.where(i > j, 1.0, 0.0), precision=EXACT))
        turned = turn_over(steps)
        expander = expander_ref[...]
        inject = inject_ref[span, :]
        readout = read_ref[span, :]
        scores = jnp.where(i >= j, dot(readout, inject, ((1,), (1,))), 0.0)
        per = LANES // dim
        lane = lax.broadcasted_iota(jnp.int32, (BLOCK, LANES), 1)
        for k in range(heads // per):
            cut = slice(k * LANES, (k + 1) * LANES)
            pair = values_ref[span, cut]
            mixes, parts = [], []
            for q in range(per):
                h = k * per + q
                gap = jnp.minimum(running_t[:, h : h + 1] - running[h : h + 1, :], 0.0)
                mixes.append((scores * jnp.exp(gap) * steps[h : h + 1, :]).astype(BF16))
                parts.append(jnp.where(lane // dim == q, pair, jnp.zeros_like(pair)))
            part_ref[:, cut] = dot(jnp.concatenate(mixes, axis=1), jnp.concatenate(parts, axis=0))
            if hook is not None and 2 * (k + 1) == heads // per:
                hook(HOOKS * b)
        if hook is not None:
            hook(HOOKS * b + 1)
        decay = spread(jnp.exp(running_t), expander)
        values = values_ref[span, :].astype(F32)
        opened = silu(gate_ref[span, :].astype(F32))
        total = part_ref[...] + skip_ref[0:1, :] * values
        total = total + dot(readout, state_ref[...].astype(BF16)) * decay
        normed_ref[span, :] = (total * opened).astype(BF16)
        if hook is not None:
            hook(HOOKS * b + 2)
        offset = offset_ref[0:1, :]
        gate_ref[span, :] = (opened * spread(jnp.exp(running_t + offset), expander)).astype(BF16)
        offset_ref[0:1, :] = offset + running_t[BLOCK - 1 : BLOCK, :]
        scaled = (spread(jnp.exp(after) * turned, expander) * values).astype(BF16)
        state_ref[...] = state_ref[...] * decay[BLOCK - 1 : BLOCK, :] + dot(
            inject, scaled, ((0,), (0,))
        )
        if hook is not None:
            hook(HOOKS * b + 3)

    def hook(g):
        if squared:
            run_events(row == 0, square_events()[0][g : g + 1])
            return

        for s in range(2, levels + 1):

            @pl.when(g == s - 1)
            def _():
                exchange_logs(s)

        for s in range(1, levels + 1):
            c = g - LAG * (s - 1)

            @pl.when((c >= 0) & (c < chunks))
            def _():
                scan_step(s, c)

    def picked_copy(p):
        return remote(
            picked_ref, picked_all.at[p], small_ssems.at[0], picked_sems.at[0], {"ctx": last_seat}
        )

    def reply_copy(p):
        return remote(
            reply_ref.at[p], reply_got, reply_sems.at[0], small_rsems.at[0], {"ctx": p}
        )

    def late_round(g, carry):
        hook(g)
        return carry

    block_local(0, hook)
    if squared:
        first, second = square_events()
        run_events(row == 0, first[HOOKS:])
        run_events(row == 1, second)
    else:
        lax.fori_loop(HOOKS, max(chunks + LAG * (levels - 1), HOOKS), late_round, 0)
    swap_copy(slice(0, channels), other_rows).wait_recv()
    tile_copy.wait()

    def share(d, q):
        rows = rows_of(q // PARTS)
        start = pl.multiple_of(d * cols + q % PARTS * part, part)
        return dot(normed_ref[rows, :], tiles_ref[:, pl.ds(start, part)])

    def hop_up(d, b):
        return remote(
            sent.at[d, b],
            landing.at[d + 1, b],
            sent_sems.at[d],
            land_sems.at[d + 1, b],
            {"head": place + 1},
        )

    def hop_down(d, b):
        return remote(
            sent.at[d, b],
            landing.at[d, b],
            sent_sems.at[d],
            land_sems.at[d, b],
            {"head": place - 1},
        )

    def all_up(d):
        return remote(
            sent.at[d], landing.at[d + 1], sent_sems.at[d], land_sems.at[0, 0], {"head": place + 1}
        )

    def all_down(d):
        return remote(
            sent.at[d], landing.at[d], sent_sems.at[d], land_sems.at[0, 0], {"head": place - 1}
        )

    def shop_up(d):
        return remote(
            ssent.at[d],
            slanding.at[d + 1],
            ssent_sems.at[d],
            sland_sems.at[d + 1],
            {"head": place + 1},
        )

    def shop_down(d):
        return remote(
            ssent.at[d], slanding.at[d], ssent_sems.at[d], sland_sems.at[d], {"head": place - 1}
        )

    def rows_of(b):
        return pl.ds(pl.multiple_of(b * BLOCK, BLOCK), BLOCK)

    def pass_on(d, b, slot, move, fed):
        acc_ref[...] = share(d, b)

        @pl.when(fed)
        def _():
            move(d, b).wait_recv()
            acc_ref[...] = acc_ref[...] + landing[slot, b].astype(F32)

        sent[d, b] = acc_ref[...].astype(BF16)
        move(d, b).start()

    def finish_block(b):
        span = rows_of(b)
        readout = read_ref[span, :]
        pieces = []
        for q in range(groups):
            lanes = group_lanes(q)
            arrival = dot(readout, enter_ref[:, lanes])
            piece = normed_ref[span, lanes].astype(F32)
            pieces.append(piece + arrival * gate_ref[span, lanes].astype(F32))
        normed_ref[span, :] = finish_rows(jnp.concatenate(pieces, axis=1), norm_ref[...])

    padded = slocal_ref.shape[0]
    few_rows = reply_got.shape[0]
    srows = pl.ds(tokens, padded)

    def answer():
        picked_all[last_seat] = picked_ref[...]
        others = picked_all.at[pl.ds(0, peers - 1)]
        remote(others, others, small_ssems.at[0], picked_sems.at[0], {"ctx": 0}).wait_recv()
        asked = picked_all[...].reshape(peers * padded, entries)
        for q in range(groups):
            lanes = group_lanes(q)
            entered = enter_ref[:, lanes].astype(F32) * pair_scale[0:1, lanes]
            final = entered + mine_state[:, lanes].astype(F32)
            told = dot(asked, final.astype(BF16))
            for p in range(peers - 1):
                reply_ref[p, :, lanes] = told[p * padded : p * padded + few_rows]
            reply_got[:, lanes] = told[last_seat * padded : last_seat * padded + few_rows]
        for p in range(peers - 1):
            reply_copy(p).start()

    def finish_samples():
        @pl.when(jnp.logical_not(holds_final))
        def _():
            reply_copy(0).wait_recv()

        total = slocal_ref[:few_rows] + reply_got[...] * sgain_ref[:few_rows]
        normed = finish_rows(total, norm_ref[...])
        if few_rows < padded:
            normed = jnp.concatenate([normed, jnp.zeros((padded - few_rows, channels), BF16)], axis=0)
        normed_ref[srows, :] = normed

    few = sresult_ref.shape[0]

    def sshare(d):
        wide = dot(normed_ref[srows, :], tiles_ref[:, pl.ds(pl.multiple_of(d * cols, cols), cols)])
        return jnp.concatenate([wide[:few, q * LANES : (q + 1) * LANES] for q in range(cols // LANES)], axis=0)

    def spass_on(d, slot, move, fed):
        sown_ref[...] = sshare(d)

        @pl.when(fed)
        def _():
            move(d).wait_recv()
            sown_ref[...] = sown_ref[...] + slanding[slot].astype(F32)

        ssent[d] = sown_ref[...].astype(BF16)
        move(d).start()

    sample_start = PARTS * (blocks + 1)

    def step(t, carry):
        block, first_part, last_part = t // PARTS, t % PARTS == 0, t % PARTS == PARTS - 1

        @pl.when((block < blocks) & first_part)
        def _():
            finish_block(block)

        @pl.when(t == sample_start)
        def _():
            finish_samples()

        rising, falling = t - place, t - (n - 1 - place)
        up, down = n - 1 - rising // per, falling // per

        @pl.when((rising >= 0) & (up > place))
        def _():
            pass_on(up, rising % per, up + 1, hop_up, place > 0)

        @pl.when((falling >= 0) & (down < place))
        def _():
            pass_on(down, falling % per, down, hop_down, place < n - 1)

        srising, sfalling = rising - sample_start, falling - sample_start
        sup, sdown = n - 1 - srising, sfalling

        @pl.when((srising >= 0) & (sup > place))
        def _():
            spass_on(sup, sup + 1, shop_up, place > 0)

        @pl.when((sfalling >= 0) & (sdown < place))
        def _():
            spass_on(sdown, sdown, shop_down, place < n - 1)

        @pl.when((block + 1 < blocks) & last_part)
        def _():
            block_local(block + 1, None)

        @pl.when((block == blocks - 2) & last_part)
        def _():
            sample_local()

            @pl.when(jnp.logical_not(holds_final))
            def _():
                picked_copy(seat).start()

        @pl.when((block == blocks - 1) & last_part & holds_final)
        def _():
            answer()

        return carry

    lax.fori_loop(0, (n - 1) * per, step, 0)
    sown_ref[...] = sshare(place)

    @pl.when(place < n - 1)
    def _():
        shop_down(place).wait_recv()
        sown_ref[...] = sown_ref[...] + slanding[place].astype(F32)

    @pl.when(place > 0)
    def _():
        shop_up(place).wait_recv()
        sown_ref[...] = sown_ref[...] + slanding[place + 1].astype(F32)

    for q in range(cols // LANES):
        sresult_ref[:, q * LANES : (q + 1) * LANES] = sown_ref[q * few : (q + 1) * few, :].astype(BF16)
    sout_copy = pltpu.make_async_copy(sresult_ref, sout_hbm, late_sems.at[len(late)])
    sout_copy.start()

    remote(
        mine_state.at[other_rows], pair_state, pair_ssems.at[0], pair_rsems.at[0], {"ctx": mate(0)}
    ).wait_send()
    swap_copy(slice(0, channels), own_rows).wait_send()

    def scan_sent(s, count):
        span = pl.ds(0, count)
        remote(
            totals.at[s - 1, span],
            arrived.at[s - 1, span],
            scan_ssems.at[s - 1],
            scan_rsems.at[s - 1, 0],
            {"ctx": mate(1)},
        ).wait_send()

    for s in range(1, scan_steps + 1):
        if not squared:
            scan_sent(s, chunks)
        elif s == 1:

            @pl.when((column == 0) & (row == 0))
            def _():
                scan_sent(1, chunks)

            @pl.when(column + row == 1)
            def _():
                scan_sent(1, pairs)

        else:

            @pl.when(row == s - 2)
            def _():
                scan_sent(s, pairs)

    for s in range(log_steps):
        log_copy(s).wait_send()

    @pl.when(holds_final)
    def _():
        remote(reply_ref, reply_ref, reply_sems.at[0], small_rsems.at[0], {"ctx": 0}).wait_send()

    @pl.when(jnp.logical_not(holds_final))
    def _():
        picked_copy(seat).wait_send()

    def out_place(b):
        return pl.ds(pl.multiple_of(b % PARTS * part, part), part), rows_of(b // PARTS)

    def gather(b, carry):
        acc_ref[...] = share(place, b)

        @pl.when(place < n - 1)
        def _():
            hop_down(place, b).wait_recv()
            acc_ref[...] = acc_ref[...] + landing[place, b].astype(F32)

        @pl.when(place > 0)
        def _():
            hop_up(place, b).wait_recv()
            acc_ref[...] = acc_ref[...] + landing[place + 1, b].astype(F32)

        where = out_place(b)
        result_ref[where] = turn_over(acc_ref[...]).astype(BF16)
        pltpu.make_async_copy(result_ref.at[where], out_hbm.at[where], out_sems.at[0]).start()
        return carry

    lax.fori_loop(0, per, gather, 0)
    for d in range(n):

        @pl.when(d > place)
        def _():
            all_up(d).wait_send()
            shop_up(d).wait_send()

        @pl.when(d < place)
        def _():
            all_down(d).wait_send()
            shop_down(d).wait_send()

    sout_copy.wait()
    pltpu.make_async_copy(result_ref, out_hbm, out_sems.at[0]).wait()


def hand_over_kernel(bands, mixed_hbm, smixed_hbm, out_hbm, sout_hbm, bands_ref, few_ref, sems):
    rows = mixed_hbm.shape[0] // bands
    moves = [(smixed_hbm, few_ref, sout_hbm)]
    for q in range(bands):
        part = pl.ds(q * rows, rows)
        moves.append((mixed_hbm.at[part], bands_ref.at[q], out_hbm.at[part]))
    ins = [pltpu.make_async_copy(a, b, sems.at[0, q]) for q, (a, b, _) in enumerate(moves)]
    outs = [pltpu.make_async_copy(b, c, sems.at[1, q]) for q, (_, b, c) in enumerate(moves)]
    for copy in ins:
        copy.start()
    for into, out in zip(ins, outs):
        into.wait()
        out.start()
    for copy in outs:
        copy.wait()


def per_device(
    prompt_values,
    prompt_gate,
    prompt_inject,
    prompt_read,
    prompt_step,
    decay_log,
    skip_gain,
    norm_weight,
    out_weight,
    sample_values,
    sample_gate,
    sample_inject,
    sample_read,
    sample_step,
    sample_length,
):
    n, peers = lax.axis_size("head"), lax.axis_size("ctx")
    levels = peers.bit_length() - 2
    scan_steps = 3 if levels == 2 else levels
    log_steps = 2 if levels == 2 else levels + 1
    tokens, channels = prompt_values.shape
    heads = prompt_step.shape[0]
    dim = channels // heads
    entries = prompt_inject.shape[2]
    half = entries // 2
    samples, length = sample_values.shape[:2]
    padded = -(-samples // (2 * PAD)) * 2 * PAD
    cols = out_weight.shape[1] // n
    blocks, chunks = tokens // BLOCK, channels // CHUNK
    part, per = cols // PARTS, blocks * PARTS
    vmem = pl.BlockSpec(memory_space=pltpu.VMEM)
    hbm = pl.BlockSpec(memory_space=pl.ANY)
    dma = pltpu.SemaphoreType.DMA
    shape = jax.ShapeDtypeStruct
    V = pltpu.VMEM
    mixed, smixed = pl.pallas_call(
        functools.partial(layer_kernel, dim, n, peers),
        out_shape=(shape((cols, tokens), BF16), shape((samples, cols), BF16)),
        in_specs=[
            pl.BlockSpec(memory_space=pltpu.SMEM),
            hbm,
            hbm,
            vmem,
            hbm,
            vmem,
            vmem,
            vmem,
            vmem,
            hbm,
            hbm,
            hbm,
            hbm,
            hbm,
            hbm,
        ],
        out_specs=(hbm, hbm),
        scratch_shapes=[
            V((tokens, channels), BF16),
            V((tokens, channels), BF16),
            V((tokens, entries), BF16),
            V(sample_values.shape, BF16),
            V(sample_gate.shape, BF16),
            V((samples, length, entries), BF16),
            V((samples, length, entries), BF16),
            V((samples, length, heads), F32),
            V(out_weight.shape, BF16),
            V((blocks, heads, BLOCK), F32),
            V((blocks, heads, BLOCK), F32),
            V((tokens, 2 * heads), BF16),
            V((2 * heads, channels), BF16),
            V((entries, tokens), BF16),
            V((PAD, channels), F32),
            V((entries, channels), BF16),
            V((half, channels), BF16),
            V((levels + 1, chunks, half, CHUNK), BF16),
            V((scan_steps, chunks, half, CHUNK), BF16),
            V((chunks, half, CHUNK), F32),
            V((half, channels), BF16),
            V((entries, channels), BF16),
            V((log_steps, PAD, heads), F32),
            V((log_steps, PAD, heads), F32),
            V((PAD, heads), F32),
            V((PAD, channels), F32),
            V((levels, PAD, channels), F32),
            V((entries, channels), F32),
            V((PAD, heads), F32),
            V((BLOCK, channels), F32),
            V((tokens + padded, channels), BF16),
            V((padded, channels), F32),
            V((padded, channels), F32),
            V((padded, entries), BF16),
            V((peers, padded, entries), BF16),
            V((peers - 1, -(-samples // PAD) * PAD, channels), F32),
            V((-(-samples // PAD) * PAD, channels), F32),
            V((BLOCK, part), F32),
            V((n, per, BLOCK, part), BF16),
            V((n + 1, per, BLOCK, part), BF16),
            V((n, samples * cols // LANES, LANES), BF16),
            V((n + 1, samples * cols // LANES, LANES), BF16),
            V((samples * cols // LANES, LANES), F32),
            V((cols, tokens), BF16),
            V((samples, cols), BF16),
            dma((chunks // GROUP,)),
            dma((8,)),
            dma((1,)),
            dma((1,)),
            dma((log_steps,)),
            dma((log_steps,)),
            dma((1,)),
            dma((chunks // GROUP,)),
            dma((scan_steps,)),
            dma((scan_steps, chunks)),
            dma((1,)),
            dma((1,)),
            dma((1,)),
            dma((1,)),
            dma((1,)),
            dma((1,)),
            dma((n,)),
            dma((n + 1, per)),
            dma((n,)),
            dma((n + 1,)),
        ],
        compiler_params=pltpu.CompilerParams(
            collective_id=0, has_side_effects=True, vmem_limit_bytes=VMEM_LIMIT
        ),
    )(
        sample_length,
        prompt_values,
        prompt_gate,
        prompt_inject.reshape(tokens, entries),
        prompt_read.reshape(tokens, entries),
        prompt_step,
        decay_log[None],
        skip_gain[None],
        norm_weight[None],
        out_weight,
        sample_values,
        sample_gate,
        sample_inject.reshape(samples, length, entries),
        sample_read.reshape(samples, length, entries),
        sample_step.transpose(1, 2, 0),
    )
    bands = 4
    band = (cols // bands, tokens)
    mixed, smixed = pl.pallas_call(
        functools.partial(hand_over_kernel, bands),
        out_shape=(shape((cols, tokens), BF16), shape((samples, cols), BF16)),
        in_specs=[hbm, hbm],
        out_specs=(hbm, hbm),
        scratch_shapes=[
            V((bands, *band), BF16),
            V((samples, cols), BF16),
            dma((2, bands + 1)),
        ],
    )(mixed, smixed)
    return mixed, smixed.T


def solution(mesh):
    in_specs = (
        P("ctx", "head"),
        P("ctx", "head"),
        P("ctx", "head", None),
        P("ctx", "head", None),
        P("head", "ctx"),
        P("head"),
        P("head"),
        P("head"),
        P("head", None),
        P("ctx", None, "head"),
        P("ctx", None, "head"),
        P("ctx", None, "head", None),
        P("ctx", None, "head", None),
        P("head", "ctx", None),
        P("ctx"),
    )
    out_specs = (P("head", "ctx"), P("head", "ctx"))
    return jax.shard_map(
        per_device, mesh=mesh, in_specs=in_specs, out_specs=out_specs, check_vma=False
    )
```

```python
import functools

import jax
import jax.numpy as jnp
from jax import lax
from jax.experimental import pallas as pl
from jax.experimental.pallas import tpu as pltpu
from jax.sharding import PartitionSpec as P

BLOCK = 128
LANES = 128
PAD = 8
F32 = jnp.float32
BF16 = jnp.bfloat16
EXACT = lax.Precision.HIGHEST
VMEM_LIMIT = 60 * 1024 * 1024


def dot(a, b, dims=((1,), (0,)), precision=None):
    return lax.dot_general(a, b, (dims, ((), ())), precision=precision, preferred_element_type=F32)


def softplus(v):
    return jnp.maximum(v, 0.0) + jnp.log1p(jnp.exp(-jnp.abs(v)))


def silu(v):
    return v / (1.0 + jnp.exp(-v))


def spread(w, expander):
    high = w.astype(BF16)
    low = (w - high.astype(F32)).astype(BF16)
    return dot(jnp.concatenate([high, low], axis=1), expander)


def expander_of(heads, dim):
    row = lax.broadcasted_iota(jnp.int32, (2 * heads, heads * dim), 0)
    lane = lax.broadcasted_iota(jnp.int32, (2 * heads, heads * dim), 1)
    head = lane // dim
    return jnp.where((row == head) | (row == head + heads), 1.0, 0.0).astype(BF16)


def square(n):
    return (
        lax.broadcasted_iota(jnp.int32, (n, n), 0),
        lax.broadcasted_iota(jnp.int32, (n, n), 1),
    )


def finish_rows(total, weight):
    mean = jnp.mean(total * total, axis=1, keepdims=True)
    return (total * lax.rsqrt(mean + 1e-05) * weight).astype(BF16)


CHUNK = LANES
GROUP = 4
PARTS = 2
LAG = 3
HOOKS = 4


def turn_over(w):
    return jnp.transpose(w, (1, 0))


def layer_kernel(
    dim,
    n,
    peers,
    length_ref,
    values_hbm,
    gate_hbm,
    inject_ref,
    read_hbm,
    step_ref,
    decay_ref,
    gain_in_ref,
    norm_ref,
    weight_hbm,
    svalues_hbm,
    sgate_hbm,
    sinject_hbm,
    sread_hbm,
    sstep_hbm,
    out_hbm,
    sout_hbm,
    values_ref,
    gate_ref,
    read_ref,
    svalues_ref,
    sgate_ref,
    sinject_ref,
    sread_ref,
    sstep_ref,
    tiles_ref,
    steps_ref,
    logs_ref,
    wide_ref,
    expander_ref,
    turned_ref,
    skip_ref,
    mine_state,
    pair_state,
    totals,
    arrived,
    before_ref,
    swap_ref,
    enter_ref,
    log_sent,
    log_got,
    before_logs,
    pair_scale,
    scale_ref,
    state_ref,
    offset_ref,
    part_ref,
    normed_ref,
    slocal_ref,
    sgain_ref,
    picked_ref,
    picked_all,
    reply_ref,
    reply_got,
    acc_ref,
    sent,
    landing,
    ssent,
    slanding,
    sown_ref,
    result_ref,
    sresult_ref,
    value_sems,
    late_sems,
    tile_sems,
    out_sems,
    log_ssems,
    log_rsems,
    pair_ssems,
    pair_rsems,
    scan_ssems,
    scan_rsems,
    swap_ssems,
    swap_rsems,
    small_ssems,
    small_rsems,
    picked_sems,
    reply_sems,
    sent_sems,
    land_sems,
    ssent_sems,
    sland_sems,
):
    tokens, channels = values_ref.shape
    heads = step_ref.shape[0]
    entries = inject_ref.shape[1]
    half = entries // 2
    cols = weight_hbm.shape[1] // n
    part = acc_ref.shape[1]
    per = sent.shape[1]
    chunks = channels // CHUNK
    blocks = tokens // BLOCK
    levels = peers.bit_length() - 2
    squared = levels == 2
    log_steps = 2 if squared else levels + 1
    scan_steps = arrived.shape[0]
    place = lax.axis_index("head")
    seat = lax.axis_index("ctx")
    side = seat % 2
    odd = side == 1
    own_rows = pl.ds(pl.multiple_of(side * half, half), half)
    other_rows = pl.ds(pl.multiple_of((1 - side) * half, half), half)

    def lanes_of(c):
        return slice(c * CHUNK, (c + 1) * CHUNK)

    def some_lanes(c):
        return pl.ds(pl.multiple_of(c * CHUNK, CHUNK), CHUNK)

    groups = chunks // GROUP

    def group_lanes(q):
        return slice(q * GROUP * CHUNK, (q + 1) * GROUP * CHUNK)

    def value_copy(q):
        lanes = group_lanes(q)
        return pltpu.make_async_copy(values_hbm.at[:, lanes], values_ref.at[:, lanes], value_sems.at[q])

    late = [
        (gate_hbm, gate_ref),
        (read_hbm, read_ref),
        (svalues_hbm, svalues_ref),
        (sgate_hbm, sgate_ref),
        (sinject_hbm, sinject_ref),
        (sread_hbm, sread_ref),
        (sstep_hbm, sstep_ref),
    ]
    late_copies = [pltpu.make_async_copy(*refs, late_sems.at[q]) for q, refs in enumerate(late)]

    tile_copy = pltpu.make_async_copy(weight_hbm, tiles_ref, tile_sems.at[0])

    for q in range(groups):
        value_copy(q).start()

    def digit(s):
        return (seat // (1 << s)) % 2

    def mate(s):
        return seat + (1 << s) - (2 << s) * digit(s)

    barrier = pltpu.get_barrier_semaphore()

    def greet(device):
        pl.semaphore_signal(
            barrier, inc=1, device_id=device, device_id_type=pl.DeviceIdType.MESH
        )

    for s in range(levels + 1):
        greet({"ctx": mate(s)})

    last_seat = peers - 1
    holds_final = seat == last_seat

    @pl.when(holds_final)
    def _():
        for p in range(peers - 1):
            greet({"ctx": p})

    @pl.when(jnp.logical_not(holds_final))
    def _():
        greet({"ctx": last_seat})

    @pl.when(place > 0)
    def _():
        greet({"head": place - 1})

    @pl.when(place < n - 1)
    def _():
        greet({"head": place + 1})

    rows, lanes = square(heads)
    rate_row = -jnp.exp(decay_ref[...])
    rate = jnp.sum(jnp.where(rows == lanes, rate_row, 0.0), axis=1, keepdims=True)
    steps = softplus(step_ref[...])
    logs = steps * rate
    i, j = square(BLOCK)

    def fill_expander():
        expander_ref[...] = expander_of(heads, dim)

    fill_expander()
    def stack(ref, wide):
        for b in range(blocks):
            ref[b] = wide[:, b * BLOCK : (b + 1) * BLOCK]
        return ref[...].reshape(blocks * heads, BLOCK)

    tall_steps, tall_logs = stack(steps_ref, steps), stack(logs_ref, logs)
    after = dot(tall_logs, jnp.where(i > j, 1.0, 0.0), precision=EXACT)
    sums = jnp.sum(tall_logs, axis=1, keepdims=True)
    later, offsets = jnp.zeros((heads, 1), F32), []
    for b in reversed(range(blocks)):
        offsets.insert(0, later)
        later = later + sums[b * heads : (b + 1) * heads]
    w = turn_over(jnp.exp(after + jnp.concatenate(offsets, axis=0)) * tall_steps)
    for b in range(blocks):
        block_w = w[:, b * heads : (b + 1) * heads]
        high = block_w.astype(BF16)
        low = (block_w - high.astype(F32)).astype(BF16)
        wide_ref[b * BLOCK : (b + 1) * BLOCK, :] = jnp.concatenate([high, low], axis=1)
    total_logs = jnp.sum(jnp.where(rows == lanes, later, 0.0), axis=0, keepdims=True)
    total_logs = jnp.broadcast_to(total_logs, (PAD, heads))

    def turn_inject():
        turned_ref[...] = turn_over(inject_ref[...].astype(F32)).astype(BF16)

    turn_inject()
    top = lax.broadcasted_iota(jnp.int32, (PAD, heads), 0) == 0

    inside = (place > 0) & (place < n - 1)
    log_sent[0] = total_logs
    before_logs[...] = jnp.zeros_like(before_logs)

    def state_of(q):
        lanes = group_lanes(q)
        value_copy(q).wait()
        wide = dot(wide_ref[...], expander_ref[:, lanes])
        scaled = (wide * values_ref[:, lanes].astype(F32)).astype(BF16)
        mine_state[:, lanes] = dot(turned_ref[...], scaled).astype(BF16)

    state_of(0)

    for middle in (False, True):
        for final in (False, True):

            @pl.when((inside == middle) & (holds_final == final))
            def _():
                pl.semaphore_wait(barrier, levels + 2 + middle + (peers - 1 if final else 1))

    def remote(src, dst, ssem, rsem, device):
        return pltpu.make_async_remote_copy(
            src_ref=src,
            dst_ref=dst,
            send_sem=ssem,
            recv_sem=rsem,
            device_id=device,
            device_id_type=pl.DeviceIdType.MESH,
        )

    def log_copy(s):
        return remote(
            log_sent.at[s], log_got.at[s], log_ssems.at[s], log_rsems.at[s], {"ctx": mate(s)}
        )

    def pair_copy(q):
        return remote(
            mine_state.at[other_rows, group_lanes(q)],
            pair_state.at[:, group_lanes(q)],
            pair_ssems.at[0],
            pair_rsems.at[q],
            {"ctx": mate(0)},
        )

    def scan_copy(s, c):
        slot = c // 2 + (s - 2) * (chunks // 2) if squared and s > 1 else c
        return remote(
            totals.at[s - 1, c],
            arrived.at[s - 1, c],
            scan_ssems.at[s - 1],
            scan_rsems.at[s - 1 if not squared or s == 1 else 1, slot],
            {"ctx": mate(1 if squared and s == 3 else s)},
        )

    def swap_copy(lanes, where):
        return remote(
            swap_ref.at[:, lanes],
            enter_ref.at[where, lanes],
            swap_ssems.at[0],
            swap_rsems.at[0],
            {"ctx": mate(0)},
        )

    log_copy(0).start()

    def exchange_logs(s):
        log_copy(s).wait_recv()
        got, own = log_got[s], log_sent[s]
        upper = digit(s) == 1
        above = jnp.where(upper, own, got)
        if s == 0:
            pair = jnp.where(top, above, jnp.where(odd, got, own))
            pair_scale[...] = spread(jnp.exp(pair), expander_ref[...])
        else:
            held = before_logs[...]
            crossed = jnp.where(digit(2) == 1, jnp.where(upper, got, own), above) if squared else above
            scale_ref[s - 1] = spread(jnp.exp(jnp.where(top, crossed, held)), expander_ref[...])
            before_logs[...] = held + jnp.where(upper, got, 0.0)
        if s < log_steps - 1:
            log_sent[s + 1] = own + got
            log_copy(s + 1).start()

    column, row = digit(1), digit(2)

    def at_once(c):
        if not squared:
            return seat >= 0
        if c % 2:
            return column == 0
        return (column == 1) & (row == 0)

    def pair_up(c):
        mine = mine_state[own_rows, lanes_of(c)].astype(F32)
        theirs = pair_state[:, lanes_of(c)].astype(F32)
        first, second = jnp.where(odd, theirs, mine), jnp.where(odd, mine, theirs)
        totals[0, c] = (first * pair_scale[0:1, lanes_of(c)] + second).astype(BF16)

        @pl.when(at_once(c))
        def _():
            scan_copy(1, c).start()

    pairs = chunks // 2

    def pair_group(q):
        pair_copy(q).wait_recv()
        for c in sorted(range(q * GROUP, (q + 1) * GROUP), key=lambda c: 1 - c % 2):
            pair_up(c)

    for q in range(groups):
        if q:
            state_of(q)
        pair_copy(q).start()
        if q == 0:
            for copy in late_copies:
                copy.start()
        if q == 1:
            exchange_logs(0)
        if q:
            pair_group(q - 1)
    pair_group(groups - 1)
    if squared:
        for c in range(0, chunks, 2):

            @pl.when((column == 0) & (row == 0))
            def _():
                scan_copy(1, c).start()

    def enter(c, before):
        even_state = jnp.where(odd, pair_state[:, some_lanes(c)].astype(F32), mine_state[own_rows, some_lanes(c)].astype(F32))
        moved = before * pair_scale[1:2, some_lanes(c)] + even_state
        enter_ref[own_rows, some_lanes(c)] = jnp.where(odd, moved, before).astype(BF16)
        swap_ref[:, some_lanes(c)] = jnp.where(odd, before, moved).astype(BF16)
        swap_copy(some_lanes(c), own_rows).start()

    def cross_row(q):
        c = 2 * q + column
        scan_copy(1, c).wait_recv()
        far, near = arrived[0, c].astype(F32), totals[0, c].astype(F32)
        right = column == 1
        first, second = jnp.where(right, far, near), jnp.where(right, near, far)
        totals[1, c] = (first * scale_ref[0, 0:1, some_lanes(c)] + second).astype(BF16)
        scan_copy(2, c).start()
        enter(c, jnp.where(right, far, 0.0))

        @pl.when(column == 0)
        def _():
            enter(c + 1, jnp.zeros((half, CHUNK), F32))

    def end_row(q):
        @pl.when(column == 1)
        def _():
            scan_copy(1, 2 * q).wait_recv()
            enter(2 * q, arrived[0, 2 * q].astype(F32))

    def next_row(q):
        c = 2 * q + column
        right = column == 1

        @pl.when(right)
        def _():
            scan_copy(1, c).wait_recv()
            totals[0, c] = arrived[0, c]

        scan_copy(2, c).wait_recv()
        far = arrived[1, c].astype(F32)
        joined = far * scale_ref[0, 0:1, some_lanes(c)] + totals[0, c].astype(F32)
        totals[2, c] = jnp.where(right, far, joined).astype(BF16)
        scan_copy(3, c).start()
        enter(c, jnp.where(right, joined, far))

    def last_column(q):
        c = 2 * q + 1 - column
        scan_copy(3, c).wait_recv()
        enter(c, arrived[2, c].astype(F32))

    def square_events():
        first = [(q, cross_row, q) for q in range(pairs)]
        first += [(q + pairs, end_row, q) for q in range(pairs)]
        second = [(q, next_row, q) for q in range(pairs)]
        second += [(q + 4.5, last_column, q) for q in range(pairs)]
        return [sorted(events, key=lambda event: event[0]) for events in (first, second)]

    def run_events(here, events):
        @pl.when(here)
        def _():
            for _, work, q in events:
                work(q)

    def scan_step(s, c):
        scan_copy(s, c).wait_recv()
        upper = digit(s) == 1
        far = arrived[s - 1, c].astype(F32)
        near = totals[s - 1, c].astype(F32)
        first, second = jnp.where(upper, far, near), jnp.where(upper, near, far)
        total_scale = scale_ref[s - 1, 0:1, some_lanes(c)]
        totals[s, c] = (first * total_scale + second).astype(BF16)
        if s == 1:
            before = jnp.where(upper, far, 0.0)
        else:
            held = before_ref[c]
            before = jnp.where(upper, far * scale_ref[s - 1, 1:2, some_lanes(c)] + held, held)
        if s < levels:
            before_ref[c] = before
            scan_copy(s + 1, c).start()
        else:
            enter(c, before)

    exchange_logs(1)

    skip_ref[...] = spread(jnp.broadcast_to(gain_in_ref[...], (PAD, heads)), expander_ref[...])

    def sample_local():
        samples, length = svalues_ref.shape[:2]
        slocal_ref[...] = jnp.zeros_like(slocal_ref)
        sgain_ref[...] = jnp.zeros_like(sgain_ref)
        picked_ref[...] = jnp.zeros_like(picked_ref)
        u, s = square(length)
        own = lax.broadcasted_iota(jnp.int32, (heads, channels), 1) // dim == (
            lax.broadcasted_iota(jnp.int32, (heads, channels), 0)
        )
        at = lax.broadcasted_iota(jnp.int32, (1, length), 1)
        for k in range(samples):
            last = length_ref[k] - 1
            hot = jnp.where(
                lax.broadcasted_iota(jnp.int32, (PAD, length), 1) == last, 1.0, 0.0
            ).astype(BF16)
            tall = softplus(sstep_ref[k])
            tall_logs = tall * rate_row
            flip = ((0,), (0,))
            gap = dot(tall_logs, jnp.where((u > s) & (u <= last), 1.0, 0.0), flip, EXACT)
            running = dot(tall_logs, jnp.where(u <= last, 1.0, 0.0), flip, EXACT)[:, 0:1]
            wide_steps = dot(tall, jnp.where(u == s, 1.0, 0.0), flip, EXACT)
            row = dot(hot, sread_ref[k])
            score = dot(row.astype(BF16), sinject_ref[k], ((1,), (1,)))[0:1]
            mixing = jnp.where(at <= last, score * jnp.exp(gap) * wide_steps, 0.0).astype(BF16)
            values = svalues_ref[k]
            local = jnp.sum(jnp.where(own, dot(mixing, values), 0.0), axis=0, keepdims=True)
            decay = jnp.sum(jnp.where(own, jnp.exp(running), 0.0), axis=0, keepdims=True)
            value = dot(hot, values)[0:1]
            opened = silu(dot(hot, sgate_ref[k])[0:1])
            slocal_ref[k : k + 1, :] = (local + skip_ref[0:1, :] * value) * opened
            sgain_ref[k : k + 1, :] = decay * opened
            picked_ref[k : k + 1, :] = row[0:1].astype(BF16)

    state_ref[...] = jnp.zeros_like(state_ref)
    offset_ref[...] = jnp.zeros_like(offset_ref)
    for copy in late_copies:
        copy.wait()
    tile_copy.start()

    def block_local(b, hook):
        span = pl.ds(pl.multiple_of(b * BLOCK, BLOCK), BLOCK)
        steps, logs = steps_ref[b], logs_ref[b]
        i, j = square(BLOCK)
        lower = jnp.where(i >= j, 1.0, 0.0)
        running = dot(logs, lower, ((1,), (1,)), EXACT)
        running_t = turn_over(running)
        after = turn_over(dot(logs, jnp.where(i > j, 1.0, 0.0), precision=EXACT))
        turned = turn_over(steps)
        expander = expander_ref[...]
        inject = inject_ref[span, :]
        readout = read_ref[span, :]
        scores = jnp.where(i >= j, dot(readout, inject, ((1,), (1,))), 0.0)
        per = LANES // dim
        lane = lax.broadcasted_iota(jnp.int32, (BLOCK, LANES), 1)
        for k in range(heads // per):
            cut = slice(k * LANES, (k + 1) * LANES)
            pair = values_ref[span, cut]
            mixes, parts = [], []
            for q in range(per):
                h = k * per + q
                gap = jnp.minimum(running_t[:, h : h + 1] - running[h : h + 1, :], 0.0)
                mixes.append((scores * jnp.exp(gap) * steps[h : h + 1, :]).astype(BF16))
                parts.append(jnp.where(lane // dim == q, pair, jnp.zeros_like(pair)))
            part_ref[:, cut] = dot(jnp.concatenate(mixes, axis=1), jnp.concatenate(parts, axis=0))
            if hook is not None and 2 * (k + 1) == heads // per:
                hook(HOOKS * b)
        if hook is not None:
            hook(HOOKS * b + 1)
        decay = spread(jnp.exp(running_t), expander)
        values = values_ref[span, :].astype(F32)
        opened = silu(gate_ref[span, :].astype(F32))
        total = part_ref[...] + skip_ref[0:1, :] * values
        total = total + dot(readout, state_ref[...].astype(BF16)) * decay
        normed_ref[span, :] = (total * opened).astype(BF16)
        if hook is not None:
            hook(HOOKS * b + 2)
        offset = offset_ref[0:1, :]
        gate_ref[span, :] = (opened * spread(jnp.exp(running_t + offset), expander)).astype(BF16)
        offset_ref[0:1, :] = offset + running_t[BLOCK - 1 : BLOCK, :]
        scaled = (spread(jnp.exp(after) * turned, expander) * values).astype(BF16)
        state_ref[...] = state_ref[...] * decay[BLOCK - 1 : BLOCK, :] + dot(
            inject, scaled, ((0,), (0,))
        )
        if hook is not None:
            hook(HOOKS * b + 3)

    def hook(g):
        if squared:
            run_events(row == 0, square_events()[0][g : g + 1])
            return

        for s in range(2, levels + 1):

            @pl.when(g == s - 1)
            def _():
                exchange_logs(s)

        for s in range(1, levels + 1):
            c = g - LAG * (s - 1)

            @pl.when((c >= 0) & (c < chunks))
            def _():
                scan_step(s, c)

    def picked_copy(p):
        return remote(
            picked_ref, picked_all.at[p], small_ssems.at[0], picked_sems.at[0], {"ctx": last_seat}
        )

    def reply_copy(p):
        return remote(
            reply_ref.at[p], reply_got, reply_sems.at[0], small_rsems.at[0], {"ctx": p}
        )

    def late_round(g, carry):
        hook(g)
        return carry

    block_local(0, hook)
    if squared:
        first, second = square_events()
        run_events(row == 0, first[HOOKS:])
        run_events(row == 1, second)
    else:
        lax.fori_loop(HOOKS, max(chunks + LAG * (levels - 1), HOOKS), late_round, 0)
    swap_copy(slice(0, channels), other_rows).wait_recv()
    tile_copy.wait()

    def share(d, q):
        rows = rows_of(q // PARTS)
        start = pl.multiple_of(d * cols + q % PARTS * part, part)
        return dot(normed_ref[rows, :], tiles_ref[:, pl.ds(start, part)])

    def hop_up(d, b):
        return remote(
            sent.at[d, b],
            landing.at[d + 1, b],
            sent_sems.at[d],
            land_sems.at[d + 1, b],
            {"head": place + 1},
        )

    def hop_down(d, b):
        return remote(
            sent.at[d, b],
            landing.at[d, b],
            sent_sems.at[d],
            land_sems.at[d, b],
            {"head": place - 1},
        )

    def all_up(d):
        return remote(
            sent.at[d], landing.at[d + 1], sent_sems.at[d], land_sems.at[0, 0], {"head": place + 1}
        )

    def all_down(d):
        return remote(
            sent.at[d], landing.at[d], sent_sems.at[d], land_sems.at[0, 0], {"head": place - 1}
        )

    def shop_up(d):
        return remote(
            ssent.at[d],
            slanding.at[d + 1],
            ssent_sems.at[d],
            sland_sems.at[d + 1],
            {"head": place + 1},
        )

    def shop_down(d):
        return remote(
            ssent.at[d], slanding.at[d], ssent_sems.at[d], sland_sems.at[d], {"head": place - 1}
        )

    def rows_of(b):
        return pl.ds(pl.multiple_of(b * BLOCK, BLOCK), BLOCK)

    def pass_on(d, b, slot, move, fed):
        acc_ref[...] = share(d, b)

        @pl.when(fed)
        def _():
            move(d, b).wait_recv()
            acc_ref[...] = acc_ref[...] + landing[slot, b].astype(F32)

        sent[d, b] = acc_ref[...].astype(BF16)
        move(d, b).start()

    def finish_block(b):
        span = rows_of(b)
        readout = read_ref[span, :]
        pieces = []
        for q in range(groups):
            lanes = group_lanes(q)
            arrival = dot(readout, enter_ref[:, lanes])
            piece = normed_ref[span, lanes].astype(F32)
            pieces.append(piece + arrival * gate_ref[span, lanes].astype(F32))
        normed_ref[span, :] = finish_rows(jnp.concatenate(pieces, axis=1), norm_ref[...])

    padded = slocal_ref.shape[0]
    few_rows = reply_got.shape[0]
    srows = pl.ds(tokens, padded)

    def answer():
        picked_all[last_seat] = picked_ref[...]
        others = picked_all.at[pl.ds(0, peers - 1)]
        remote(others, others, small_ssems.at[0], picked_sems.at[0], {"ctx": 0}).wait_recv()
        asked = picked_all[...].reshape(peers * padded, entries)
        for q in range(groups):
            lanes = group_lanes(q)
            entered = enter_ref[:, lanes].astype(F32) * pair_scale[0:1, lanes]
            final = entered + mine_state[:, lanes].astype(F32)
            told = dot(asked, final.astype(BF16))
            for p in range(peers - 1):
                reply_ref[p, :, lanes] = told[p * padded : p * padded + few_rows]
            reply_got[:, lanes] = told[last_seat * padded : last_seat * padded + few_rows]
        for p in range(peers - 1):
            reply_copy(p).start()

    def finish_samples():
        @pl.when(jnp.logical_not(holds_final))
        def _():
            reply_copy(0).wait_recv()

        total = slocal_ref[:few_rows] + reply_got[...] * sgain_ref[:few_rows]
        normed = finish_rows(total, norm_ref[...])
        if few_rows < padded:
            normed = jnp.concatenate([normed, jnp.zeros((padded - few_rows, channels), BF16)], axis=0)
        normed_ref[srows, :] = normed

    few = sresult_ref.shape[0]

    def sshare(d):
        wide = dot(normed_ref[srows, :], tiles_ref[:, pl.ds(pl.multiple_of(d * cols, cols), cols)])
        return jnp.concatenate([wide[:few, q * LANES : (q + 1) * LANES] for q in range(cols // LANES)], axis=0)

    def spass_on(d, slot, move, fed):
        sown_ref[...] = sshare(d)

        @pl.when(fed)
        def _():
            move(d).wait_recv()
            sown_ref[...] = sown_ref[...] + slanding[slot].astype(F32)

        ssent[d] = sown_ref[...].astype(BF16)
        move(d).start()

    sample_start = PARTS * (blocks + 1)

    def step(t, carry):
        block, first_part, last_part = t // PARTS, t % PARTS == 0, t % PARTS == PARTS - 1

        @pl.when((block < blocks) & first_part)
        def _():
            finish_block(block)

        @pl.when(t == sample_start)
        def _():
            finish_samples()

        rising, falling = t - place, t - (n - 1 - place)
        up, down = n - 1 - rising // per, falling // per

        @pl.when((rising >= 0) & (up > place))
        def _():
            pass_on(up, rising % per, up + 1, hop_up, place > 0)

        @pl.when((falling >= 0) & (down < place))
        def _():
            pass_on(down, falling % per, down, hop_down, place < n - 1)

        srising, sfalling = rising - sample_start, falling - sample_start
        sup, sdown = n - 1 - srising, sfalling

        @pl.when((srising >= 0) & (sup > place))
        def _():
            spass_on(sup, sup + 1, shop_up, place > 0)

        @pl.when((sfalling >= 0) & (sdown < place))
        def _():
            spass_on(sdown, sdown, shop_down, place < n - 1)

        @pl.when((block + 1 < blocks) & last_part)
        def _():
            block_local(block + 1, None)

        @pl.when((block == blocks - 2) & last_part)
        def _():
            sample_local()

            @pl.when(jnp.logical_not(holds_final))
            def _():
                picked_copy(seat).start()

        @pl.when((block == blocks - 1) & last_part & holds_final)
        def _():
            answer()

        return carry

    lax.fori_loop(0, (n - 1) * per, step, 0)
    sown_ref[...] = sshare(place)

    @pl.when(place < n - 1)
    def _():
        shop_down(place).wait_recv()
        sown_ref[...] = sown_ref[...] + slanding[place].astype(F32)

    @pl.when(place > 0)
    def _():
        shop_up(place).wait_recv()
        sown_ref[...] = sown_ref[...] + slanding[place + 1].astype(F32)

    for q in range(cols // LANES):
        sresult_ref[:, q * LANES : (q + 1) * LANES] = sown_ref[q * few : (q + 1) * few, :].astype(BF16)
    sout_copy = pltpu.make_async_copy(sresult_ref, sout_hbm, late_sems.at[len(late)])
    sout_copy.start()

    remote(
        mine_state.at[other_rows], pair_state, pair_ssems.at[0], pair_rsems.at[0], {"ctx": mate(0)}
    ).wait_send()
    swap_copy(slice(0, channels), own_rows).wait_send()

    def scan_sent(s, count):
        span = pl.ds(0, count)
        remote(
            totals.at[s - 1, span],
            arrived.at[s - 1, span],
            scan_ssems.at[s - 1],
            scan_rsems.at[s - 1, 0],
            {"ctx": mate(1)},
        ).wait_send()

    for s in range(1, scan_steps + 1):
        if not squared:
            scan_sent(s, chunks)
        elif s == 1:

            @pl.when((column == 0) & (row == 0))
            def _():
                scan_sent(1, chunks)

            @pl.when(column + row == 1)
            def _():
                scan_sent(1, pairs)

        else:

            @pl.when(row == s - 2)
            def _():
                scan_sent(s, pairs)

    for s in range(log_steps):
        log_copy(s).wait_send()

    @pl.when(holds_final)
    def _():
        remote(reply_ref, reply_ref, reply_sems.at[0], small_rsems.at[0], {"ctx": 0}).wait_send()

    @pl.when(jnp.logical_not(holds_final))
    def _():
        picked_copy(seat).wait_send()

    def out_place(b):
        return pl.ds(pl.multiple_of(b % PARTS * part, part), part), rows_of(b // PARTS)

    def gather(b, carry):
        acc_ref[...] = share(place, b)

        @pl.when(place < n - 1)
        def _():
            hop_down(place, b).wait_recv()
            acc_ref[...] = acc_ref[...] + landing[place, b].astype(F32)

        @pl.when(place > 0)
        def _():
            hop_up(place, b).wait_recv()
            acc_ref[...] = acc_ref[...] + landing[place + 1, b].astype(F32)

        where = out_place(b)
        result_ref[where] = turn_over(acc_ref[...]).astype(BF16)
        pltpu.make_async_copy(result_ref.at[where], out_hbm.at[where], out_sems.at[0]).start()
        return carry

    lax.fori_loop(0, per, gather, 0)
    for d in range(n):

        @pl.when(d > place)
        def _():
            all_up(d).wait_send()
            shop_up(d).wait_send()

        @pl.when(d < place)
        def _():
            all_down(d).wait_send()
            shop_down(d).wait_send()

    sout_copy.wait()
    pltpu.make_async_copy(result_ref, out_hbm, out_sems.at[0]).wait()


def hand_over_kernel(bands, mixed_hbm, smixed_hbm, out_hbm, sout_hbm, bands_ref, few_ref, sems):
    rows = mixed_hbm.shape[0] // bands
    moves = [(smixed_hbm, few_ref, sout_hbm)]
    for q in range(bands):
        part = pl.ds(q * rows, rows)
        moves.append((mixed_hbm.at[part], bands_ref.at[q], out_hbm.at[part]))
    ins = [pltpu.make_async_copy(a, b, sems.at[0, q]) for q, (a, b, _) in enumerate(moves)]
    outs = [pltpu.make_async_copy(b, c, sems.at[1, q]) for q, (_, b, c) in enumerate(moves)]
    for copy in ins:
        copy.start()
    for into, out in zip(ins, outs):
        into.wait()
        out.start()
    for copy in outs:
        copy.wait()


def per_device(
    prompt_values,
    prompt_gate,
    prompt_inject,
    prompt_read,
    prompt_step,
    decay_log,
    skip_gain,
    norm_weight,
    out_weight,
    sample_values,
    sample_gate,
    sample_inject,
    sample_read,
    sample_step,
    sample_length,
):
    n, peers = lax.axis_size("head"), lax.axis_size("ctx")
    levels = peers.bit_length() - 2
    scan_steps = 3 if levels == 2 else levels
    log_steps = 2 if levels == 2 else levels + 1
    tokens, channels = prompt_values.shape
    heads = prompt_step.shape[0]
    dim = channels // heads
    entries = prompt_inject.shape[2]
    half = entries // 2
    samples, length = sample_values.shape[:2]
    padded = -(-samples // (2 * PAD)) * 2 * PAD
    cols = out_weight.shape[1] // n
    blocks, chunks = tokens // BLOCK, channels // CHUNK
    part, per = cols // PARTS, blocks * PARTS
    vmem = pl.BlockSpec(memory_space=pltpu.VMEM)
    hbm = pl.BlockSpec(memory_space=pl.ANY)
    dma = pltpu.SemaphoreType.DMA
    shape = jax.ShapeDtypeStruct
    V = pltpu.VMEM
    mixed, smixed = pl.pallas_call(
        functools.partial(layer_kernel, dim, n, peers),
        out_shape=(shape((cols, tokens), BF16), shape((samples, cols), BF16)),
        in_specs=[
            pl.BlockSpec(memory_space=pltpu.SMEM),
            hbm,
            hbm,
            vmem,
            hbm,
            vmem,
            vmem,
            vmem,
            vmem,
            hbm,
            hbm,
            hbm,
            hbm,
            hbm,
            hbm,
        ],
        out_specs=(hbm, hbm),
        scratch_shapes=[
            V((tokens, channels), BF16),
            V((tokens, channels), BF16),
            V((tokens, entries), BF16),
            V(sample_values.shape, BF16),
            V(sample_gate.shape, BF16),
            V((samples, length, entries), BF16),
            V((samples, length, entries), BF16),
            V((samples, length, heads), F32),
            V(out_weight.shape, BF16),
            V((blocks, heads, BLOCK), F32),
            V((blocks, heads, BLOCK), F32),
            V((tokens, 2 * heads), BF16),
            V((2 * heads, channels), BF16),
            V((entries, tokens), BF16),
            V((PAD, channels), F32),
            V((entries, channels), BF16),
            V((half, channels), BF16),
            V((levels + 1, chunks, half, CHUNK), BF16),
            V((scan_steps, chunks, half, CHUNK), BF16),
            V((chunks, half, CHUNK), F32),
            V((half, channels), BF16),
            V((entries, channels), BF16),
            V((log_steps, PAD, heads), F32),
            V((log_steps, PAD, heads), F32),
            V((PAD, heads), F32),
            V((PAD, channels), F32),
            V((levels, PAD, channels), F32),
            V((entries, channels), F32),
            V((PAD, heads), F32),
            V((BLOCK, channels), F32),
            V((tokens + padded, channels), BF16),
            V((padded, channels), F32),
            V((padded, channels), F32),
            V((padded, entries), BF16),
            V((peers, padded, entries), BF16),
            V((peers - 1, -(-samples // PAD) * PAD, channels), F32),
            V((-(-samples // PAD) * PAD, channels), F32),
            V((BLOCK, part), F32),
            V((n, per, BLOCK, part), BF16),
            V((n + 1, per, BLOCK, part), BF16),
            V((n, samples * cols // LANES, LANES), BF16),
            V((n + 1, samples * cols // LANES, LANES), BF16),
            V((samples * cols // LANES, LANES), F32),
            V((cols, tokens), BF16),
            V((samples, cols), BF16),
            dma((chunks // GROUP,)),
            dma((8,)),
            dma((1,)),
            dma((1,)),
            dma((log_steps,)),
            dma((log_steps,)),
            dma((1,)),
            dma((chunks // GROUP,)),
            dma((scan_steps,)),
            dma((2 if levels == 2 else levels, chunks)),
            dma((1,)),
            dma((1,)),
            dma((1,)),
            dma((1,)),
            dma((1,)),
            dma((1,)),
            dma((n,)),
            dma((n + 1, per)),
            dma((n,)),
            dma((n + 1,)),
        ],
        compiler_params=pltpu.CompilerParams(
            collective_id=0, has_side_effects=True, vmem_limit_bytes=VMEM_LIMIT
        ),
    )(
        sample_length,
        prompt_values,
        prompt_gate,
        prompt_inject.reshape(tokens, entries),
        prompt_read.reshape(tokens, entries),
        prompt_step,
        decay_log[None],
        skip_gain[None],
        norm_weight[None],
        out_weight,
        sample_values,
        sample_gate,
        sample_inject.reshape(samples, length, entries),
        sample_read.reshape(samples, length, entries),
        sample_step.transpose(1, 2, 0),
    )
    bands = 4
    band = (cols // bands, tokens)
    mixed, smixed = pl.pallas_call(
        functools.partial(hand_over_kernel, bands),
        out_shape=(shape((cols, tokens), BF16), shape((samples, cols), BF16)),
        in_specs=[hbm, hbm],
        out_specs=(hbm, hbm),
        scratch_shapes=[
            V((bands, *band), BF16),
            V((samples, cols), BF16),
            dma((2, bands + 1)),
        ],
    )(mixed, smixed)
    return mixed, smixed.T


def solution(mesh):
    in_specs = (
        P("ctx", "head"),
        P("ctx", "head"),
        P("ctx", "head", None),
        P("ctx", "head", None),
        P("head", "ctx"),
        P("head"),
        P("head"),
        P("head"),
        P("head", None),
        P("ctx", None, "head"),
        P("ctx", None, "head"),
        P("ctx", None, "head", None),
        P("ctx", None, "head", None),
        P("head", "ctx", None),
        P("ctx"),
    )
    out_specs = (P("head", "ctx"), P("head", "ctx"))
    return jax.shard_map(
        per_device, mesh=mesh, in_specs=in_specs, out_specs=out_specs, check_vma=False
    )
```

```python
import functools

import jax
import jax.numpy as jnp
from jax import lax
from jax.experimental import pallas as pl
from jax.experimental.pallas import tpu as pltpu
from jax.sharding import PartitionSpec as P

BLOCK = 128
LANES = 128
PAD = 8
F32 = jnp.float32
BF16 = jnp.bfloat16
EXACT = lax.Precision.HIGHEST
VMEM_LIMIT = 60 * 1024 * 1024


def dot(a, b, dims=((1,), (0,)), precision=None):
    return lax.dot_general(a, b, (dims, ((), ())), precision=precision, preferred_element_type=F32)


def softplus(v):
    return jnp.maximum(v, 0.0) + jnp.log1p(jnp.exp(-jnp.abs(v)))


def silu(v):
    return v / (1.0 + jnp.exp(-v))


def spread(w, expander):
    high = w.astype(BF16)
    low = (w - high.astype(F32)).astype(BF16)
    return dot(jnp.concatenate([high, low], axis=1), expander)


def expander_of(heads, dim):
    row = lax.broadcasted_iota(jnp.int32, (2 * heads, heads * dim), 0)
    lane = lax.broadcasted_iota(jnp.int32, (2 * heads, heads * dim), 1)
    head = lane // dim
    return jnp.where((row == head) | (row == head + heads), 1.0, 0.0).astype(BF16)


def square(n):
    return (
        lax.broadcasted_iota(jnp.int32, (n, n), 0),
        lax.broadcasted_iota(jnp.int32, (n, n), 1),
    )


def finish_rows(total, weight):
    mean = jnp.mean(total * total, axis=1, keepdims=True)
    return (total * lax.rsqrt(mean + 1e-05) * weight).astype(BF16)


CHUNK = 2 * LANES
GROUP = 2
PARTS = 2
LAG = 3
HOOKS = 4


def turn_over(w):
    return jnp.transpose(w, (1, 0))


def layer_kernel(
    dim,
    n,
    peers,
    length_ref,
    values_hbm,
    gate_hbm,
    inject_ref,
    read_hbm,
    step_ref,
    decay_ref,
    gain_in_ref,
    norm_ref,
    weight_hbm,
    svalues_hbm,
    sgate_hbm,
    sinject_hbm,
    sread_hbm,
    sstep_hbm,
    out_hbm,
    sout_hbm,
    values_ref,
    gate_ref,
    read_ref,
    svalues_ref,
    sgate_ref,
    sinject_ref,
    sread_ref,
    sstep_ref,
    tiles_ref,
    steps_ref,
    logs_ref,
    wide_ref,
    expander_ref,
    turned_ref,
    skip_ref,
    mine_state,
    pair_state,
    totals,
    arrived,
    before_ref,
    swap_ref,
    enter_ref,
    log_sent,
    log_got,
    before_logs,
    pair_scale,
    scale_ref,
    state_ref,
    offset_ref,
    part_ref,
    normed_ref,
    slocal_ref,
    sgain_ref,
    picked_ref,
    picked_all,
    reply_ref,
    reply_got,
    acc_ref,
    sent,
    landing,
    ssent,
    slanding,
    sown_ref,
    result_ref,
    sresult_ref,
    value_sems,
    late_sems,
    tile_sems,
    out_sems,
    log_ssems,
    log_rsems,
    pair_ssems,
    pair_rsems,
    scan_ssems,
    scan_rsems,
    swap_ssems,
    swap_rsems,
    small_ssems,
    small_rsems,
    picked_sems,
    reply_sems,
    sent_sems,
    land_sems,
    ssent_sems,
    sland_sems,
):
    tokens, channels = values_ref.shape
    heads = step_ref.shape[0]
    entries = inject_ref.shape[1]
    half = entries // 2
    cols = weight_hbm.shape[1] // n
    part = acc_ref.shape[1]
    per = sent.shape[1]
    chunks = channels // CHUNK
    blocks = tokens // BLOCK
    levels = peers.bit_length() - 2
    squared = levels == 2
    log_steps = 2 if squared else levels + 1
    scan_steps = arrived.shape[0]
    place = lax.axis_index("head")
    seat = lax.axis_index("ctx")
    side = seat % 2
    odd = side == 1
    own_rows = pl.ds(pl.multiple_of(side * half, half), half)
    other_rows = pl.ds(pl.multiple_of((1 - side) * half, half), half)

    def lanes_of(c):
        return slice(c * CHUNK, (c + 1) * CHUNK)

    def some_lanes(c):
        return pl.ds(pl.multiple_of(c * CHUNK, CHUNK), CHUNK)

    groups = chunks // GROUP

    def group_lanes(q):
        return slice(q * GROUP * CHUNK, (q + 1) * GROUP * CHUNK)

    def value_copy(q):
        lanes = group_lanes(q)
        return pltpu.make_async_copy(values_hbm.at[:, lanes], values_ref.at[:, lanes], value_sems.at[q])

    late = [
        (gate_hbm, gate_ref),
        (read_hbm, read_ref),
        (svalues_hbm, svalues_ref),
        (sgate_hbm, sgate_ref),
        (sinject_hbm, sinject_ref),
        (sread_hbm, sread_ref),
        (sstep_hbm, sstep_ref),
    ]
    late_copies = [pltpu.make_async_copy(*refs, late_sems.at[q]) for q, refs in enumerate(late)]

    tile_copy = pltpu.make_async_copy(weight_hbm, tiles_ref, tile_sems.at[0])

    for q in range(groups):
        value_copy(q).start()

    def digit(s):
        return (seat // (1 << s)) % 2

    def mate(s):
        return seat + (1 << s) - (2 << s) * digit(s)

    barrier = pltpu.get_barrier_semaphore()

    def greet(device):
        pl.semaphore_signal(
            barrier, inc=1, device_id=device, device_id_type=pl.DeviceIdType.MESH
        )

    for s in range(levels + 1):
        greet({"ctx": mate(s)})

    last_seat = peers - 1
    holds_final = seat == last_seat

    @pl.when(holds_final)
    def _():
        for p in range(peers - 1):
            greet({"ctx": p})

    @pl.when(jnp.logical_not(holds_final))
    def _():
        greet({"ctx": last_seat})

    @pl.when(place > 0)
    def _():
        greet({"head": place - 1})

    @pl.when(place < n - 1)
    def _():
        greet({"head": place + 1})

    rows, lanes = square(heads)
    rate_row = -jnp.exp(decay_ref[...])
    rate = jnp.sum(jnp.where(rows == lanes, rate_row, 0.0), axis=1, keepdims=True)
    steps = softplus(step_ref[...])
    logs = steps * rate
    i, j = square(BLOCK)

    def fill_expander():
        expander_ref[...] = expander_of(heads, dim)

    fill_expander()
    def stack(ref, wide):
        for b in range(blocks):
            ref[b] = wide[:, b * BLOCK : (b + 1) * BLOCK]
        return ref[...].reshape(blocks * heads, BLOCK)

    tall_steps, tall_logs = stack(steps_ref, steps), stack(logs_ref, logs)
    after = dot(tall_logs, jnp.where(i > j, 1.0, 0.0), precision=EXACT)
    sums = jnp.sum(tall_logs, axis=1, keepdims=True)
    later, offsets = jnp.zeros((heads, 1), F32), []
    for b in reversed(range(blocks)):
        offsets.insert(0, later)
        later = later + sums[b * heads : (b + 1) * heads]
    w = turn_over(jnp.exp(after + jnp.concatenate(offsets, axis=0)) * tall_steps)
    for b in range(blocks):
        block_w = w[:, b * heads : (b + 1) * heads]
        high = block_w.astype(BF16)
        low = (block_w - high.astype(F32)).astype(BF16)
        wide_ref[b * BLOCK : (b + 1) * BLOCK, :] = jnp.concatenate([high, low], axis=1)
    total_logs = jnp.sum(jnp.where(rows == lanes, later, 0.0), axis=0, keepdims=True)
    total_logs = jnp.broadcast_to(total_logs, (PAD, heads))

    def turn_inject():
        turned_ref[...] = turn_over(inject_ref[...].astype(F32)).astype(BF16)

    turn_inject()
    top = lax.broadcasted_iota(jnp.int32, (PAD, heads), 0) == 0

    inside = (place > 0) & (place < n - 1)
    log_sent[0] = total_logs
    before_logs[...] = jnp.zeros_like(before_logs)

    def state_of(q):
        lanes = group_lanes(q)
        value_copy(q).wait()
        wide = dot(wide_ref[...], expander_ref[:, lanes])
        scaled = (wide * values_ref[:, lanes].astype(F32)).astype(BF16)
        mine_state[:, lanes] = dot(turned_ref[...], scaled).astype(BF16)

    state_of(0)

    for middle in (False, True):
        for final in (False, True):

            @pl.when((inside == middle) & (holds_final == final))
            def _():
                pl.semaphore_wait(barrier, levels + 2 + middle + (peers - 1 if final else 1))

    def remote(src, dst, ssem, rsem, device):
        return pltpu.make_async_remote_copy(
            src_ref=src,
            dst_ref=dst,
            send_sem=ssem,
            recv_sem=rsem,
            device_id=device,
            device_id_type=pl.DeviceIdType.MESH,
        )

    def log_copy(s):
        return remote(
            log_sent.at[s], log_got.at[s], log_ssems.at[s], log_rsems.at[s], {"ctx": mate(s)}
        )

    def pair_copy(q):
        return remote(
            mine_state.at[other_rows, group_lanes(q)],
            pair_state.at[:, group_lanes(q)],
            pair_ssems.at[0],
            pair_rsems.at[q],
            {"ctx": mate(0)},
        )

    def scan_copy(s, c):
        slot = c // 2 + (s - 2) * (chunks // 2) if squared and s > 1 else c
        return remote(
            totals.at[s - 1, c],
            arrived.at[s - 1, c],
            scan_ssems.at[s - 1],
            scan_rsems.at[s - 1 if not squared or s == 1 else 1, slot],
            {"ctx": mate(1 if squared and s == 3 else s)},
        )

    def swap_copy(lanes, where):
        return remote(
            swap_ref.at[:, lanes],
            enter_ref.at[where, lanes],
            swap_ssems.at[0],
            swap_rsems.at[0],
            {"ctx": mate(0)},
        )

    log_copy(0).start()

    def exchange_logs(s):
        log_copy(s).wait_recv()
        got, own = log_got[s], log_sent[s]
        upper = digit(s) == 1
        above = jnp.where(upper, own, got)
        if s == 0:
            pair = jnp.where(top, above, jnp.where(odd, got, own))
            pair_scale[...] = spread(jnp.exp(pair), expander_ref[...])
        else:
            held = before_logs[...]
            crossed = jnp.where(digit(2) == 1, jnp.where(upper, got, own), above) if squared else above
            scale_ref[s - 1] = spread(jnp.exp(jnp.where(top, crossed, held)), expander_ref[...])
            before_logs[...] = held + jnp.where(upper, got, 0.0)
        if s < log_steps - 1:
            log_sent[s + 1] = own + got
            log_copy(s + 1).start()

    column, row = digit(1), digit(2)

    def at_once(c):
        if not squared:
            return seat >= 0
        if c % 2:
            return column == 0
        return (column == 1) & (row == 0)

    def pair_up(c):
        mine = mine_state[own_rows, lanes_of(c)].astype(F32)
        theirs = pair_state[:, lanes_of(c)].astype(F32)
        first, second = jnp.where(odd, theirs, mine), jnp.where(odd, mine, theirs)
        totals[0, c] = (first * pair_scale[0:1, lanes_of(c)] + second).astype(BF16)

        @pl.when(at_once(c))
        def _():
            scan_copy(1, c).start()

    pairs = chunks // 2

    def pair_group(q):
        pair_copy(q).wait_recv()
        for c in sorted(range(q * GROUP, (q + 1) * GROUP), key=lambda c: 1 - c % 2):
            pair_up(c)

    for q in range(groups):
        if q:
            state_of(q)
        pair_copy(q).start()
        if q == 0:
            for copy in late_copies:
                copy.start()
        if q == 1:
            exchange_logs(0)
        if q:
            pair_group(q - 1)
    pair_group(groups - 1)
    if squared:
        for c in range(0, chunks, 2):

            @pl.when((column == 0) & (row == 0))
            def _():
                scan_copy(1, c).start()

    def enter(c, before):
        even_state = jnp.where(odd, pair_state[:, some_lanes(c)].astype(F32), mine_state[own_rows, some_lanes(c)].astype(F32))
        moved = before * pair_scale[1:2, some_lanes(c)] + even_state
        enter_ref[own_rows, some_lanes(c)] = jnp.where(odd, moved, before).astype(BF16)
        swap_ref[:, some_lanes(c)] = jnp.where(odd, before, moved).astype(BF16)
        swap_copy(some_lanes(c), own_rows).start()

    def cross_row(q):
        c = 2 * q + column
        scan_copy(1, c).wait_recv()
        far, near = arrived[0, c].astype(F32), totals[0, c].astype(F32)
        right = column == 1
        first, second = jnp.where(right, far, near), jnp.where(right, near, far)
        totals[1, c] = (first * scale_ref[0, 0:1, some_lanes(c)] + second).astype(BF16)
        scan_copy(2, c).start()
        enter(c, jnp.where(right, far, 0.0))

        @pl.when(column == 0)
        def _():
            enter(c + 1, jnp.zeros((half, CHUNK), F32))

    def end_row(q):
        @pl.when(column == 1)
        def _():
            scan_copy(1, 2 * q).wait_recv()
            enter(2 * q, arrived[0, 2 * q].astype(F32))

    def next_row(q):
        c = 2 * q + column
        right = column == 1

        @pl.when(right)
        def _():
            scan_copy(1, c).wait_recv()
            totals[0, c] = arrived[0, c]

        scan_copy(2, c).wait_recv()
        far = arrived[1, c].astype(F32)
        joined = far * scale_ref[0, 0:1, some_lanes(c)] + totals[0, c].astype(F32)
        totals[2, c] = jnp.where(right, far, joined).astype(BF16)
        scan_copy(3, c).start()
        enter(c, jnp.where(right, joined, far))

    def last_column(q):
        c = 2 * q + 1 - column
        scan_copy(3, c).wait_recv()
        enter(c, arrived[2, c].astype(F32))

    def square_events():
        first = [(q, cross_row, q) for q in range(pairs)]
        first += [(q + pairs, end_row, q) for q in range(pairs)]
        second = [(q, next_row, q) for q in range(pairs)]
        second += [(q + 2.5, last_column, q) for q in range(pairs)]
        return [sorted(events, key=lambda event: event[0]) for events in (first, second)]

    def run_events(here, events):
        @pl.when(here)
        def _():
            for _, work, q in events:
                work(q)

    def scan_step(s, c):
        scan_copy(s, c).wait_recv()
        upper = digit(s) == 1
        far = arrived[s - 1, c].astype(F32)
        near = totals[s - 1, c].astype(F32)
        first, second = jnp.where(upper, far, near), jnp.where(upper, near, far)
        total_scale = scale_ref[s - 1, 0:1, some_lanes(c)]
        totals[s, c] = (first * total_scale + second).astype(BF16)
        if s == 1:
            before = jnp.where(upper, far, 0.0)
        else:
            held = before_ref[c]
            before = jnp.where(upper, far * scale_ref[s - 1, 1:2, some_lanes(c)] + held, held)
        if s < levels:
            before_ref[c] = before
            scan_copy(s + 1, c).start()
        else:
            enter(c, before)

    exchange_logs(1)

    skip_ref[...] = spread(jnp.broadcast_to(gain_in_ref[...], (PAD, heads)), expander_ref[...])

    def sample_local():
        samples, length = svalues_ref.shape[:2]
        slocal_ref[...] = jnp.zeros_like(slocal_ref)
        sgain_ref[...] = jnp.zeros_like(sgain_ref)
        picked_ref[...] = jnp.zeros_like(picked_ref)
        u, s = square(length)
        own = lax.broadcasted_iota(jnp.int32, (heads, channels), 1) // dim == (
            lax.broadcasted_iota(jnp.int32, (heads, channels), 0)
        )
        at = lax.broadcasted_iota(jnp.int32, (1, length), 1)
        for k in range(samples):
            last = length_ref[k] - 1
            hot = jnp.where(
                lax.broadcasted_iota(jnp.int32, (PAD, length), 1) == last, 1.0, 0.0
            ).astype(BF16)
            tall = softplus(sstep_ref[k])
            tall_logs = tall * rate_row
            flip = ((0,), (0,))
            gap = dot(tall_logs, jnp.where((u > s) & (u <= last), 1.0, 0.0), flip, EXACT)
            running = dot(tall_logs, jnp.where(u <= last, 1.0, 0.0), flip, EXACT)[:, 0:1]
            wide_steps = dot(tall, jnp.where(u == s, 1.0, 0.0), flip, EXACT)
            row = dot(hot, sread_ref[k])
            score = dot(row.astype(BF16), sinject_ref[k], ((1,), (1,)))[0:1]
            mixing = jnp.where(at <= last, score * jnp.exp(gap) * wide_steps, 0.0).astype(BF16)
            values = svalues_ref[k]
            local = jnp.sum(jnp.where(own, dot(mixing, values), 0.0), axis=0, keepdims=True)
            decay = jnp.sum(jnp.where(own, jnp.exp(running), 0.0), axis=0, keepdims=True)
            value = dot(hot, values)[0:1]
            opened = silu(dot(hot, sgate_ref[k])[0:1])
            slocal_ref[k : k + 1, :] = (local + skip_ref[0:1, :] * value) * opened
            sgain_ref[k : k + 1, :] = decay * opened
            picked_ref[k : k + 1, :] = row[0:1].astype(BF16)

    state_ref[...] = jnp.zeros_like(state_ref)
    offset_ref[...] = jnp.zeros_like(offset_ref)
    for copy in late_copies:
        copy.wait()
    tile_copy.start()

    def block_local(b, hook):
        span = pl.ds(pl.multiple_of(b * BLOCK, BLOCK), BLOCK)
        steps, logs = steps_ref[b], logs_ref[b]
        i, j = square(BLOCK)
        lower = jnp.where(i >= j, 1.0, 0.0)
        running = dot(logs, lower, ((1,), (1,)), EXACT)
        running_t = turn_over(running)
        after = turn_over(dot(logs, jnp.where(i > j, 1.0, 0.0), precision=EXACT))
        turned = turn_over(steps)
        expander = expander_ref[...]
        inject = inject_ref[span, :]
        readout = read_ref[span, :]
        scores = jnp.where(i >= j, dot(readout, inject, ((1,), (1,))), 0.0)
        per = LANES // dim
        lane = lax.broadcasted_iota(jnp.int32, (BLOCK, LANES), 1)
        for k in range(heads // per):
            cut = slice(k * LANES, (k + 1) * LANES)
            pair = values_ref[span, cut]
            mixes, parts = [], []
            for q in range(per):
                h = k * per + q
                gap = jnp.minimum(running_t[:, h : h + 1] - running[h : h + 1, :], 0.0)
                mixes.append((scores * jnp.exp(gap) * steps[h : h + 1, :]).astype(BF16))
                parts.append(jnp.where(lane // dim == q, pair, jnp.zeros_like(pair)))
            part_ref[:, cut] = dot(jnp.concatenate(mixes, axis=1), jnp.concatenate(parts, axis=0))
            if hook is not None and 2 * (k + 1) == heads // per:
                hook(HOOKS * b)
        if hook is not None:
            hook(HOOKS * b + 1)
        decay = spread(jnp.exp(running_t), expander)
        values = values_ref[span, :].astype(F32)
        opened = silu(gate_ref[span, :].astype(F32))
        total = part_ref[...] + skip_ref[0:1, :] * values
        total = total + dot(readout, state_ref[...].astype(BF16)) * decay
        normed_ref[span, :] = (total * opened).astype(BF16)
        if hook is not None:
            hook(HOOKS * b + 2)
        offset = offset_ref[0:1, :]
        gate_ref[span, :] = (opened * spread(jnp.exp(running_t + offset), expander)).astype(BF16)
        offset_ref[0:1, :] = offset + running_t[BLOCK - 1 : BLOCK, :]
        scaled = (spread(jnp.exp(after) * turned, expander) * values).astype(BF16)
        state_ref[...] = state_ref[...] * decay[BLOCK - 1 : BLOCK, :] + dot(
            inject, scaled, ((0,), (0,))
        )
        if hook is not None:
            hook(HOOKS * b + 3)

    def hook(g):
        if squared:
            run_events(row == 0, square_events()[0][g : g + 1])
            return

        for s in range(2, levels + 1):

            @pl.when(g == s - 1)
            def _():
                exchange_logs(s)

        for s in range(1, levels + 1):
            c = g - LAG * (s - 1)

            @pl.when((c >= 0) & (c < chunks))
            def _():
                scan_step(s, c)

    def picked_copy(p):
        return remote(
            picked_ref, picked_all.at[p], small_ssems.at[0], picked_sems.at[0], {"ctx": last_seat}
        )

    def reply_copy(p):
        return remote(
            reply_ref.at[p], reply_got, reply_sems.at[0], small_rsems.at[0], {"ctx": p}
        )

    def late_round(g, carry):
        hook(g)
        return carry

    block_local(0, hook)
    if squared:
        first, second = square_events()
        run_events(row == 0, first[HOOKS:])
        run_events(row == 1, second)
    else:
        lax.fori_loop(HOOKS, max(chunks + LAG * (levels - 1), HOOKS), late_round, 0)
    swap_copy(slice(0, channels), other_rows).wait_recv()
    tile_copy.wait()

    def share(d, q):
        rows = rows_of(q // PARTS)
        start = pl.multiple_of(d * cols + q % PARTS * part, part)
        return dot(normed_ref[rows, :], tiles_ref[:, pl.ds(start, part)])

    def hop_up(d, b):
        return remote(
            sent.at[d, b],
            landing.at[d + 1, b],
            sent_sems.at[d],
            land_sems.at[d + 1, b],
            {"head": place + 1},
        )

    def hop_down(d, b):
        return remote(
            sent.at[d, b],
            landing.at[d, b],
            sent_sems.at[d],
            land_sems.at[d, b],
            {"head": place - 1},
        )

    def all_up(d):
        return remote(
            sent.at[d], landing.at[d + 1], sent_sems.at[d], land_sems.at[0, 0], {"head": place + 1}
        )

    def all_down(d):
        return remote(
            sent.at[d], landing.at[d], sent_sems.at[d], land_sems.at[0, 0], {"head": place - 1}
        )

    def shop_up(d):
        return remote(
            ssent.at[d],
            slanding.at[d + 1],
            ssent_sems.at[d],
            sland_sems.at[d + 1],
            {"head": place + 1},
        )

    def shop_down(d):
        return remote(
            ssent.at[d], slanding.at[d], ssent_sems.at[d], sland_sems.at[d], {"head": place - 1}
        )

    def rows_of(b):
        return pl.ds(pl.multiple_of(b * BLOCK, BLOCK), BLOCK)

    def pass_on(d, b, slot, move, fed):
        acc_ref[...] = share(d, b)

        @pl.when(fed)
        def _():
            move(d, b).wait_recv()
            acc_ref[...] = acc_ref[...] + landing[slot, b].astype(F32)

        sent[d, b] = acc_ref[...].astype(BF16)
        move(d, b).start()

    def finish_block(b):
        span = rows_of(b)
        readout = read_ref[span, :]
        pieces = []
        for q in range(groups):
            lanes = group_lanes(q)
            arrival = dot(readout, enter_ref[:, lanes])
            piece = normed_ref[span, lanes].astype(F32)
            pieces.append(piece + arrival * gate_ref[span, lanes].astype(F32))
        normed_ref[span, :] = finish_rows(jnp.concatenate(pieces, axis=1), norm_ref[...])

    padded = slocal_ref.shape[0]
    few_rows = reply_got.shape[0]
    srows = pl.ds(tokens, padded)

    def answer():
        picked_all[last_seat] = picked_ref[...]
        others = picked_all.at[pl.ds(0, peers - 1)]
        remote(others, others, small_ssems.at[0], picked_sems.at[0], {"ctx": 0}).wait_recv()
        asked = picked_all[...].reshape(peers * padded, entries)
        for q in range(groups):
            lanes = group_lanes(q)
            entered = enter_ref[:, lanes].astype(F32) * pair_scale[0:1, lanes]
            final = entered + mine_state[:, lanes].astype(F32)
            told = dot(asked, final.astype(BF16))
            for p in range(peers - 1):
                reply_ref[p, :, lanes] = told[p * padded : p * padded + few_rows]
            reply_got[:, lanes] = told[last_seat * padded : last_seat * padded + few_rows]
        for p in range(peers - 1):
            reply_copy(p).start()

    def finish_samples():
        @pl.when(jnp.logical_not(holds_final))
        def _():
            reply_copy(0).wait_recv()

        total = slocal_ref[:few_rows] + reply_got[...] * sgain_ref[:few_rows]
        normed = finish_rows(total, norm_ref[...])
        if few_rows < padded:
            normed = jnp.concatenate([normed, jnp.zeros((padded - few_rows, channels), BF16)], axis=0)
        normed_ref[srows, :] = normed

    few = sresult_ref.shape[0]

    def sshare(d):
        wide = dot(normed_ref[srows, :], tiles_ref[:, pl.ds(pl.multiple_of(d * cols, cols), cols)])
        return jnp.concatenate([wide[:few, q * LANES : (q + 1) * LANES] for q in range(cols // LANES)], axis=0)

    def spass_on(d, slot, move, fed):
        sown_ref[...] = sshare(d)

        @pl.when(fed)
        def _():
            move(d).wait_recv()
            sown_ref[...] = sown_ref[...] + slanding[slot].astype(F32)

        ssent[d] = sown_ref[...].astype(BF16)
        move(d).start()

    sample_start = PARTS * (blocks + 1)

    def step(t, carry):
        block, first_part, last_part = t // PARTS, t % PARTS == 0, t % PARTS == PARTS - 1

        @pl.when((block < blocks) & first_part)
        def _():
            finish_block(block)

        @pl.when(t == sample_start)
        def _():
            finish_samples()

        rising, falling = t - place, t - (n - 1 - place)
        up, down = n - 1 - rising // per, falling // per

        @pl.when((rising >= 0) & (up > place))
        def _():
            pass_on(up, rising % per, up + 1, hop_up, place > 0)

        @pl.when((falling >= 0) & (down < place))
        def _():
            pass_on(down, falling % per, down, hop_down, place < n - 1)

        srising, sfalling = rising - sample_start, falling - sample_start
        sup, sdown = n - 1 - srising, sfalling

        @pl.when((srising >= 0) & (sup > place))
        def _():
            spass_on(sup, sup + 1, shop_up, place > 0)

        @pl.when((sfalling >= 0) & (sdown < place))
        def _():
            spass_on(sdown, sdown, shop_down, place < n - 1)

        @pl.when((block + 1 < blocks) & last_part)
        def _():
            block_local(block + 1, None)

        @pl.when((block == blocks - 2) & last_part)
        def _():
            sample_local()

            @pl.when(jnp.logical_not(holds_final))
            def _():
                picked_copy(seat).start()

        @pl.when((block == blocks - 1) & last_part & holds_final)
        def _():
            answer()

        return carry

    lax.fori_loop(0, (n - 1) * per, step, 0)
    sown_ref[...] = sshare(place)

    @pl.when(place < n - 1)
    def _():
        shop_down(place).wait_recv()
        sown_ref[...] = sown_ref[...] + slanding[place].astype(F32)

    @pl.when(place > 0)
    def _():
        shop_up(place).wait_recv()
        sown_ref[...] = sown_ref[...] + slanding[place + 1].astype(F32)

    for q in range(cols // LANES):
        sresult_ref[:, q * LANES : (q + 1) * LANES] = sown_ref[q * few : (q + 1) * few, :].astype(BF16)
    sout_copy = pltpu.make_async_copy(sresult_ref, sout_hbm, late_sems.at[len(late)])
    sout_copy.start()

    remote(
        mine_state.at[other_rows], pair_state, pair_ssems.at[0], pair_rsems.at[0], {"ctx": mate(0)}
    ).wait_send()
    swap_copy(slice(0, channels), own_rows).wait_send()

    def scan_sent(s, count):
        span = pl.ds(0, count)
        remote(
            totals.at[s - 1, span],
            arrived.at[s - 1, span],
            scan_ssems.at[s - 1],
            scan_rsems.at[s - 1, 0],
            {"ctx": mate(1)},
        ).wait_send()

    for s in range(1, scan_steps + 1):
        if not squared:
            scan_sent(s, chunks)
        elif s == 1:

            @pl.when((column == 0) & (row == 0))
            def _():
                scan_sent(1, chunks)

            @pl.when(column + row == 1)
            def _():
                scan_sent(1, pairs)

        else:

            @pl.when(row == s - 2)
            def _():
                scan_sent(s, pairs)

    for s in range(log_steps):
        log_copy(s).wait_send()

    @pl.when(holds_final)
    def _():
        remote(reply_ref, reply_ref, reply_sems.at[0], small_rsems.at[0], {"ctx": 0}).wait_send()

    @pl.when(jnp.logical_not(holds_final))
    def _():
        picked_copy(seat).wait_send()

    def out_place(b):
        return pl.ds(pl.multiple_of(b % PARTS * part, part), part), rows_of(b // PARTS)

    def gather(b, carry):
        acc_ref[...] = share(place, b)

        @pl.when(place < n - 1)
        def _():
            hop_down(place, b).wait_recv()
            acc_ref[...] = acc_ref[...] + landing[place, b].astype(F32)

        @pl.when(place > 0)
        def _():
            hop_up(place, b).wait_recv()
            acc_ref[...] = acc_ref[...] + landing[place + 1, b].astype(F32)

        where = out_place(b)
        result_ref[where] = turn_over(acc_ref[...]).astype(BF16)
        pltpu.make_async_copy(result_ref.at[where], out_hbm.at[where], out_sems.at[0]).start()
        return carry

    lax.fori_loop(0, per, gather, 0)
    for d in range(n):

        @pl.when(d > place)
        def _():
            all_up(d).wait_send()
            shop_up(d).wait_send()

        @pl.when(d < place)
        def _():
            all_down(d).wait_send()
            shop_down(d).wait_send()

    sout_copy.wait()
    pltpu.make_async_copy(result_ref, out_hbm, out_sems.at[0]).wait()


def hand_over_kernel(bands, mixed_hbm, smixed_hbm, out_hbm, sout_hbm, bands_ref, few_ref, sems):
    rows = mixed_hbm.shape[0] // bands
    moves = [(smixed_hbm, few_ref, sout_hbm)]
    for q in range(bands):
        part = pl.ds(q * rows, rows)
        moves.append((mixed_hbm.at[part], bands_ref.at[q], out_hbm.at[part]))
    ins = [pltpu.make_async_copy(a, b, sems.at[0, q]) for q, (a, b, _) in enumerate(moves)]
    outs = [pltpu.make_async_copy(b, c, sems.at[1, q]) for q, (_, b, c) in enumerate(moves)]
    for copy in ins:
        copy.start()
    for into, out in zip(ins, outs):
        into.wait()
        out.start()
    for copy in outs:
        copy.wait()


def per_device(
    prompt_values,
    prompt_gate,
    prompt_inject,
    prompt_read,
    prompt_step,
    decay_log,
    skip_gain,
    norm_weight,
    out_weight,
    sample_values,
    sample_gate,
    sample_inject,
    sample_read,
    sample_step,
    sample_length,
):
    n, peers = lax.axis_size("head"), lax.axis_size("ctx")
    levels = peers.bit_length() - 2
    scan_steps = 3 if levels == 2 else levels
    log_steps = 2 if levels == 2 else levels + 1
    tokens, channels = prompt_values.shape
    heads = prompt_step.shape[0]
    dim = channels // heads
    entries = prompt_inject.shape[2]
    half = entries // 2
    samples, length = sample_values.shape[:2]
    padded = -(-samples // (2 * PAD)) * 2 * PAD
    cols = out_weight.shape[1] // n
    blocks, chunks = tokens // BLOCK, channels // CHUNK
    part, per = cols // PARTS, blocks * PARTS
    vmem = pl.BlockSpec(memory_space=pltpu.VMEM)
    hbm = pl.BlockSpec(memory_space=pl.ANY)
    dma = pltpu.SemaphoreType.DMA
    shape = jax.ShapeDtypeStruct
    V = pltpu.VMEM
    mixed, smixed = pl.pallas_call(
        functools.partial(layer_kernel, dim, n, peers),
        out_shape=(shape((cols, tokens), BF16), shape((samples, cols), BF16)),
        in_specs=[
            pl.BlockSpec(memory_space=pltpu.SMEM),
            hbm,
            hbm,
            vmem,
            hbm,
            vmem,
            vmem,
            vmem,
            vmem,
            hbm,
            hbm,
            hbm,
            hbm,
            hbm,
            hbm,
        ],
        out_specs=(hbm, hbm),
        scratch_shapes=[
            V((tokens, channels), BF16),
            V((tokens, channels), BF16),
            V((tokens, entries), BF16),
            V(sample_values.shape, BF16),
            V(sample_gate.shape, BF16),
            V((samples, length, entries), BF16),
            V((samples, length, entries), BF16),
            V((samples, length, heads), F32),
            V(out_weight.shape, BF16),
            V((blocks, heads, BLOCK), F32),
            V((blocks, heads, BLOCK), F32),
            V((tokens, 2 * heads), BF16),
            V((2 * heads, channels), BF16),
            V((entries, tokens), BF16),
            V((PAD, channels), F32),
            V((entries, channels), BF16),
            V((half, channels), BF16),
            V((levels + 1, chunks, half, CHUNK), BF16),
            V((scan_steps, chunks, half, CHUNK), BF16),
            V((chunks, half, CHUNK), F32),
            V((half, channels), BF16),
            V((entries, channels), BF16),
            V((log_steps, PAD, heads), F32),
            V((log_steps, PAD, heads), F32),
            V((PAD, heads), F32),
            V((PAD, channels), F32),
            V((levels, PAD, channels), F32),
            V((entries, channels), F32),
            V((PAD, heads), F32),
            V((BLOCK, channels), F32),
            V((tokens + padded, channels), BF16),
            V((padded, channels), F32),
            V((padded, channels), F32),
            V((padded, entries), BF16),
            V((peers, padded, entries), BF16),
            V((peers - 1, -(-samples // PAD) * PAD, channels), F32),
            V((-(-samples // PAD) * PAD, channels), F32),
            V((BLOCK, part), F32),
            V((n, per, BLOCK, part), BF16),
            V((n + 1, per, BLOCK, part), BF16),
            V((n, samples * cols // LANES, LANES), BF16),
            V((n + 1, samples * cols // LANES, LANES), BF16),
            V((samples * cols // LANES, LANES), F32),
            V((cols, tokens), BF16),
            V((samples, cols), BF16),
            dma((chunks // GROUP,)),
            dma((8,)),
            dma((1,)),
            dma((1,)),
            dma((log_steps,)),
            dma((log_steps,)),
            dma((1,)),
            dma((chunks // GROUP,)),
            dma((scan_steps,)),
            dma((2 if levels == 2 else levels, chunks)),
            dma((1,)),
            dma((1,)),
            dma((1,)),
            dma((1,)),
            dma((1,)),
            dma((1,)),
            dma((n,)),
            dma((n + 1, per)),
            dma((n,)),
            dma((n + 1,)),
        ],
        compiler_params=pltpu.CompilerParams(
            collective_id=0, has_side_effects=True, vmem_limit_bytes=VMEM_LIMIT
        ),
    )(
        sample_length,
        prompt_values,
        prompt_gate,
        prompt_inject.reshape(tokens, entries),
        prompt_read.reshape(tokens, entries),
        prompt_step,
        decay_log[None],
        skip_gain[None],
        norm_weight[None],
        out_weight,
        sample_values,
        sample_gate,
        sample_inject.reshape(samples, length, entries),
        sample_read.reshape(samples, length, entries),
        sample_step.transpose(1, 2, 0),
    )
    bands = 4
    band = (cols // bands, tokens)
    mixed, smixed = pl.pallas_call(
        functools.partial(hand_over_kernel, bands),
        out_shape=(shape((cols, tokens), BF16), shape((samples, cols), BF16)),
        in_specs=[hbm, hbm],
        out_specs=(hbm, hbm),
        scratch_shapes=[
            V((bands, *band), BF16),
            V((samples, cols), BF16),
            dma((2, bands + 1)),
        ],
    )(mixed, smixed)
    return mixed, smixed.T


def solution(mesh):
    in_specs = (
        P("ctx", "head"),
        P("ctx", "head"),
        P("ctx", "head", None),
        P("ctx", "head", None),
        P("head", "ctx"),
        P("head"),
        P("head"),
        P("head"),
        P("head", None),
        P("ctx", None, "head"),
        P("ctx", None, "head"),
        P("ctx", None, "head", None),
        P("ctx", None, "head", None),
        P("head", "ctx", None),
        P("ctx"),
    )
    out_specs = (P("head", "ctx"), P("head", "ctx"))
    return jax.shard_map(
        per_device, mesh=mesh, in_specs=in_specs, out_specs=out_specs, check_vma=False
    )
```

```python
import functools

import jax
import jax.numpy as jnp
from jax import lax
from jax.experimental import pallas as pl
from jax.experimental.pallas import tpu as pltpu
from jax.sharding import PartitionSpec as P

BLOCK = 128
LANES = 128
PAD = 8
F32 = jnp.float32
BF16 = jnp.bfloat16
EXACT = lax.Precision.HIGHEST
VMEM_LIMIT = 60 * 1024 * 1024


def dot(a, b, dims=((1,), (0,)), precision=None):
    return lax.dot_general(a, b, (dims, ((), ())), precision=precision, preferred_element_type=F32)


def softplus(v):
    return jnp.maximum(v, 0.0) + jnp.log1p(jnp.exp(-jnp.abs(v)))


def silu(v):
    return v / (1.0 + jnp.exp(-v))


def spread(w, expander):
    high = w.astype(BF16)
    low = (w - high.astype(F32)).astype(BF16)
    return dot(jnp.concatenate([high, low], axis=1), expander)


def expander_of(heads, dim):
    row = lax.broadcasted_iota(jnp.int32, (2 * heads, heads * dim), 0)
    lane = lax.broadcasted_iota(jnp.int32, (2 * heads, heads * dim), 1)
    head = lane // dim
    return jnp.where((row == head) | (row == head + heads), 1.0, 0.0).astype(BF16)


def square(n):
    return (
        lax.broadcasted_iota(jnp.int32, (n, n), 0),
        lax.broadcasted_iota(jnp.int32, (n, n), 1),
    )


def finish_rows(total, weight):
    mean = jnp.mean(total * total, axis=1, keepdims=True)
    return (total * lax.rsqrt(mean + 1e-05) * weight).astype(BF16)


CHUNK = LANES
GROUP = 4
PARTS = 2
LAG = 3
HOOKS = 4


def turn_over(w):
    return jnp.transpose(w, (1, 0))


def layer_kernel(
    dim,
    n,
    peers,
    length_ref,
    values_hbm,
    gate_hbm,
    inject_ref,
    read_hbm,
    step_ref,
    decay_ref,
    gain_in_ref,
    norm_ref,
    weight_hbm,
    svalues_hbm,
    sgate_hbm,
    sinject_hbm,
    sread_hbm,
    sstep_hbm,
    out_hbm,
    sout_hbm,
    values_ref,
    gate_ref,
    read_ref,
    svalues_ref,
    sgate_ref,
    sinject_ref,
    sread_ref,
    sstep_ref,
    tiles_ref,
    steps_ref,
    logs_ref,
    wide_ref,
    expander_ref,
    turned_ref,
    skip_ref,
    mine_state,
    pair_state,
    totals,
    arrived,
    before_ref,
    swap_ref,
    enter_ref,
    log_sent,
    log_got,
    before_logs,
    pair_scale,
    scale_ref,
    state_ref,
    offset_ref,
    part_ref,
    normed_ref,
    slocal_ref,
    sgain_ref,
    picked_ref,
    picked_all,
    reply_ref,
    reply_got,
    acc_ref,
    sent,
    landing,
    ssent,
    slanding,
    sown_ref,
    result_ref,
    sresult_ref,
    value_sems,
    late_sems,
    tile_sems,
    out_sems,
    log_ssems,
    log_rsems,
    pair_ssems,
    pair_rsems,
    scan_ssems,
    scan_rsems,
    swap_ssems,
    swap_rsems,
    small_ssems,
    small_rsems,
    picked_sems,
    reply_sems,
    sent_sems,
    land_sems,
    ssent_sems,
    sland_sems,
):
    tokens, channels = values_ref.shape
    heads = step_ref.shape[0]
    entries = inject_ref.shape[1]
    half = entries // 2
    cols = weight_hbm.shape[1] // n
    part = acc_ref.shape[1]
    per = sent.shape[1]
    chunks = channels // CHUNK
    blocks = tokens // BLOCK
    levels = peers.bit_length() - 2
    squared = levels == 2
    log_steps = 2 if squared else levels + 1
    scan_steps = arrived.shape[0]
    place = lax.axis_index("head")
    seat = lax.axis_index("ctx")
    side = seat % 2
    odd = side == 1
    own_rows = pl.ds(pl.multiple_of(side * half, half), half)
    other_rows = pl.ds(pl.multiple_of((1 - side) * half, half), half)

    def lanes_of(c):
        return slice(c * CHUNK, (c + 1) * CHUNK)

    def some_lanes(c):
        return pl.ds(pl.multiple_of(c * CHUNK, CHUNK), CHUNK)

    groups = chunks // GROUP

    def group_lanes(q):
        return slice(q * GROUP * CHUNK, (q + 1) * GROUP * CHUNK)

    def value_copy(q):
        lanes = group_lanes(q)
        return pltpu.make_async_copy(values_hbm.at[:, lanes], values_ref.at[:, lanes], value_sems.at[q])

    late = [
        (gate_hbm, gate_ref),
        (read_hbm, read_ref),
        (svalues_hbm, svalues_ref),
        (sgate_hbm, sgate_ref),
        (sinject_hbm, sinject_ref),
        (sread_hbm, sread_ref),
        (sstep_hbm, sstep_ref),
    ]
    late_copies = [pltpu.make_async_copy(*refs, late_sems.at[q]) for q, refs in enumerate(late)]

    tile_copy = pltpu.make_async_copy(weight_hbm, tiles_ref, tile_sems.at[0])

    value_copy(0).start()

    def digit(s):
        return (seat // (1 << s)) % 2

    def mate(s):
        return seat + (1 << s) - (2 << s) * digit(s)

    barrier = pltpu.get_barrier_semaphore()

    def greet(device):
        pl.semaphore_signal(
            barrier, inc=1, device_id=device, device_id_type=pl.DeviceIdType.MESH
        )

    for s in range(levels + 1):
        greet({"ctx": mate(s)})

    last_seat = peers - 1
    holds_final = seat == last_seat

    @pl.when(holds_final)
    def _():
        for p in range(peers - 1):
            greet({"ctx": p})

    @pl.when(jnp.logical_not(holds_final))
    def _():
        greet({"ctx": last_seat})

    @pl.when(place > 0)
    def _():
        greet({"head": place - 1})

    @pl.when(place < n - 1)
    def _():
        greet({"head": place + 1})

    rows, lanes = square(heads)
    rate_row = -jnp.exp(decay_ref[...])
    rate = jnp.sum(jnp.where(rows == lanes, rate_row, 0.0), axis=1, keepdims=True)
    steps = softplus(step_ref[...])
    logs = steps * rate
    i, j = square(BLOCK)

    def fill_expander():
        expander_ref[...] = expander_of(heads, dim)

    fill_expander()
    def stack(ref, wide):
        for b in range(blocks):
            ref[b] = wide[:, b * BLOCK : (b + 1) * BLOCK]
        return ref[...].reshape(blocks * heads, BLOCK)

    tall_steps, tall_logs = stack(steps_ref, steps), stack(logs_ref, logs)
    after = dot(tall_logs, jnp.where(i > j, 1.0, 0.0), precision=EXACT)
    sums = jnp.sum(tall_logs, axis=1, keepdims=True)
    later, offsets = jnp.zeros((heads, 1), F32), []
    for b in reversed(range(blocks)):
        offsets.insert(0, later)
        later = later + sums[b * heads : (b + 1) * heads]
    w = turn_over(jnp.exp(after + jnp.concatenate(offsets, axis=0)) * tall_steps)
    for b in range(blocks):
        block_w = w[:, b * heads : (b + 1) * heads]
        high = block_w.astype(BF16)
        low = (block_w - high.astype(F32)).astype(BF16)
        wide_ref[b * BLOCK : (b + 1) * BLOCK, :] = jnp.concatenate([high, low], axis=1)
    total_logs = jnp.sum(jnp.where(rows == lanes, later, 0.0), axis=0, keepdims=True)
    total_logs = jnp.broadcast_to(total_logs, (PAD, heads))

    for q in range(1, groups):
        value_copy(q).start()

    def turn_inject():
        turned_ref[...] = turn_over(inject_ref[...].astype(F32)).astype(BF16)

    turn_inject()
    top = lax.broadcasted_iota(jnp.int32, (PAD, heads), 0) == 0

    inside = (place > 0) & (place < n - 1)
    log_sent[0] = total_logs
    before_logs[...] = jnp.zeros_like(before_logs)

    def state_of(q):
        lanes = group_lanes(q)
        value_copy(q).wait()
        wide = dot(wide_ref[...], expander_ref[:, lanes])
        scaled = (wide * values_ref[:, lanes].astype(F32)).astype(BF16)
        mine_state[:, lanes] = dot(turned_ref[...], scaled).astype(BF16)

    state_of(0)

    for middle in (False, True):
        for final in (False, True):

            @pl.when((inside == middle) & (holds_final == final))
            def _():
                pl.semaphore_wait(barrier, levels + 2 + middle + (peers - 1 if final else 1))

    def remote(src, dst, ssem, rsem, device):
        return pltpu.make_async_remote_copy(
            src_ref=src,
            dst_ref=dst,
            send_sem=ssem,
            recv_sem=rsem,
            device_id=device,
            device_id_type=pl.DeviceIdType.MESH,
        )

    def log_copy(s):
        return remote(
            log_sent.at[s], log_got.at[s], log_ssems.at[s], log_rsems.at[s], {"ctx": mate(s)}
        )

    def pair_copy(q):
        return remote(
            mine_state.at[other_rows, group_lanes(q)],
            pair_state.at[:, group_lanes(q)],
            pair_ssems.at[0],
            pair_rsems.at[q],
            {"ctx": mate(0)},
        )

    def scan_copy(s, c):
        slot = c // 2 + (s - 2) * (chunks // 2) if squared and s > 1 else c
        return remote(
            totals.at[s - 1, c],
            arrived.at[s - 1, c],
            scan_ssems.at[s - 1],
            scan_rsems.at[s - 1 if not squared or s == 1 else 1, slot],
            {"ctx": mate(1 if squared and s == 3 else s)},
        )

    def swap_copy(lanes, where):
        return remote(
            swap_ref.at[:, lanes],
            enter_ref.at[where, lanes],
            swap_ssems.at[0],
            swap_rsems.at[0],
            {"ctx": mate(0)},
        )

    log_copy(0).start()

    def exchange_logs(s):
        log_copy(s).wait_recv()
        got, own = log_got[s], log_sent[s]
        upper = digit(s) == 1
        above = jnp.where(upper, own, got)
        if s == 0:
            pair = jnp.where(top, above, jnp.where(odd, got, own))
            pair_scale[...] = spread(jnp.exp(pair), expander_ref[...])
        else:
            held = before_logs[...]
            crossed = jnp.where(digit(2) == 1, jnp.where(upper, got, own), above) if squared else above
            scale_ref[s - 1] = spread(jnp.exp(jnp.where(top, crossed, held)), expander_ref[...])
            before_logs[...] = held + jnp.where(upper, got, 0.0)
        if s < log_steps - 1:
            log_sent[s + 1] = own + got
            log_copy(s + 1).start()

    column, row = digit(1), digit(2)

    def at_once(c):
        if not squared:
            return seat >= 0
        if c % 2:
            return column == 0
        return (column == 1) & (row == 0)

    def pair_up(c):
        mine = mine_state[own_rows, lanes_of(c)].astype(F32)
        theirs = pair_state[:, lanes_of(c)].astype(F32)
        first, second = jnp.where(odd, theirs, mine), jnp.where(odd, mine, theirs)
        totals[0, c] = (first * pair_scale[0:1, lanes_of(c)] + second).astype(BF16)

        @pl.when(at_once(c))
        def _():
            scan_copy(1, c).start()

    pairs = chunks // 2

    def pair_group(q):
        pair_copy(q).wait_recv()
        for c in sorted(range(q * GROUP, (q + 1) * GROUP), key=lambda c: 1 - c % 2):
            pair_up(c)

    for q in range(groups):
        if q:
            state_of(q)
        pair_copy(q).start()
        if q == 0:
            for copy in late_copies:
                copy.start()
        if q == 1:
            exchange_logs(0)
        if q:
            pair_group(q - 1)
    pair_group(groups - 1)
    if squared:
        for c in range(0, chunks, 2):

            @pl.when((column == 0) & (row == 0))
            def _():
                scan_copy(1, c).start()

    def enter(c, before):
        even_state = jnp.where(odd, pair_state[:, some_lanes(c)].astype(F32), mine_state[own_rows, some_lanes(c)].astype(F32))
        moved = before * pair_scale[1:2, some_lanes(c)] + even_state
        enter_ref[own_rows, some_lanes(c)] = jnp.where(odd, moved, before).astype(BF16)
        swap_ref[:, some_lanes(c)] = jnp.where(odd, before, moved).astype(BF16)
        swap_copy(some_lanes(c), own_rows).start()

    def cross_row(q):
        c = 2 * q + column
        scan_copy(1, c).wait_recv()
        far, near = arrived[0, c].astype(F32), totals[0, c].astype(F32)
        right = column == 1
        first, second = jnp.where(right, far, near), jnp.where(right, near, far)
        totals[1, c] = (first * scale_ref[0, 0:1, some_lanes(c)] + second).astype(BF16)
        scan_copy(2, c).start()
        enter(c, jnp.where(right, far, 0.0))

        @pl.when(column == 0)
        def _():
            enter(c + 1, jnp.zeros((half, CHUNK), F32))

    def end_row(q):
        @pl.when(column == 1)
        def _():
            scan_copy(1, 2 * q).wait_recv()
            enter(2 * q, arrived[0, 2 * q].astype(F32))

    def next_row(q):
        c = 2 * q + column
        right = column == 1

        @pl.when(right)
        def _():
            scan_copy(1, c).wait_recv()
            totals[0, c] = arrived[0, c]

        scan_copy(2, c).wait_recv()
        far = arrived[1, c].astype(F32)
        joined = far * scale_ref[0, 0:1, some_lanes(c)] + totals[0, c].astype(F32)
        totals[2, c] = jnp.where(right, far, joined).astype(BF16)
        scan_copy(3, c).start()
        enter(c, jnp.where(right, joined, far))

    def last_column(q):
        c = 2 * q + 1 - column
        scan_copy(3, c).wait_recv()
        enter(c, arrived[2, c].astype(F32))

    def square_events():
        first = [(q, cross_row, q) for q in range(pairs)]
        first += [(q + pairs, end_row, q) for q in range(pairs)]
        second = [(q, next_row, q) for q in range(pairs)]
        second += [(q + 4.5, last_column, q) for q in range(pairs)]
        return [sorted(events, key=lambda event: event[0]) for events in (first, second)]

    def run_events(here, events):
        @pl.when(here)
        def _():
            for _, work, q in events:
                work(q)

    def scan_step(s, c):
        scan_copy(s, c).wait_recv()
        upper = digit(s) == 1
        far = arrived[s - 1, c].astype(F32)
        near = totals[s - 1, c].astype(F32)
        first, second = jnp.where(upper, far, near), jnp.where(upper, near, far)
        total_scale = scale_ref[s - 1, 0:1, some_lanes(c)]
        totals[s, c] = (first * total_scale + second).astype(BF16)
        if s == 1:
            before = jnp.where(upper, far, 0.0)
        else:
            held = before_ref[c]
            before = jnp.where(upper, far * scale_ref[s - 1, 1:2, some_lanes(c)] + held, held)
        if s < levels:
            before_ref[c] = before
            scan_copy(s + 1, c).start()
        else:
            enter(c, before)

    exchange_logs(1)

    skip_ref[...] = spread(jnp.broadcast_to(gain_in_ref[...], (PAD, heads)), expander_ref[...])

    def sample_local():
        samples, length = svalues_ref.shape[:2]
        slocal_ref[...] = jnp.zeros_like(slocal_ref)
        sgain_ref[...] = jnp.zeros_like(sgain_ref)
        picked_ref[...] = jnp.zeros_like(picked_ref)
        u, s = square(length)
        own = lax.broadcasted_iota(jnp.int32, (heads, channels), 1) // dim == (
            lax.broadcasted_iota(jnp.int32, (heads, channels), 0)
        )
        at = lax.broadcasted_iota(jnp.int32, (1, length), 1)
        for k in range(samples):
            last = length_ref[k] - 1
            hot = jnp.where(
                lax.broadcasted_iota(jnp.int32, (PAD, length), 1) == last, 1.0, 0.0
            ).astype(BF16)
            tall = softplus(sstep_ref[k])
            tall_logs = tall * rate_row
            flip = ((0,), (0,))
            gap = dot(tall_logs, jnp.where((u > s) & (u <= last), 1.0, 0.0), flip, EXACT)
            running = dot(tall_logs, jnp.where(u <= last, 1.0, 0.0), flip, EXACT)[:, 0:1]
            wide_steps = dot(tall, jnp.where(u == s, 1.0, 0.0), flip, EXACT)
            row = dot(hot, sread_ref[k])
            score = dot(row.astype(BF16), sinject_ref[k], ((1,), (1,)))[0:1]
            mixing = jnp.where(at <= last, score * jnp.exp(gap) * wide_steps, 0.0).astype(BF16)
            values = svalues_ref[k]
            local = jnp.sum(jnp.where(own, dot(mixing, values), 0.0), axis=0, keepdims=True)
            decay = jnp.sum(jnp.where(own, jnp.exp(running), 0.0), axis=0, keepdims=True)
            value = dot(hot, values)[0:1]
            opened = silu(dot(hot, sgate_ref[k])[0:1])
            slocal_ref[k : k + 1, :] = (local + skip_ref[0:1, :] * value) * opened
            sgain_ref[k : k + 1, :] = decay * opened
            picked_ref[k : k + 1, :] = row[0:1].astype(BF16)

    state_ref[...] = jnp.zeros_like(state_ref)
    offset_ref[...] = jnp.zeros_like(offset_ref)
    for copy in late_copies:
        copy.wait()
    tile_copy.start()

    def block_local(b, hook):
        span = pl.ds(pl.multiple_of(b * BLOCK, BLOCK), BLOCK)
        steps, logs = steps_ref[b], logs_ref[b]
        i, j = square(BLOCK)
        lower = jnp.where(i >= j, 1.0, 0.0)
        running = dot(logs, lower, ((1,), (1,)), EXACT)
        running_t = turn_over(running)
        after = turn_over(dot(logs, jnp.where(i > j, 1.0, 0.0), precision=EXACT))
        turned = turn_over(steps)
        expander = expander_ref[...]
        inject = inject_ref[span, :]
        readout = read_ref[span, :]
        scores = jnp.where(i >= j, dot(readout, inject, ((1,), (1,))), 0.0)
        per = LANES // dim
        lane = lax.broadcasted_iota(jnp.int32, (BLOCK, LANES), 1)
        for k in range(heads // per):
            cut = slice(k * LANES, (k + 1) * LANES)
            pair = values_ref[span, cut]
            mixes, parts = [], []
            for q in range(per):
                h = k * per + q
                gap = jnp.minimum(running_t[:, h : h + 1] - running[h : h + 1, :], 0.0)
                mixes.append((scores * jnp.exp(gap) * steps[h : h + 1, :]).astype(BF16))
                parts.append(jnp.where(lane // dim == q, pair, jnp.zeros_like(pair)))
            part_ref[:, cut] = dot(jnp.concatenate(mixes, axis=1), jnp.concatenate(parts, axis=0))
            if hook is not None and 2 * (k + 1) == heads // per:
                hook(HOOKS * b)
        if hook is not None:
            hook(HOOKS * b + 1)
        decay = spread(jnp.exp(running_t), expander)
        values = values_ref[span, :].astype(F32)
        opened = silu(gate_ref[span, :].astype(F32))
        total = part_ref[...] + skip_ref[0:1, :] * values
        total = total + dot(readout, state_ref[...].astype(BF16)) * decay
        normed_ref[span, :] = (total * opened).astype(BF16)
        if hook is not None:
            hook(HOOKS * b + 2)
        offset = offset_ref[0:1, :]
        gate_ref[span, :] = (opened * spread(jnp.exp(running_t + offset), expander)).astype(BF16)
        offset_ref[0:1, :] = offset + running_t[BLOCK - 1 : BLOCK, :]
        scaled = (spread(jnp.exp(after) * turned, expander) * values).astype(BF16)
        state_ref[...] = state_ref[...] * decay[BLOCK - 1 : BLOCK, :] + dot(
            inject, scaled, ((0,), (0,))
        )
        if hook is not None:
            hook(HOOKS * b + 3)

    def hook(g):
        if squared:
            run_events(row == 0, square_events()[0][g : g + 1])
            return

        for s in range(2, levels + 1):

            @pl.when(g == s - 1)
            def _():
                exchange_logs(s)

        for s in range(1, levels + 1):
            c = g - LAG * (s - 1)

            @pl.when((c >= 0) & (c < chunks))
            def _():
                scan_step(s, c)

    def picked_copy(p):
        return remote(
            picked_ref, picked_all.at[p], small_ssems.at[0], picked_sems.at[0], {"ctx": last_seat}
        )

    def reply_copy(p):
        return remote(
            reply_ref.at[p], reply_got, reply_sems.at[0], small_rsems.at[0], {"ctx": p}
        )

    def late_round(g, carry):
        hook(g)
        return carry

    block_local(0, hook)
    if squared:
        first, second = square_events()
        run_events(row == 0, first[HOOKS:])
        run_events(row == 1, second)
    else:
        lax.fori_loop(HOOKS, max(chunks + LAG * (levels - 1), HOOKS), late_round, 0)
    swap_copy(slice(0, channels), other_rows).wait_recv()
    tile_copy.wait()

    def share(d, q):
        rows = rows_of(q // PARTS)
        start = pl.multiple_of(d * cols + q % PARTS * part, part)
        return dot(normed_ref[rows, :], tiles_ref[:, pl.ds(start, part)])

    def hop_up(d, b):
        return remote(
            sent.at[d, b],
            landing.at[d + 1, b],
            sent_sems.at[d],
            land_sems.at[d + 1, b],
            {"head": place + 1},
        )

    def hop_down(d, b):
        return remote(
            sent.at[d, b],
            landing.at[d, b],
            sent_sems.at[d],
            land_sems.at[d, b],
            {"head": place - 1},
        )

    def all_up(d):
        return remote(
            sent.at[d], landing.at[d + 1], sent_sems.at[d], land_sems.at[0, 0], {"head": place + 1}
        )

    def all_down(d):
        return remote(
            sent.at[d], landing.at[d], sent_sems.at[d], land_sems.at[0, 0], {"head": place - 1}
        )

    def shop_up(d):
        return remote(
            ssent.at[d],
            slanding.at[d + 1],
            ssent_sems.at[d],
            sland_sems.at[d + 1],
            {"head": place + 1},
        )

    def shop_down(d):
        return remote(
            ssent.at[d], slanding.at[d], ssent_sems.at[d], sland_sems.at[d], {"head": place - 1}
        )

    def rows_of(b):
        return pl.ds(pl.multiple_of(b * BLOCK, BLOCK), BLOCK)

    def pass_on(d, b, slot, move, fed):
        acc_ref[...] = share(d, b)

        @pl.when(fed)
        def _():
            move(d, b).wait_recv()
            acc_ref[...] = acc_ref[...] + landing[slot, b].astype(F32)

        sent[d, b] = acc_ref[...].astype(BF16)
        move(d, b).start()

    def finish_block(b):
        span = rows_of(b)
        readout = read_ref[span, :]
        pieces = []
        for q in range(groups):
            lanes = group_lanes(q)
            arrival = dot(readout, enter_ref[:, lanes])
            piece = normed_ref[span, lanes].astype(F32)
            pieces.append(piece + arrival * gate_ref[span, lanes].astype(F32))
        normed_ref[span, :] = finish_rows(jnp.concatenate(pieces, axis=1), norm_ref[...])

    padded = slocal_ref.shape[0]
    few_rows = reply_got.shape[0]
    srows = pl.ds(tokens, padded)

    def answer():
        picked_all[last_seat] = picked_ref[...]
        others = picked_all.at[pl.ds(0, peers - 1)]
        remote(others, others, small_ssems.at[0], picked_sems.at[0], {"ctx": 0}).wait_recv()
        asked = picked_all[...].reshape(peers * padded, entries)
        for q in range(groups):
            lanes = group_lanes(q)
            entered = enter_ref[:, lanes].astype(F32) * pair_scale[0:1, lanes]
            final = entered + mine_state[:, lanes].astype(F32)
            told = dot(asked, final.astype(BF16))
            for p in range(peers - 1):
                reply_ref[p, :, lanes] = told[p * padded : p * padded + few_rows]
            reply_got[:, lanes] = told[last_seat * padded : last_seat * padded + few_rows]
        for p in range(peers - 1):
            reply_copy(p).start()

    def finish_samples():
        @pl.when(jnp.logical_not(holds_final))
        def _():
            reply_copy(0).wait_recv()

        total = slocal_ref[:few_rows] + reply_got[...] * sgain_ref[:few_rows]
        normed = finish_rows(total, norm_ref[...])
        if few_rows < padded:
            normed = jnp.concatenate([normed, jnp.zeros((padded - few_rows, channels), BF16)], axis=0)
        normed_ref[srows, :] = normed

    few = sresult_ref.shape[0]

    def sshare(d):
        wide = dot(normed_ref[srows, :], tiles_ref[:, pl.ds(pl.multiple_of(d * cols, cols), cols)])
        return jnp.concatenate([wide[:few, q * LANES : (q + 1) * LANES] for q in range(cols // LANES)], axis=0)

    def spass_on(d, slot, move, fed):
        sown_ref[...] = sshare(d)

        @pl.when(fed)
        def _():
            move(d).wait_recv()
            sown_ref[...] = sown_ref[...] + slanding[slot].astype(F32)

        ssent[d] = sown_ref[...].astype(BF16)
        move(d).start()

    sample_start = PARTS * (blocks + 1)

    def step(t, carry):
        block, first_part, last_part = t // PARTS, t % PARTS == 0, t % PARTS == PARTS - 1

        @pl.when((block < blocks) & first_part)
        def _():
            finish_block(block)

        @pl.when(t == sample_start)
        def _():
            finish_samples()

        rising, falling = t - place, t - (n - 1 - place)
        up, down = n - 1 - rising // per, falling // per

        @pl.when((rising >= 0) & (up > place))
        def _():
            pass_on(up, rising % per, up + 1, hop_up, place > 0)

        @pl.when((falling >= 0) & (down < place))
        def _():
            pass_on(down, falling % per, down, hop_down, place < n - 1)

        srising, sfalling = rising - sample_start, falling - sample_start
        sup, sdown = n - 1 - srising, sfalling

        @pl.when((srising >= 0) & (sup > place))
        def _():
            spass_on(sup, sup + 1, shop_up, place > 0)

        @pl.when((sfalling >= 0) & (sdown < place))
        def _():
            spass_on(sdown, sdown, shop_down, place < n - 1)

        @pl.when((block + 1 < blocks) & last_part)
        def _():
            block_local(block + 1, None)

        @pl.when((block == blocks - 2) & last_part)
        def _():
            sample_local()

            @pl.when(jnp.logical_not(holds_final))
            def _():
                picked_copy(seat).start()

        @pl.when((block == blocks - 1) & last_part & holds_final)
        def _():
            answer()

        return carry

    lax.fori_loop(0, (n - 1) * per, step, 0)
    sown_ref[...] = sshare(place)

    @pl.when(place < n - 1)
    def _():
        shop_down(place).wait_recv()
        sown_ref[...] = sown_ref[...] + slanding[place].astype(F32)

    @pl.when(place > 0)
    def _():
        shop_up(place).wait_recv()
        sown_ref[...] = sown_ref[...] + slanding[place + 1].astype(F32)

    for q in range(cols // LANES):
        sresult_ref[:, q * LANES : (q + 1) * LANES] = sown_ref[q * few : (q + 1) * few, :].astype(BF16)
    sout_copy = pltpu.make_async_copy(sresult_ref, sout_hbm, late_sems.at[len(late)])
    sout_copy.start()

    remote(
        mine_state.at[other_rows], pair_state, pair_ssems.at[0], pair_rsems.at[0], {"ctx": mate(0)}
    ).wait_send()
    swap_copy(slice(0, channels), own_rows).wait_send()

    def scan_sent(s, count):
        span = pl.ds(0, count)
        remote(
            totals.at[s - 1, span],
            arrived.at[s - 1, span],
            scan_ssems.at[s - 1],
            scan_rsems.at[s - 1, 0],
            {"ctx": mate(1)},
        ).wait_send()

    for s in range(1, scan_steps + 1):
        if not squared:
            scan_sent(s, chunks)
        elif s == 1:

            @pl.when((column == 0) & (row == 0))
            def _():
                scan_sent(1, chunks)

            @pl.when(column + row == 1)
            def _():
                scan_sent(1, pairs)

        else:

            @pl.when(row == s - 2)
            def _():
                scan_sent(s, pairs)

    for s in range(log_steps):
        log_copy(s).wait_send()

    @pl.when(holds_final)
    def _():
        remote(reply_ref, reply_ref, reply_sems.at[0], small_rsems.at[0], {"ctx": 0}).wait_send()

    @pl.when(jnp.logical_not(holds_final))
    def _():
        picked_copy(seat).wait_send()

    def out_place(b):
        return pl.ds(pl.multiple_of(b % PARTS * part, part), part), rows_of(b // PARTS)

    def gather(b, carry):
        acc_ref[...] = share(place, b)

        @pl.when(place < n - 1)
        def _():
            hop_down(place, b).wait_recv()
            acc_ref[...] = acc_ref[...] + landing[place, b].astype(F32)

        @pl.when(place > 0)
        def _():
            hop_up(place, b).wait_recv()
            acc_ref[...] = acc_ref[...] + landing[place + 1, b].astype(F32)

        where = out_place(b)
        result_ref[where] = turn_over(acc_ref[...]).astype(BF16)
        pltpu.make_async_copy(result_ref.at[where], out_hbm.at[where], out_sems.at[0]).start()
        return carry

    lax.fori_loop(0, per, gather, 0)
    for d in range(n):

        @pl.when(d > place)
        def _():
            all_up(d).wait_send()
            shop_up(d).wait_send()

        @pl.when(d < place)
        def _():
            all_down(d).wait_send()
            shop_down(d).wait_send()

    sout_copy.wait()
    pltpu.make_async_copy(result_ref, out_hbm, out_sems.at[0]).wait()


def hand_over_kernel(bands, mixed_hbm, smixed_hbm, out_hbm, sout_hbm, bands_ref, few_ref, sems):
    rows = mixed_hbm.shape[0] // bands
    moves = [(smixed_hbm, few_ref, sout_hbm)]
    for q in range(bands):
        part = pl.ds(q * rows, rows)
        moves.append((mixed_hbm.at[part], bands_ref.at[q], out_hbm.at[part]))
    ins = [pltpu.make_async_copy(a, b, sems.at[0, q]) for q, (a, b, _) in enumerate(moves)]
    outs = [pltpu.make_async_copy(b, c, sems.at[1, q]) for q, (_, b, c) in enumerate(moves)]
    for copy in ins:
        copy.start()
    for into, out in zip(ins, outs):
        into.wait()
        out.start()
    for copy in outs:
        copy.wait()


def per_device(
    prompt_values,
    prompt_gate,
    prompt_inject,
    prompt_read,
    prompt_step,
    decay_log,
    skip_gain,
    norm_weight,
    out_weight,
    sample_values,
    sample_gate,
    sample_inject,
    sample_read,
    sample_step,
    sample_length,
):
    n, peers = lax.axis_size("head"), lax.axis_size("ctx")
    levels = peers.bit_length() - 2
    scan_steps = 3 if levels == 2 else levels
    log_steps = 2 if levels == 2 else levels + 1
    tokens, channels = prompt_values.shape
    heads = prompt_step.shape[0]
    dim = channels // heads
    entries = prompt_inject.shape[2]
    half = entries // 2
    samples, length = sample_values.shape[:2]
    padded = -(-samples // (2 * PAD)) * 2 * PAD
    cols = out_weight.shape[1] // n
    blocks, chunks = tokens // BLOCK, channels // CHUNK
    part, per = cols // PARTS, blocks * PARTS
    vmem = pl.BlockSpec(memory_space=pltpu.VMEM)
    hbm = pl.BlockSpec(memory_space=pl.ANY)
    dma = pltpu.SemaphoreType.DMA
    shape = jax.ShapeDtypeStruct
    V = pltpu.VMEM
    mixed, smixed = pl.pallas_call(
        functools.partial(layer_kernel, dim, n, peers),
        out_shape=(shape((cols, tokens), BF16), shape((samples, cols), BF16)),
        in_specs=[
            pl.BlockSpec(memory_space=pltpu.SMEM),
            hbm,
            hbm,
            vmem,
            hbm,
            vmem,
            vmem,
            vmem,
            vmem,
            hbm,
            hbm,
            hbm,
            hbm,
            hbm,
            hbm,
        ],
        out_specs=(hbm, hbm),
        scratch_shapes=[
            V((tokens, channels), BF16),
            V((tokens, channels), BF16),
            V((tokens, entries), BF16),
            V(sample_values.shape, BF16),
            V(sample_gate.shape, BF16),
            V((samples, length, entries), BF16),
            V((samples, length, entries), BF16),
            V((samples, length, heads), F32),
            V(out_weight.shape, BF16),
            V((blocks, heads, BLOCK), F32),
            V((blocks, heads, BLOCK), F32),
            V((tokens, 2 * heads), BF16),
            V((2 * heads, channels), BF16),
            V((entries, tokens), BF16),
            V((PAD, channels), F32),
            V((entries, channels), BF16),
            V((half, channels), BF16),
            V((levels + 1, chunks, half, CHUNK), BF16),
            V((scan_steps, chunks, half, CHUNK), BF16),
            V((chunks, half, CHUNK), F32),
            V((half, channels), BF16),
            V((entries, channels), BF16),
            V((log_steps, PAD, heads), F32),
            V((log_steps, PAD, heads), F32),
            V((PAD, heads), F32),
            V((PAD, channels), F32),
            V((levels, PAD, channels), F32),
            V((entries, channels), F32),
            V((PAD, heads), F32),
            V((BLOCK, channels), F32),
            V((tokens + padded, channels), BF16),
            V((padded, channels), F32),
            V((padded, channels), F32),
            V((padded, entries), BF16),
            V((peers, padded, entries), BF16),
            V((peers - 1, -(-samples // PAD) * PAD, channels), F32),
            V((-(-samples // PAD) * PAD, channels), F32),
            V((BLOCK, part), F32),
            V((n, per, BLOCK, part), BF16),
            V((n + 1, per, BLOCK, part), BF16),
            V((n, samples * cols // LANES, LANES), BF16),
            V((n + 1, samples * cols // LANES, LANES), BF16),
            V((samples * cols // LANES, LANES), F32),
            V((cols, tokens), BF16),
            V((samples, cols), BF16),
            dma((chunks // GROUP,)),
            dma((8,)),
            dma((1,)),
            dma((1,)),
            dma((log_steps,)),
            dma((log_steps,)),
            dma((1,)),
            dma((chunks // GROUP,)),
            dma((scan_steps,)),
            dma((2 if levels == 2 else levels, chunks)),
            dma((1,)),
            dma((1,)),
            dma((1,)),
            dma((1,)),
            dma((1,)),
            dma((1,)),
            dma((n,)),
            dma((n + 1, per)),
            dma((n,)),
            dma((n + 1,)),
        ],
        compiler_params=pltpu.CompilerParams(
            collective_id=0, has_side_effects=True, vmem_limit_bytes=VMEM_LIMIT
        ),
    )(
        sample_length,
        prompt_values,
        prompt_gate,
        prompt_inject.reshape(tokens, entries),
        prompt_read.reshape(tokens, entries),
        prompt_step,
        decay_log[None],
        skip_gain[None],
        norm_weight[None],
        out_weight,
        sample_values,
        sample_gate,
        sample_inject.reshape(samples, length, entries),
        sample_read.reshape(samples, length, entries),
        sample_step.transpose(1, 2, 0),
    )
    bands = 4
    band = (cols // bands, tokens)
    mixed, smixed = pl.pallas_call(
        functools.partial(hand_over_kernel, bands),
        out_shape=(shape((cols, tokens), BF16), shape((samples, cols), BF16)),
        in_specs=[hbm, hbm],
        out_specs=(hbm, hbm),
        scratch_shapes=[
            V((bands, *band), BF16),
            V((samples, cols), BF16),
            dma((2, bands + 1)),
        ],
    )(mixed, smixed)
    return mixed, smixed.T


def solution(mesh):
    in_specs = (
        P("ctx", "head"),
        P("ctx", "head"),
        P("ctx", "head", None),
        P("ctx", "head", None),
        P("head", "ctx"),
        P("head"),
        P("head"),
        P("head"),
        P("head", None),
        P("ctx", None, "head"),
        P("ctx", None, "head"),
        P("ctx", None, "head", None),
        P("ctx", None, "head", None),
        P("head", "ctx", None),
        P("ctx"),
    )
    out_specs = (P("head", "ctx"), P("head", "ctx"))
    return jax.shard_map(
        per_device, mesh=mesh, in_specs=in_specs, out_specs=out_specs, check_vma=False
    )
```
